16 devices in a mesh: sp: 16 (over z, y, x, core).
Axes of the slice: x: 2, y: 2, z: 2, core: 2. Of those that a mesh axis runs over, the one named last changes fastest.
Arguments:
- x_act: bfloat16 [4096, 1024], P('sp')
- positions: int32 [4096], P('sp')
- grad_out: bfloat16 [4096, 1024], P('sp')
- g_attn: bfloat16 [1024], P('sp')
- w_q: bfloat16 [1024, 16, 64], P('sp')
- w_k: bfloat16 [1024, 16, 64], P('sp')
- w_v: bfloat16 [1024, 16, 64], P('sp')
- w_o: bfloat16 [16, 64, 1024], P('sp')
- g_mlp: bfloat16 [1024], P('sp')
- w_gate: bfloat16 [1024, 2816], P('sp')
- w_up: bfloat16 [1024, 2816], P('sp')
- w_down: bfloat16 [2816, 1024], P('sp')
Outputs:
- output 1: bfloat16 [4096, 1024], P('sp')
- output 2: bfloat16 [4096, 1024], P('sp')
- output 3: float32 [1024], P('sp')
- output 4: float32 [1024, 16, 64], P('sp')
- output 5: float32 [1024, 16, 64], P('sp')
- output 6: float32 [1024, 16, 64], P('sp')
- output 7: float32 [16, 64, 1024], P('sp')
- output 8: float32 [1024], P('sp')
- output 9: float32 [1024, 2816], P('sp')
- output 10: float32 [1024, 2816], P('sp')
- output 11: float32 [2816, 1024], P('sp')
All inputs are finite; a program needn't handle non-finite values.
Results may differ from the reference program's by a relative error of at most 0.0169985.
Values are sent between devices in bfloat16 or wider.
A program may use at most 1 GiB of HBM per device.

```python
import jax
import jax.numpy as jnp
from jax import lax

D = 1024
HEADS = 16
KV_HEADS = 16
HEAD = 64
FF = 2816
SEQ = 4096

RMS_EPS = 1e-5
ROPE_BASE = 10000.0


def setup_inputs(seed: int = 0) -> dict:
    key_list = jax.random.split(jax.random.key(seed), 12)
    x_act = jax.random.normal(key_list[0], (SEQ, D), jnp.float32)
    steps_drawn = jax.random.randint(key_list[1], (SEQ,), 1, 3)
    positions = (jnp.cumsum(steps_drawn) - steps_drawn[0]).astype(jnp.int32)
    grad_out = jax.random.normal(key_list[2], (SEQ, D), jnp.float32)
    g_attn = 1.0 + 0.25 * jax.random.normal(key_list[3], (D,), jnp.float32)
    w_q = jax.random.normal(key_list[4], (D, HEADS, HEAD), jnp.float32) * (1.4 * D ** -0.5)
    w_k = jax.random.normal(key_list[5], (D, KV_HEADS, HEAD), jnp.float32) * (1.4 * D ** -0.5)
    w_v = jax.random.normal(key_list[6], (D, KV_HEADS, HEAD), jnp.float32) * (D ** -0.5)
    w_o = jax.random.normal(key_list[7], (HEADS, HEAD, D), jnp.float32) * ((HEADS * HEAD) ** -0.5)
    g_mlp = 1.0 + 0.25 * jax.random.normal(key_list[8], (D,), jnp.float32)
    w_gate = jax.random.normal(key_list[9], (D, FF), jnp.float32) * (D ** -0.5)
    w_up = jax.random.normal(key_list[10], (D, FF), jnp.float32) * (D ** -0.5)
    w_down = jax.random.normal(key_list[11], (FF, D), jnp.float32) * (FF ** -0.5)
    return dict(x_act=x_act.astype(jnp.bfloat16), positions=positions, grad_out=grad_out.astype(jnp.bfloat16), g_attn=g_attn.astype(jnp.bfloat16), w_q=w_q.astype(jnp.bfloat16), w_k=w_k.astype(jnp.bfloat16), w_v=w_v.astype(jnp.bfloat16), w_o=w_o.astype(jnp.bfloat16), g_mlp=g_mlp.astype(jnp.bfloat16), w_gate=w_gate.astype(jnp.bfloat16), w_up=w_up.astype(jnp.bfloat16), w_down=w_down.astype(jnp.bfloat16))


def rope_tables(positions):
    half_dim = HEAD // 2
    inv_freq = ROPE_BASE ** (-(jnp.arange(half_dim, dtype=jnp.float32) * (2.0 / HEAD)))
    angle_tab = positions.astype(jnp.float32)[:, None] * inv_freq[None, :]
    return jnp.cos(angle_tab)[:, None, :], jnp.sin(angle_tab)[:, None, :]


def apply_rope(values_in, cos_tab, sin_tab):
    half_dim = values_in.shape[-1] // 2
    first_half = values_in[..., :half_dim]
    second_half = values_in[..., half_dim:]
    return jnp.concatenate([first_half * cos_tab - second_half * sin_tab, second_half * cos_tab + first_half * sin_tab], axis=-1)


def rms_norm(act_in, gain_vec):
    act_f = act_in.astype(jnp.float32)
    inv_rms = lax.rsqrt(jnp.mean(act_f * act_f, axis=-1, keepdims=True) + RMS_EPS)
    return (act_f * inv_rms * gain_vec).astype(jnp.bfloat16)


def head_attention(head_in):
    q_head, k_head, v_head = head_in
    scores = jnp.einsum('sgd,td->gst', q_head.astype(jnp.float32), k_head.astype(jnp.float32)) * (HEAD ** -0.5)
    causal = jnp.arange(SEQ)[:, None] >= jnp.arange(SEQ)[None, :]
    scores = jnp.where(causal[None, :, :], scores, -1e30)
    attn_prob = jax.nn.softmax(scores, axis=-1).astype(jnp.bfloat16)
    attn_out = jnp.einsum('gst,td->sgd', attn_prob.astype(jnp.float32), v_head.astype(jnp.float32))
    return attn_out.astype(jnp.bfloat16)


def layer_forward(x_act, positions, params):
    g_attn, w_q, w_k, w_v, w_o, g_mlp, w_gate, w_up, w_down = params
    group_size = HEADS // KV_HEADS
    cos_tab, sin_tab = rope_tables(positions)
    normed_f = rms_norm(x_act, g_attn).astype(jnp.float32)
    queries = apply_rope(jnp.einsum('sd,dhe->she', normed_f, w_q), cos_tab, sin_tab).astype(jnp.bfloat16)
    key_proj = apply_rope(jnp.einsum('sd,dhe->she', normed_f, w_k), cos_tab, sin_tab).astype(jnp.bfloat16)
    value_proj = jnp.einsum('sd,dhe->she', normed_f, w_v).astype(jnp.bfloat16)
    q_heads = jnp.transpose(queries.reshape(SEQ, KV_HEADS, group_size, HEAD), (1, 0, 2, 3))
    attn_heads = lax.map(jax.checkpoint(head_attention), (q_heads, jnp.transpose(key_proj, (1, 0, 2)), jnp.transpose(value_proj, (1, 0, 2))))
    attn_heads = jnp.transpose(attn_heads, (1, 0, 2, 3)).reshape(SEQ, HEADS, HEAD)
    hidden = (x_act.astype(jnp.float32) + jnp.einsum('she,hed->sd', attn_heads.astype(jnp.float32), w_o)).astype(jnp.bfloat16)
    normed_mlp = rms_norm(hidden, g_mlp).astype(jnp.float32)
    gate_pre = jnp.dot(normed_mlp, w_gate, preferred_element_type=jnp.float32)
    up_pre = jnp.dot(normed_mlp, w_up, preferred_element_type=jnp.float32)
    mixed_act = (jax.nn.silu(gate_pre) * up_pre).astype(jnp.bfloat16)
    return (hidden.astype(jnp.float32) + jnp.dot(mixed_act.astype(jnp.float32), w_down, preferred_element_type=jnp.float32)).astype(jnp.bfloat16)


def reference(x_act, positions, grad_out, g_attn, w_q, w_k, w_v, w_o, g_mlp, w_gate, w_up, w_down):
    params = tuple(weight.astype(jnp.float32) for weight in (g_attn, w_q, w_k, w_v, w_o, g_mlp, w_gate, w_up, w_down))

    def layer_of(act_in, param_in):
        return layer_forward(act_in, positions, param_in)

    y_out, pullback = jax.vjp(layer_of, x_act, params)
    grad_x, grad_params = pullback(grad_out)
    return (y_out, grad_x, grad_params[0], grad_params[1], grad_params[2], grad_params[3], grad_params[4], grad_params[5], grad_params[6], grad_params[7], grad_params[8])
```

```python
import jax
import jax.numpy as jnp
from jax import lax
from jax.experimental import pallas as pl
from jax.experimental.pallas import tpu as pltpu
from jax.sharding import PartitionSpec as P

SEQ_AXIS = 'sp'
RMS_EPS = 1e-5
ROPE_BASE = 10000.0
MASK_VALUE = -1e30
TILE = 512
F32 = jnp.float32
BF16 = jnp.bfloat16


def rms_norm(act_in, gain_vec):
    act_f = act_in.astype(F32)
    inv_rms = lax.rsqrt(jnp.mean(act_f * act_f, axis=-1, keepdims=True) + RMS_EPS)
    return (act_f * inv_rms * gain_vec.astype(F32)).astype(BF16), inv_rms


def rms_norm_bwd(act_in, gain_vec, inv_rms, d_normed):
    act_f = act_in.astype(F32)
    d_f = d_normed.astype(F32)
    scaled_d = d_f * gain_vec.astype(F32)
    proj_mean = jnp.mean(scaled_d * act_f, axis=-1, keepdims=True)
    d_act = inv_rms * scaled_d - act_f * (inv_rms * inv_rms * inv_rms) * proj_mean
    d_gain = jnp.sum(d_f * act_f * inv_rms, axis=0)
    return d_act, d_gain


def dot(lhs, rhs, l_dim, r_dim):
    return lax.dot_general(lhs, rhs, (((l_dim,), (r_dim,)), ((), ())), preferred_element_type=F32)


def gather(shard):
    return lax.all_gather(shard, SEQ_AXIS, axis=0, tiled=True)


def exchange(blocks):
    return lax.all_to_all(blocks, SEQ_AXIS, 0, 0, tiled=True)


def rope_t(vals, cos_tab, sin_tab):
    half = vals.shape[0] // 2
    first, second = vals[:half], vals[half:]
    return jnp.concatenate([first * cos_tab - second * sin_tab, second * cos_tab + first * sin_tab], axis=0)


def mm(lhs, rhs):
    return jnp.dot(lhs, rhs, preferred_element_type=F32)


def diag_mask(tile):
    key_at = lax.broadcasted_iota(jnp.int32, (tile, tile), 0)
    query_at = lax.broadcasted_iota(jnp.int32, (tile, tile), 1)
    return key_at <= query_at


def attn_fwd_kernel(tile, q_t, k_ref, v_t, o_ref, of_ref, lse_ref, s_buf):
    step = pl.program_id(0)
    query = q_t[...]

    def scores(j):
        return mm(k_ref[pl.ds(pl.multiple_of(j * tile, tile), tile), :], query)

    def absorb(j, logits, top, total):
        new_top = jnp.maximum(top, jnp.max(logits, axis=0, keepdims=True))
        s_buf[pl.ds(pl.multiple_of(j * tile, tile), tile), :] = logits
        return new_top, total * jnp.exp(top - new_top) + jnp.sum(jnp.exp(logits - new_top), axis=0, keepdims=True)

    top, total = absorb(step, jnp.where(diag_mask(tile), scores(step), MASK_VALUE), jnp.full((1, tile), MASK_VALUE, F32), jnp.zeros((1, tile), F32))
    top, total = lax.fori_loop(0, step, lambda j, c: absorb(j, scores(j), *c), (top, total))
    lse = top + jnp.log(total)

    def weigh(j, acc):
        at = pl.ds(pl.multiple_of(j * tile, tile), tile)
        prob = jnp.exp(s_buf[at, :] - lse).astype(BF16)
        return acc + mm(v_t[:, at], prob)

    out = lax.fori_loop(0, step + 1, weigh, jnp.zeros((v_t.shape[0], tile), F32))
    of_ref[...] = out
    lse_ref[...] = lse
    block = o_ref.shape[2]
    for part in range(tile // block):
        o_ref[part] = out[:, part * block:(part + 1) * block].astype(BF16)


def attention_fwd(q_t, k_in, v_t, n_blocks):
    head_dim, seq = q_t.shape
    block = seq // n_blocks
    per = TILE // block
    return pl.pallas_call(
        lambda *refs: attn_fwd_kernel(TILE, *refs),
        grid=(seq // TILE,),
        in_specs=[pl.BlockSpec((head_dim, TILE), lambda i: (0, i)), pl.BlockSpec((seq, head_dim), lambda i: (0, 0)), pl.BlockSpec((head_dim, seq), lambda i: (0, 0))],
        out_specs=[pl.BlockSpec((per, head_dim, block), lambda i: (i, 0, 0)), pl.BlockSpec((head_dim, TILE), lambda i: (0, i)), pl.BlockSpec((1, TILE), lambda i: (0, i))],
        out_shape=[jax.ShapeDtypeStruct((n_blocks, head_dim, block), BF16), jax.ShapeDtypeStruct((head_dim, seq), F32), jax.ShapeDtypeStruct((1, seq), F32)],
        scratch_shapes=[pltpu.VMEM((seq, TILE), F32)],
        cost_estimate=pl.CostEstimate(flops=8 * seq * seq * head_dim, bytes_accessed=8 * seq * head_dim, transcendentals=seq * seq),
        name='attn_fwd',
    )(q_t, k_in, v_t)


def attn_bwd_kernel(tile, q_ref, q_t, do_ref, do_t, of_t, lse_ref, k_ref, k_t, v_ref, dq_t, dk_ref, dv_ref, acc):
    step = pl.program_id(0)
    query, query_t, d_out, d_out_t = q_ref[...], q_t[...], do_ref[...], do_t[...]
    lse = lse_ref[...]
    delta = jnp.sum(d_out_t.astype(F32) * of_t[...], axis=0, keepdims=True)

    @pl.when(step == 0)
    def _():
        dk_ref[...] = jnp.zeros_like(dk_ref)
        dv_ref[...] = jnp.zeros_like(dv_ref)

    acc[...] = jnp.zeros_like(acc)

    def visit(j, masked):
        at = pl.ds(pl.multiple_of(j * tile, tile), tile)
        logits = mm(k_ref[at, :], query_t)
        prob = jnp.exp(logits - lse)
        if masked:
            prob = jnp.where(diag_mask(tile), prob, 0.0)
        d_prob = mm(v_ref[at, :], d_out_t).astype(BF16).astype(F32)
        d_logits = (prob * (d_prob - delta)).astype(BF16)
        dv_ref[at, :] += mm(prob.astype(BF16), d_out)
        dk_ref[at, :] += mm(d_logits, query)
        acc[...] += mm(k_t[:, at], d_logits)

    visit(step, True)

    @pl.loop(0, step)
    def _(j):
        visit(j, False)

    dq_t[...] = acc[...]


def attention_bwd(q_in, q_t, do_in, do_t, of_t, lse, k_in, k_t, v_in):
    head_dim, seq = q_t.shape
    rows = pl.BlockSpec((TILE, head_dim), lambda i: (i, 0))
    cols = pl.BlockSpec((head_dim, TILE), lambda i: (0, i))
    all_rows = pl.BlockSpec((seq, head_dim), lambda i: (0, 0))
    all_cols = pl.BlockSpec((head_dim, seq), lambda i: (0, 0))
    return pl.pallas_call(
        lambda *refs: attn_bwd_kernel(TILE, *refs),
        grid=(seq // TILE,),
        in_specs=[rows, cols, rows, cols, cols, pl.BlockSpec((1, TILE), lambda i: (0, i)), all_rows, all_cols, all_rows],
        out_specs=[cols, all_rows, all_rows],
        out_shape=[jax.ShapeDtypeStruct((head_dim, seq), F32), jax.ShapeDtypeStruct((seq, head_dim), F32), jax.ShapeDtypeStruct((seq, head_dim), F32)],
        scratch_shapes=[pltpu.VMEM((head_dim, TILE), F32)],
        cost_estimate=pl.CostEstimate(flops=20 * seq * seq * head_dim, bytes_accessed=20 * seq * head_dim, transcendentals=seq * seq),
        name='attn_bwd',
    )(q_in, q_t, do_in, do_t, of_t, lse, k_in, k_t, v_in)


def gate_backward(d_mixed, gate_pre, up_pre):
    gate_sig = jax.nn.sigmoid(gate_pre)
    d_up = (d_mixed * gate_pre * gate_sig).astype(BF16)
    d_gate = (d_mixed * up_pre * gate_sig * (1.0 + gate_pre * (1.0 - gate_sig))).astype(BF16)
    return d_gate, d_up


def device_step(n_dev, x_act, positions, grad_out, g_attn_s, w_q, w_k, w_v, w_o, g_mlp_s, w_gate, w_up, w_down):
    tok, width = x_act.shape
    seq = tok * n_dev
    rows, heads, head_dim = w_q.shape
    ff = w_gate.shape[1]
    ff_s = ff // n_dev
    qkv = 3 * head_dim

    small = jnp.concatenate([(positions // 64).astype(BF16), (positions % 64).astype(BF16), g_attn_s, g_mlp_s])
    small = jnp.pad(small, (0, width - small.shape[0]))[None, :]
    x_ext = gather(jnp.concatenate([x_act, jnp.pad(small, ((0, 7), (0, 0)))], axis=0)[None])
    w_qkv = jnp.concatenate([w_q, w_k, w_v], axis=2)
    col_parts = jnp.concatenate([w_qkv, w_gate.reshape(rows, n_dev, ff_s), w_up.reshape(rows, n_dev, ff_s)], axis=2)
    w_cols = exchange(jnp.transpose(col_parts, (1, 0, 2))).reshape(width, qkv + 2 * ff_s)
    w_od = gather(jnp.concatenate([w_o[0], w_down], axis=0)[None])
    w_o_all = w_od[:, :head_dim].reshape(width, width)
    w_down_all = w_od[:, head_dim:].reshape(ff, width)
    w_gu = gather(jnp.concatenate([w_gate, w_up], axis=1))
    w_qkv_all = gather(w_qkv.reshape(rows, heads * qkv))

    x_all = x_ext[:, :tok].reshape(seq, width)
    extra = x_ext[:, tok].astype(F32)
    pos_all = extra[:, :tok] * 64.0 + extra[:, tok:2 * tok]
    g_attn = extra[:, 2 * tok:2 * tok + rows].reshape(width)
    g_mlp = extra[:, 2 * tok + rows:2 * tok + 2 * rows].reshape(width)
    half = head_dim // 2
    inv_freq = ROPE_BASE ** (-(jnp.arange(half, dtype=F32) * (2.0 / head_dim)))
    angle_t = inv_freq[:, None] * pos_all.reshape(1, seq)
    cos_t, sin_t = jnp.cos(angle_t), jnp.sin(angle_t)

    u_all = rms_norm(x_all, g_attn)[0]
    proj_t = dot(w_cols[:, :qkv], u_all, 0, 1)
    q_t = (rope_t(proj_t[:head_dim], cos_t, sin_t).astype(BF16).astype(F32) * (head_dim ** -0.5)).astype(BF16)
    k_t = rope_t(proj_t[head_dim:2 * head_dim], cos_t, sin_t).astype(BF16)
    v_t = proj_t[2 * head_dim:].astype(BF16)
    q_in, k_in, v_in = q_t.T, k_t.T, v_t.T
    o_blocks, of_t, lse = attention_fwd(q_t, k_in, v_t, n_dev)
    o_loc = exchange(o_blocks).reshape(width, tok)

    hidden = (x_act.astype(F32) + dot(o_loc, w_o_all, 0, 0)).astype(BF16)
    normed_mlp, inv_rms_mlp = rms_norm(hidden, g_mlp)
    a_dy = gather(jnp.concatenate([normed_mlp, grad_out], axis=1))
    pre = dot(normed_mlp, w_gu, 1, 0)
    gate_pre, up_pre = pre[:, :ff], pre[:, ff:]
    mixed = (jax.nn.silu(gate_pre) * up_pre).astype(BF16)
    y_out = (hidden.astype(F32) + dot(mixed, w_down_all, 1, 0)).astype(BF16)

    d_mixed = dot(grad_out, w_down_all, 1, 1).astype(BF16).astype(F32)
    d_gu = jnp.concatenate(gate_backward(d_mixed, gate_pre, up_pre), axis=1)
    d_normed = dot(d_gu, w_gu, 1, 1).astype(BF16)
    d_hid_norm, part_g_mlp = rms_norm_bwd(hidden, g_mlp, inv_rms_mlp, d_normed)
    d_hidden = (grad_out.astype(F32) + d_hid_norm).astype(BF16)
    do_blocks = exchange(dot(w_o_all, d_hidden, 1, 1).astype(BF16).reshape(n_dev, head_dim, tok))
    dh_all = gather(d_hidden)

    do_t = jnp.transpose(do_blocks, (1, 0, 2)).reshape(head_dim, seq)
    dq_t, dk, dv = attention_bwd(q_in, q_t, do_t.T, do_t, of_t, lse, k_in, k_t, v_in)
    dq_t = (dq_t * (head_dim ** -0.5)).astype(BF16).astype(F32)
    dk_t = dk.astype(BF16).T.astype(F32)
    d_proj_t = jnp.concatenate([rope_t(dq_t, cos_t, -sin_t).astype(BF16), rope_t(dk_t, cos_t, -sin_t).astype(BF16), dv.astype(BF16).T], axis=0)
    d_proj = exchange(jnp.transpose(d_proj_t.reshape(qkv, n_dev, tok), (1, 0, 2))).reshape(heads * qkv, tok)
    grad_w_qkv = dot(u_all, d_proj_t, 0, 1)

    inv_rms = lax.rsqrt(jnp.mean(jnp.square(x_act.astype(F32)), axis=-1, keepdims=True) + RMS_EPS)
    d_u = dot(d_proj, w_qkv_all, 0, 1).astype(BF16)
    d_x_norm, part_g_attn = rms_norm_bwd(x_act, g_attn, inv_rms, d_u)
    grad_x = (d_hidden.astype(F32) + d_x_norm).astype(BF16)

    a_all, dy_all = a_dy[:, :width], a_dy[:, width:]
    pre_t = dot(w_cols[:, qkv:], a_all, 0, 1)
    gate_t, up_t = pre_t[:ff_s], pre_t[ff_s:]
    d_mixed_t = dot(w_down, dy_all, 1, 1).astype(BF16).astype(F32)
    mixed_t = (jax.nn.silu(gate_t) * up_t).astype(BF16)
    d_gu_t = jnp.concatenate(gate_backward(d_mixed_t, gate_t, up_t), axis=0)
    grad_w_down = dot(mixed_t, dy_all, 1, 0)
    grad_w_gu = dot(a_all, d_gu_t, 0, 1)
    grad_w_o = dot(o_blocks.transpose(1, 0, 2).reshape(head_dim, seq), dh_all, 1, 0)[None]

    mlp_back = exchange(jnp.concatenate([grad_w_gu, part_g_mlp[:, None]], axis=1).reshape(n_dev, rows, 2 * ff_s + 1))
    attn_back = exchange(jnp.concatenate([grad_w_qkv, part_g_attn[:, None]], axis=1).reshape(n_dev, rows, qkv + 1))
    grad_g_mlp = jnp.sum(mlp_back[:, :, 2 * ff_s], axis=0)
    grad_g_attn = jnp.sum(attn_back[:, :, qkv], axis=0)
    mlp_rows = jnp.transpose(mlp_back, (1, 0, 2))
    attn_rows = jnp.transpose(attn_back, (1, 0, 2))
    grad_w_gate = mlp_rows[:, :, :ff_s].reshape(rows, ff)
    grad_w_up = mlp_rows[:, :, ff_s:2 * ff_s].reshape(rows, ff)
    grad_w_q, grad_w_k, grad_w_v = (attn_rows[:, :, i * head_dim:(i + 1) * head_dim] for i in range(3))
    return (y_out, grad_x, grad_g_attn, grad_w_q, grad_w_k, grad_w_v, grad_w_o, grad_g_mlp, grad_w_gate, grad_w_up, grad_w_down)


def solution(mesh):
    n_dev = mesh.shape[SEQ_AXIS]
    token_spec = P(SEQ_AXIS, None)
    cube_spec = P(SEQ_AXIS, None, None)
    gain_spec = P(SEQ_AXIS)
    weight_specs = (gain_spec, cube_spec, cube_spec, cube_spec, cube_spec, gain_spec, token_spec, token_spec, token_spec)
    return jax.shard_map(lambda *args: device_step(n_dev, *args), mesh=mesh, in_specs=(token_spec, gain_spec, token_spec) + weight_specs, out_specs=(token_spec, token_spec) + weight_specs, check_vma=False)
```

```python
import jax
import jax.numpy as jnp
from jax import lax
from jax.experimental import pallas as pl
from jax.experimental.pallas import tpu as pltpu
from jax.sharding import PartitionSpec as P

SEQ_AXIS = 'sp'
RMS_EPS = 1e-5
ROPE_BASE = 10000.0
MASK_VALUE = -1e30
TILE = 512
F32 = jnp.float32
BF16 = jnp.bfloat16


def rms_norm(act_in, gain_vec):
    act_f = act_in.astype(F32)
    inv_rms = lax.rsqrt(jnp.mean(act_f * act_f, axis=-1, keepdims=True) + RMS_EPS)
    return (act_f * inv_rms * gain_vec.astype(F32)).astype(BF16), inv_rms


def rms_norm_bwd(act_in, gain_vec, inv_rms, d_normed):
    act_f = act_in.astype(F32)
    d_f = d_normed.astype(F32)
    scaled_d = d_f * gain_vec.astype(F32)
    proj_mean = jnp.mean(scaled_d * act_f, axis=-1, keepdims=True)
    d_act = inv_rms * scaled_d - act_f * (inv_rms * inv_rms * inv_rms) * proj_mean
    d_gain = jnp.sum(d_f * act_f * inv_rms, axis=0)
    return d_act, d_gain


def dot(lhs, rhs, l_dim, r_dim):
    return lax.dot_general(lhs, rhs, (((l_dim,), (r_dim,)), ((), ())), preferred_element_type=F32)


def gather(shard):
    return lax.all_gather(shard, SEQ_AXIS, axis=0, tiled=True)


def exchange(blocks):
    return lax.all_to_all(blocks, SEQ_AXIS, 0, 0, tiled=True)


def rope_t(vals, cos_tab, sin_tab):
    half = vals.shape[0] // 2
    first, second = vals[:half], vals[half:]
    return jnp.concatenate([first * cos_tab - second * sin_tab, second * cos_tab + first * sin_tab], axis=0)


def mm(lhs, rhs):
    return jnp.dot(lhs, rhs, preferred_element_type=F32)


def diag_mask(tile):
    key_at = lax.broadcasted_iota(jnp.int32, (tile, tile), 0)
    query_at = lax.broadcasted_iota(jnp.int32, (tile, tile), 1)
    return key_at <= query_at


def attn_fwd_kernel(tile, q_t, k_ref, v_t, o_ref, of_ref, lse_ref, s_buf):
    step = pl.program_id(0)
    query = q_t[...]

    def scores(j):
        return mm(k_ref[pl.ds(pl.multiple_of(j * tile, tile), tile), :], query)

    def absorb(j, logits, top, total):
        new_top = jnp.maximum(top, jnp.max(logits, axis=0, keepdims=True))
        s_buf[pl.ds(pl.multiple_of(j * tile, tile), tile), :] = logits
        return new_top, total * jnp.exp(top - new_top) + jnp.sum(jnp.exp(logits - new_top), axis=0, keepdims=True)

    top, total = absorb(step, jnp.where(diag_mask(tile), scores(step), MASK_VALUE), jnp.full((1, tile), MASK_VALUE, F32), jnp.zeros((1, tile), F32))
    top, total = lax.fori_loop(0, step, lambda j, c: absorb(j, scores(j), *c), (top, total))
    lse = top + jnp.log(total)

    def weigh(j, acc):
        at = pl.ds(pl.multiple_of(j * tile, tile), tile)
        prob = jnp.exp(s_buf[at, :] - lse).astype(BF16)
        return acc + mm(v_t[:, at], prob)

    out = lax.fori_loop(0, step + 1, weigh, jnp.zeros((v_t.shape[0], tile), F32))
    of_ref[...] = out
    lse_ref[...] = lse
    block = o_ref.shape[2]
    for part in range(tile // block):
        o_ref[part] = out[:, part * block:(part + 1) * block].astype(BF16)


def attention_fwd(q_t, k_in, v_t, n_blocks):
    head_dim, seq = q_t.shape
    block = seq // n_blocks
    per = TILE // block
    return pl.pallas_call(
        lambda *refs: attn_fwd_kernel(TILE, *refs),
        grid=(seq // TILE,),
        in_specs=[pl.BlockSpec((head_dim, TILE), lambda i: (0, i)), pl.BlockSpec((seq, head_dim), lambda i: (0, 0)), pl.BlockSpec((head_dim, seq), lambda i: (0, 0))],
        out_specs=[pl.BlockSpec((per, head_dim, block), lambda i: (i, 0, 0)), pl.BlockSpec((head_dim, TILE), lambda i: (0, i)), pl.BlockSpec((1, TILE), lambda i: (0, i))],
        out_shape=[jax.ShapeDtypeStruct((n_blocks, head_dim, block), BF16), jax.ShapeDtypeStruct((head_dim, seq), F32), jax.ShapeDtypeStruct((1, seq), F32)],
        scratch_shapes=[pltpu.VMEM((seq, TILE), F32)],
        cost_estimate=pl.CostEstimate(flops=8 * seq * seq * head_dim, bytes_accessed=8 * seq * head_dim, transcendentals=seq * seq),
        name='attn_fwd',
    )(q_t, k_in, v_t)


def attn_bwd_kernel(tile, block, q_t, do_t, of_t, lse_ref, cos_ref, sin_ref, k_ref, k_t, v_ref, cos_all, sin_all, d_blocks, d_proj_t, dq_acc, dk_acc, dv_acc):
    step = pl.program_id(0)
    head_dim = q_t.shape[0]
    query_t, d_out_t = q_t[...], do_t[...]
    lse = lse_ref[...]
    delta = jnp.sum(d_out_t.astype(F32) * of_t[...], axis=0, keepdims=True)

    @pl.when(step == 0)
    def _():
        dk_acc[...] = jnp.zeros_like(dk_acc)
        dv_acc[...] = jnp.zeros_like(dv_acc)

    dq_acc[...] = jnp.zeros_like(dq_acc)

    def visit(j, masked):
        at = pl.ds(pl.multiple_of(j * tile, tile), tile)
        prob = jnp.exp(mm(k_ref[at, :], query_t) - lse)
        if masked:
            prob = jnp.where(diag_mask(tile), prob, 0.0)
        d_prob = mm(v_ref[at, :], d_out_t).astype(BF16).astype(F32)
        d_logits = (prob * (d_prob - delta)).astype(BF16)
        dv_acc[:, at] += dot(d_out_t, prob.astype(BF16), 1, 1)
        dk_acc[:, at] += dot(query_t, d_logits, 1, 1)
        dq_acc[...] += mm(k_t[:, at], d_logits)

    visit(step, True)

    @pl.loop(0, step)
    def _(j):
        visit(j, False)

    def put(row, col_block, values):
        rows = slice(row, row + values.shape[0])
        d_proj_t[rows, pl.ds(pl.multiple_of(col_block * block, block), values.shape[1])] = values
        for part in range(values.shape[1] // block):
            d_blocks[col_block + part, rows, :] = values[:, part * block:(part + 1) * block]

    d_q = (dq_acc[...] * (head_dim ** -0.5)).astype(BF16).astype(F32)
    per = tile // block
    put(0, step * per, rope_t(d_q, cos_ref[...], -sin_ref[...]).astype(BF16))

    @pl.when(step == pl.num_programs(0) - 1)
    def _():
        @pl.loop(0, pl.num_programs(0))
        def _(j):
            at = pl.ds(pl.multiple_of(j * tile, tile), tile)
            put(head_dim, j * per, rope_t(dk_acc[:, at].astype(BF16).astype(F32), cos_all[:, at], -sin_all[:, at]).astype(BF16))
            put(2 * head_dim, j * per, dv_acc[:, at].astype(BF16))


def attention_bwd(q_t, do_t, of_t, lse, k_in, k_t, v_in, cos_t, sin_t, n_blocks):
    head_dim, seq = q_t.shape
    block = seq // n_blocks
    cols = pl.BlockSpec((head_dim, TILE), lambda i: (0, i))
    half_cols = pl.BlockSpec((head_dim // 2, TILE), lambda i: (0, i))
    all_rows = pl.BlockSpec((seq, head_dim), lambda i: (0, 0))
    all_cols = pl.BlockSpec((head_dim, seq), lambda i: (0, 0))
    all_half = pl.BlockSpec((head_dim // 2, seq), lambda i: (0, 0))
    return pl.pallas_call(
        lambda *refs: attn_bwd_kernel(TILE, block, *refs),
        grid=(seq // TILE,),
        in_specs=[cols, cols, cols, pl.BlockSpec((1, TILE), lambda i: (0, i)), half_cols, half_cols, all_rows, all_cols, all_rows, all_half, all_half],
        out_specs=[pl.BlockSpec((n_blocks, 3 * head_dim, block), lambda i: (0, 0, 0)), pl.BlockSpec((3 * head_dim, seq), lambda i: (0, 0))],
        out_shape=[jax.ShapeDtypeStruct((n_blocks, 3 * head_dim, block), BF16), jax.ShapeDtypeStruct((3 * head_dim, seq), BF16)],
        scratch_shapes=[pltpu.VMEM((head_dim, TILE), F32), pltpu.VMEM((head_dim, seq), F32), pltpu.VMEM((head_dim, seq), F32)],
        cost_estimate=pl.CostEstimate(flops=20 * seq * seq * head_dim, bytes_accessed=20 * seq * head_dim, transcendentals=seq * seq),
        name='attn_bwd',
    )(q_t, do_t, of_t, lse, cos_t, sin_t, k_in, k_t, v_in, cos_t, sin_t)


PARTS = ((0, 96), (96, 80), (176, 80))
CORE, CHIP_AXES = 1, (2, 4, 8)


def flip(dev, bit):
    return dev + bit * (1 - 2 * ((dev // bit) % 2))


def start_copy(src, dst, send_sem, recv_sem, peer):
    copy = pltpu.make_async_remote_copy(src_ref=src, dst_ref=dst, send_sem=send_sem, recv_sem=recv_sem, device_id=(peer,), device_id_type=pl.DeviceIdType.MESH)
    copy.start()
    return copy


def landed(ref, sem):
    pltpu.make_async_copy(ref, ref, sem).wait()


def enter_all(me, n_dev):
    barrier = pltpu.get_barrier_semaphore()

    @pl.loop(1, n_dev)
    def _(hop):
        pl.semaphore_signal(barrier, inc=1, device_id=(lax.rem(me + hop, n_dev),), device_id_type=pl.DeviceIdType.MESH)

    pl.semaphore_wait(barrier, n_dev - 1)


class CubeGather:
    def __init__(self, me, buf, send_sem, recv_sem, core_sem):
        self.me, self.buf = me, buf
        self.send_sem, self.recv_sem, self.core_sem = send_sem, recv_sem, core_sem
        self.sent = []

    def part(self, dev, p):
        return self.buf.at[dev, pl.ds(PARTS[p][0], PARTS[p][1])]

    def axes(self, p):
        return [CHIP_AXES[(p + i) % 3] for i in range(3)]

    def owner(self, p, index, start=None):
        dev = self.me if start is None else start
        for i, bit in enumerate(self.axes(p)):
            if (index >> i) & 1:
                dev = flip(dev, bit)
        return dev

    def push(self, p, index, axis):
        ref = self.part(self.owner(p, index), p)
        self.sent.append(start_copy(ref, ref, self.send_sem.at[len(self.sent)], self.recv_sem.at[p, index + (1 << axis)], flip(self.me, self.axes(p)[axis])))

    def push_core(self, p, index):
        ref = self.part(self.owner(p, index), p)
        self.sent.append(start_copy(ref, ref, self.send_sem.at[len(self.sent)], self.core_sem.at[p, index], flip(self.me, CORE)))

    def begin(self):
        for axis in range(3):
            for p in range(3):
                self.push(p, 0, axis)
        for p in range(3):
            self.push_core(p, 0)

    def receive(self, index):
        for p in range(3):
            landed(self.part(self.owner(p, index), p), self.recv_sem.at[p, index])
            for axis in range(index.bit_length(), 3):
                self.push(p, index, axis)
            self.push_core(p, index)

    def receive_core(self, index):
        for p in range(3):
            landed(self.part(self.owner(p, index, flip(self.me, CORE)), p), self.core_sem.at[p, index])

    def finish(self):
        for copy in self.sent:
            copy.wait_send()


N_SENDS = 9 + 12 + 24


def gather_proj_kernel(n_dev, x_ref, small_ref, w_ref, u_out, proj_t, small_all, x_buf, u_buf, w_buf, send_sem, recv_sem, core_sem, misc_send, misc_recv, local_sem, u_sem):
    me = lax.axis_index(SEQ_AXIS)
    own = pltpu.make_async_copy(x_ref, x_buf.at[me], local_sem.at[0])
    own.start()
    own_w = pltpu.make_async_copy(w_ref.at[me], w_buf.at[me], local_sem.at[1])
    own_w.start()
    own_small = pltpu.make_async_copy(small_ref, small_all.at[me], local_sem.at[2])
    own_small.start()
    enter_all(me, n_dev)
    own.wait()
    cube = CubeGather(me, x_buf, send_sem, recv_sem, core_sem)
    cube.begin()

    def spread(hop):
        peer = lax.rem(me + hop, n_dev)
        return [
            pltpu.make_async_remote_copy(src_ref=small_ref, dst_ref=small_all.at[me], send_sem=misc_send.at[0, hop], recv_sem=misc_recv.at[0, me], device_id=(peer,), device_id_type=pl.DeviceIdType.MESH),
            pltpu.make_async_remote_copy(src_ref=w_ref.at[peer], dst_ref=w_buf.at[me], send_sem=misc_send.at[1, hop], recv_sem=misc_recv.at[1, me], device_id=(peer,), device_id_type=pl.DeviceIdType.MESH),
        ]

    for kind in range(2):
        @pl.loop(1, n_dev)
        def _(hop, kind=kind):
            spread(hop)[kind].start()

    cube.receive(1)
    cube.receive(2)
    own_w.wait()
    own_small.wait()

    @pl.loop(1, n_dev)
    def _(hop):
        src = lax.rem(me + hop, n_dev)
        landed(small_all.at[src], misc_recv.at[0, src])
        landed(w_buf.at[src], misc_recv.at[1, src])

    width = x_ref.shape[1]
    tok = x_ref.shape[0]
    rows = w_ref.shape[1]
    gain = jnp.concatenate([small_all[d, 0:1, 0:rows] for d in range(n_dev)], axis=1)
    weight = w_buf[...].reshape(width, w_ref.shape[2])
    keep = proj_t.shape[0]
    flushes = []

    def project(dev):
        act = x_buf[dev].astype(F32)
        inv = lax.rsqrt(jnp.mean(act * act, axis=-1, keepdims=True) + RMS_EPS)
        normed = (act * inv * gain).astype(BF16)
        u_buf[dev] = normed
        proj_t[:, pl.ds(pl.multiple_of(dev * tok, tok), tok)] = mm(normed, weight).T[:keep]
        flush = pltpu.make_async_copy(u_buf.at[dev], u_out.at[dev], u_sem.at[len(flushes)])
        flush.start()
        flushes.append(flush)

    other = flip(me, CORE)
    cube.receive_core(0)
    project(me)
    project(other)
    cube.receive(4)
    cube.receive(3)
    for index in (1, 2, 4):
        cube.receive_core(index)
    for bit in CHIP_AXES:
        project(flip(me, bit))
        project(flip(other, bit))
    cube.receive(5)
    cube.receive(6)
    for index in (3, 5, 6):
        cube.receive_core(index)
    for skip in range(3):
        bits = [bit for i, bit in enumerate(CHIP_AXES) if i != skip]
        project(flip(flip(me, bits[0]), bits[1]))
        project(flip(flip(other, bits[0]), bits[1]))
    cube.receive(7)
    cube.receive_core(7)
    far = flip(flip(flip(me, 2), 4), 8)
    project(far)
    project(flip(far, CORE))

    cube.finish()

    @pl.loop(1, n_dev)
    def _(hop):
        for copy in spread(hop):
            copy.wait_send()

    for flush in flushes:
        flush.wait()


def gather_proj(n_dev, x_act, small, w_blocks, qkv):
    tok, width = x_act.shape
    seq = tok * n_dev
    any_spec = pl.BlockSpec(memory_space=pl.ANY)
    vmem_spec = pl.BlockSpec(memory_space=pltpu.VMEM)
    return pl.pallas_call(
        lambda *refs: gather_proj_kernel(n_dev, *refs),
        in_specs=[any_spec, vmem_spec, vmem_spec],
        out_specs=[any_spec, vmem_spec, vmem_spec],
        out_shape=[jax.ShapeDtypeStruct((n_dev, tok, width), BF16), jax.ShapeDtypeStruct((qkv, seq), F32), jax.ShapeDtypeStruct((n_dev,) + small.shape, F32)],
        scratch_shapes=[
            pltpu.VMEM((n_dev, tok, width), BF16),
            pltpu.VMEM((n_dev, tok, width), BF16),
            pltpu.VMEM(w_blocks.shape, BF16),
            pltpu.SemaphoreType.DMA((N_SENDS,)),
            pltpu.SemaphoreType.DMA((3, 8)),
            pltpu.SemaphoreType.DMA((3, 8)),
            pltpu.SemaphoreType.DMA((2, n_dev)),
            pltpu.SemaphoreType.DMA((2, n_dev)),
            pltpu.SemaphoreType.DMA((3,)),
            pltpu.SemaphoreType.DMA((n_dev,)),
        ],
        compiler_params=pltpu.CompilerParams(collective_id=0, has_side_effects=True),
        cost_estimate=pl.CostEstimate(flops=30 * seq * width * width, bytes_accessed=4 * seq * width, transcendentals=0),
        name='gather_proj',
    )(x_act, small, w_blocks)


def gate_backward(d_mixed, gate_pre, up_pre):
    gate_sig = jax.nn.sigmoid(gate_pre)
    d_up = (d_mixed * gate_pre * gate_sig).astype(BF16)
    d_gate = (d_mixed * up_pre * gate_sig * (1.0 + gate_pre * (1.0 - gate_sig))).astype(BF16)
    return d_gate, d_up


def device_step(n_dev, x_act, positions, grad_out, g_attn_s, w_q, w_k, w_v, w_o, g_mlp_s, w_gate, w_up, w_down):
    tok, width = x_act.shape
    seq = tok * n_dev
    rows, heads, head_dim = w_q.shape
    ff = w_gate.shape[1]
    ff_s = ff // n_dev
    qkv = 3 * head_dim

    small = jnp.concatenate([jnp.concatenate([g_attn_s, g_mlp_s]).astype(F32)[None], positions.astype(F32).reshape(-1, 2 * rows)], axis=0)
    small = jnp.pad(small, ((0, 8 - small.shape[0]), (0, 0)))
    w_qkv = jnp.concatenate([w_q, w_k, w_v], axis=2)
    w_blocks = jnp.pad(jnp.transpose(w_qkv, (1, 0, 2)), ((0, 0), (0, 0), (0, 256 - qkv)))
    u_all, proj_t, small_all = gather_proj(n_dev, x_act, small, w_blocks, qkv)
    u_all = u_all.reshape(seq, width)
    g_attn = small_all[:, 0, :rows].reshape(width)
    g_mlp = small_all[:, 0, rows:2 * rows].reshape(width)
    pos_all = small_all[:, 1:1 + tok // (2 * rows)]

    down_groups = [w_down[i:i + rows] for i in range(0, ff_s, rows)]
    down_groups = [jnp.pad(group, ((0, rows - group.shape[0]), (0, 0))) for group in down_groups]
    w_all = gather(jnp.concatenate([w_gate, w_up, w_o[0]] + down_groups + [w_qkv.reshape(rows, heads * qkv)], axis=1))
    w_gu = w_all[:, :2 * ff]
    w_o_all = w_all[:, 2 * ff:2 * ff + width]
    w_down_at = 2 * ff + width
    down_all = [w_all[:, w_down_at + i * width:w_down_at + (i + 1) * width].reshape(n_dev, rows, width) for i in range(len(down_groups))]
    w_down_all = jnp.concatenate(down_all, axis=1)[:, :ff_s].reshape(ff, width)
    w_qkv_all = w_all[:, w_down_at + len(down_groups) * width:]
    col_parts = jnp.concatenate([w_gate.reshape(rows, n_dev, ff_s), w_up.reshape(rows, n_dev, ff_s)], axis=2)
    w_cols = exchange(jnp.transpose(col_parts, (1, 0, 2))).reshape(width, 2 * ff_s)

    half = head_dim // 2
    inv_freq = ROPE_BASE ** (-(jnp.arange(half, dtype=F32) * (2.0 / head_dim)))
    angle_t = inv_freq[:, None] * pos_all.reshape(1, seq)
    cos_t, sin_t = jnp.cos(angle_t), jnp.sin(angle_t)

    q_t = (rope_t(proj_t[:head_dim], cos_t, sin_t).astype(BF16).astype(F32) * (head_dim ** -0.5)).astype(BF16)
    k_t = rope_t(proj_t[head_dim:2 * head_dim], cos_t, sin_t).astype(BF16)
    v_t = proj_t[2 * head_dim:].astype(BF16)
    k_in, v_in = k_t.T, v_t.T
    o_blocks, of_t, lse = attention_fwd(q_t, k_in, v_t, n_dev)
    o_loc = exchange(o_blocks).reshape(width, tok)

    hidden = (x_act.astype(F32) + dot(o_loc, w_o_all, 0, 0)).astype(BF16)
    normed_mlp, inv_rms_mlp = rms_norm(hidden, g_mlp)
    a_dy = gather(jnp.concatenate([normed_mlp, grad_out], axis=1))
    pre = dot(normed_mlp, w_gu, 1, 0)
    gate_pre, up_pre = pre[:, :ff], pre[:, ff:]
    mixed = (jax.nn.silu(gate_pre) * up_pre).astype(BF16)
    y_out = (hidden.astype(F32) + dot(mixed, w_down_all, 1, 0)).astype(BF16)

    d_mixed = dot(grad_out, w_down_all, 1, 1).astype(BF16).astype(F32)
    d_gu = jnp.concatenate(gate_backward(d_mixed, gate_pre, up_pre), axis=1)
    d_normed = dot(d_gu, w_gu, 1, 1).astype(BF16)
    d_hid_norm, part_g_mlp = rms_norm_bwd(hidden, g_mlp, inv_rms_mlp, d_normed)
    d_hidden = (grad_out.astype(F32) + d_hid_norm).astype(BF16)
    do_blocks = exchange(dot(w_o_all, d_hidden, 1, 1).astype(BF16).reshape(n_dev, head_dim, tok))
    dh_all = gather(d_hidden)

    do_t = jnp.transpose(do_blocks, (1, 0, 2)).reshape(head_dim, seq)
    d_blocks, d_proj_t = attention_bwd(q_t, do_t, of_t, lse, k_in, k_t, v_in, cos_t, sin_t, n_dev)
    d_proj = exchange(d_blocks).reshape(heads * qkv, tok)
    grad_w_qkv = dot(u_all, d_proj_t, 0, 1)

    inv_rms = lax.rsqrt(jnp.mean(jnp.square(x_act.astype(F32)), axis=-1, keepdims=True) + RMS_EPS)
    d_u = dot(d_proj, w_qkv_all, 0, 1).astype(BF16)
    d_x_norm, part_g_attn = rms_norm_bwd(x_act, g_attn, inv_rms, d_u)
    grad_x = (d_hidden.astype(F32) + d_x_norm).astype(BF16)

    a_all, dy_all = a_dy[:, :width], a_dy[:, width:]
    pre_t = dot(w_cols, a_all, 0, 1)
    gate_t, up_t = pre_t[:ff_s], pre_t[ff_s:]
    d_mixed_t = dot(w_down, dy_all, 1, 1).astype(BF16).astype(F32)
    mixed_t = (jax.nn.silu(gate_t) * up_t).astype(BF16)
    d_gu_t = jnp.concatenate(gate_backward(d_mixed_t, gate_t, up_t), axis=0)
    grad_w_down = dot(mixed_t, dy_all, 1, 0)
    grad_w_gu = dot(a_all, d_gu_t, 0, 1)
    grad_w_o = dot(o_blocks.transpose(1, 0, 2).reshape(head_dim, seq), dh_all, 1, 0)[None]

    mlp_back = exchange(jnp.concatenate([grad_w_gu, part_g_mlp[:, None]], axis=1).reshape(n_dev, rows, 2 * ff_s + 1))
    attn_back = exchange(jnp.concatenate([grad_w_qkv, part_g_attn[:, None]], axis=1).reshape(n_dev, rows, qkv + 1))
    grad_g_mlp = jnp.sum(mlp_back[:, :, 2 * ff_s], axis=0)
    grad_g_attn = jnp.sum(attn_back[:, :, qkv], axis=0)
    mlp_rows = jnp.transpose(mlp_back, (1, 0, 2))
    attn_rows = jnp.transpose(attn_back, (1, 0, 2))
    grad_w_gate = mlp_rows[:, :, :ff_s].reshape(rows, ff)
    grad_w_up = mlp_rows[:, :, ff_s:2 * ff_s].reshape(rows, ff)
    grad_w_q, grad_w_k, grad_w_v = (attn_rows[:, :, i * head_dim:(i + 1) * head_dim] for i in range(3))
    return (y_out, grad_x, grad_g_attn, grad_w_q, grad_w_k, grad_w_v, grad_w_o, grad_g_mlp, grad_w_gate, grad_w_up, grad_w_down)


def solution(mesh):
    n_dev = mesh.shape[SEQ_AXIS]
    token_spec = P(SEQ_AXIS, None)
    cube_spec = P(SEQ_AXIS, None, None)
    gain_spec = P(SEQ_AXIS)
    weight_specs = (gain_spec, cube_spec, cube_spec, cube_spec, cube_spec, gain_spec, token_spec, token_spec, token_spec)
    return jax.shard_map(lambda *args: device_step(n_dev, *args), mesh=mesh, in_specs=(token_spec, gain_spec, token_spec) + weight_specs, out_specs=(token_spec, token_spec) + weight_specs, check_vma=False)
```

```python
import jax
import jax.numpy as jnp
from jax import lax
from jax.experimental import pallas as pl
from jax.experimental.pallas import tpu as pltpu
from jax.sharding import PartitionSpec as P

SEQ_AXIS = 'sp'
RMS_EPS = 1e-5
ROPE_BASE = 10000.0
MASK_VALUE = -1e30
TILE = 512
F32 = jnp.float32
BF16 = jnp.bfloat16


def rms_norm(act_in, gain_vec):
    act_f = act_in.astype(F32)
    inv_rms = lax.rsqrt(jnp.mean(act_f * act_f, axis=-1, keepdims=True) + RMS_EPS)
    return (act_f * inv_rms * gain_vec.astype(F32)).astype(BF16), inv_rms


def rms_norm_bwd(act_in, gain_vec, inv_rms, d_normed):
    act_f = act_in.astype(F32)
    d_f = d_normed.astype(F32)
    scaled_d = d_f * gain_vec.astype(F32)
    proj_mean = jnp.mean(scaled_d * act_f, axis=-1, keepdims=True)
    d_act = inv_rms * scaled_d - act_f * (inv_rms * inv_rms * inv_rms) * proj_mean
    d_gain = jnp.sum(d_f * act_f * inv_rms, axis=0)
    return d_act, d_gain


def dot(lhs, rhs, l_dim, r_dim):
    return lax.dot_general(lhs, rhs, (((l_dim,), (r_dim,)), ((), ())), preferred_element_type=F32)


def gather(shard):
    return lax.all_gather(shard, SEQ_AXIS, axis=0, tiled=True)


def exchange(blocks):
    return lax.all_to_all(blocks, SEQ_AXIS, 0, 0, tiled=True)


def rope_t(vals, cos_tab, sin_tab):
    half = vals.shape[0] // 2
    first, second = vals[:half], vals[half:]
    return jnp.concatenate([first * cos_tab - second * sin_tab, second * cos_tab + first * sin_tab], axis=0)


def mm(lhs, rhs):
    return jnp.dot(lhs, rhs, preferred_element_type=F32)


def diag_mask(tile):
    key_at = lax.broadcasted_iota(jnp.int32, (tile, tile), 0)
    query_at = lax.broadcasted_iota(jnp.int32, (tile, tile), 1)
    return key_at <= query_at


def attn_fwd_kernel(tile, q_t, k_ref, v_t, o_ref, of_ref, lse_ref, s_buf):
    step = pl.program_id(0)
    query = q_t[...]

    def scores(j):
        return mm(k_ref[pl.ds(pl.multiple_of(j * tile, tile), tile), :], query)

    def absorb(j, logits, top, total):
        new_top = jnp.maximum(top, jnp.max(logits, axis=0, keepdims=True))
        s_buf[pl.ds(pl.multiple_of(j * tile, tile), tile), :] = logits
        return new_top, total * jnp.exp(top - new_top) + jnp.sum(jnp.exp(logits - new_top), axis=0, keepdims=True)

    top, total = absorb(step, jnp.where(diag_mask(tile), scores(step), MASK_VALUE), jnp.full((1, tile), MASK_VALUE, F32), jnp.zeros((1, tile), F32))
    top, total = lax.fori_loop(0, step, lambda j, c: absorb(j, scores(j), *c), (top, total))
    lse = top + jnp.log(total)

    def weigh(j, acc):
        at = pl.ds(pl.multiple_of(j * tile, tile), tile)
        prob = jnp.exp(s_buf[at, :] - lse).astype(BF16)
        return acc + mm(v_t[:, at], prob)

    out = lax.fori_loop(0, step + 1, weigh, jnp.zeros((v_t.shape[0], tile), F32))
    of_ref[...] = out
    lse_ref[...] = lse
    block = o_ref.shape[2]
    for part in range(tile // block):
        o_ref[part] = out[:, part * block:(part + 1) * block].astype(BF16)


def attention_fwd(q_t, k_in, v_t, n_blocks):
    head_dim, seq = q_t.shape
    block = seq // n_blocks
    per = TILE // block
    return pl.pallas_call(
        lambda *refs: attn_fwd_kernel(TILE, *refs),
        grid=(seq // TILE,),
        in_specs=[pl.BlockSpec((head_dim, TILE), lambda i: (0, i)), pl.BlockSpec((seq, head_dim), lambda i: (0, 0)), pl.BlockSpec((head_dim, seq), lambda i: (0, 0))],
        out_specs=[pl.BlockSpec((per, head_dim, block), lambda i: (i, 0, 0)), pl.BlockSpec((head_dim, TILE), lambda i: (0, i)), pl.BlockSpec((1, TILE), lambda i: (0, i))],
        out_shape=[jax.ShapeDtypeStruct((n_blocks, head_dim, block), BF16), jax.ShapeDtypeStruct((head_dim, seq), F32), jax.ShapeDtypeStruct((1, seq), F32)],
        scratch_shapes=[pltpu.VMEM((seq, TILE), F32)],
        cost_estimate=pl.CostEstimate(flops=8 * seq * seq * head_dim, bytes_accessed=8 * seq * head_dim, transcendentals=seq * seq),
        name='attn_fwd',
    )(q_t, k_in, v_t)


def attn_bwd_kernel(tile, block, q_t, do_t, of_t, lse_ref, cos_ref, sin_ref, k_ref, k_t, v_ref, cos_all, sin_all, d_blocks, d_proj_t, dq_acc, dk_acc, dv_acc):
    step = pl.program_id(0)
    head_dim = q_t.shape[0]
    query_t, d_out_t = q_t[...], do_t[...]
    lse = lse_ref[...]
    delta = jnp.sum(d_out_t.astype(F32) * of_t[...], axis=0, keepdims=True)

    @pl.when(step == 0)
    def _():
        dk_acc[...] = jnp.zeros_like(dk_acc)
        dv_acc[...] = jnp.zeros_like(dv_acc)

    dq_acc[...] = jnp.zeros_like(dq_acc)

    def visit(j, masked):
        at = pl.ds(pl.multiple_of(j * tile, tile), tile)
        prob = jnp.exp(mm(k_ref[at, :], query_t) - lse)
        if masked:
            prob = jnp.where(diag_mask(tile), prob, 0.0)
        d_prob = mm(v_ref[at, :], d_out_t).astype(BF16).astype(F32)
        d_logits = (prob * (d_prob - delta)).astype(BF16)
        dv_acc[:, at] += dot(d_out_t, prob.astype(BF16), 1, 1)
        dk_acc[:, at] += dot(query_t, d_logits, 1, 1)
        dq_acc[...] += mm(k_t[:, at], d_logits)

    visit(step, True)

    @pl.loop(0, step)
    def _(j):
        visit(j, False)

    def put(row, col_block, values):
        rows = slice(row, row + values.shape[0])
        d_proj_t[rows, pl.ds(pl.multiple_of(col_block * block, block), values.shape[1])] = values
        for part in range(values.shape[1] // block):
            d_blocks[col_block + part, rows, :] = values[:, part * block:(part + 1) * block]

    d_q = (dq_acc[...] * (head_dim ** -0.5)).astype(BF16).astype(F32)
    per = tile // block
    put(0, step * per, rope_t(d_q, cos_ref[...], -sin_ref[...]).astype(BF16))

    @pl.when(step == pl.num_programs(0) - 1)
    def _():
        @pl.loop(0, pl.num_programs(0))
        def _(j):
            at = pl.ds(pl.multiple_of(j * tile, tile), tile)
            put(head_dim, j * per, rope_t(dk_acc[:, at].astype(BF16).astype(F32), cos_all[:, at], -sin_all[:, at]).astype(BF16))
            put(2 * head_dim, j * per, dv_acc[:, at].astype(BF16))


def attention_bwd(q_t, do_t, of_t, lse, k_in, k_t, v_in, cos_t, sin_t, n_blocks):
    head_dim, seq = q_t.shape
    block = seq // n_blocks
    cols = pl.BlockSpec((head_dim, TILE), lambda i: (0, i))
    half_cols = pl.BlockSpec((head_dim // 2, TILE), lambda i: (0, i))
    all_rows = pl.BlockSpec((seq, head_dim), lambda i: (0, 0))
    all_cols = pl.BlockSpec((head_dim, seq), lambda i: (0, 0))
    all_half = pl.BlockSpec((head_dim // 2, seq), lambda i: (0, 0))
    return pl.pallas_call(
        lambda *refs: attn_bwd_kernel(TILE, block, *refs),
        grid=(seq // TILE,),
        in_specs=[cols, cols, cols, pl.BlockSpec((1, TILE), lambda i: (0, i)), half_cols, half_cols, all_rows, all_cols, all_rows, all_half, all_half],
        out_specs=[pl.BlockSpec((n_blocks, 3 * head_dim, block), lambda i: (0, 0, 0)), pl.BlockSpec((3 * head_dim, seq), lambda i: (0, 0))],
        out_shape=[jax.ShapeDtypeStruct((n_blocks, 3 * head_dim, block), BF16), jax.ShapeDtypeStruct((3 * head_dim, seq), BF16)],
        scratch_shapes=[pltpu.VMEM((head_dim, TILE), F32), pltpu.VMEM((head_dim, seq), F32), pltpu.VMEM((head_dim, seq), F32)],
        cost_estimate=pl.CostEstimate(flops=20 * seq * seq * head_dim, bytes_accessed=20 * seq * head_dim, transcendentals=seq * seq),
        name='attn_bwd',
    )(q_t, do_t, of_t, lse, cos_t, sin_t, k_in, k_t, v_in, cos_t, sin_t)


PARTS = ((0, 96), (96, 80), (176, 80))
CORE, CHIP_AXES = 1, (2, 4, 8)


def flip(dev, bit):
    return dev + bit * (1 - 2 * ((dev // bit) % 2))


def start_copy(src, dst, send_sem, recv_sem, peer):
    copy = pltpu.make_async_remote_copy(src_ref=src, dst_ref=dst, send_sem=send_sem, recv_sem=recv_sem, device_id=(peer,), device_id_type=pl.DeviceIdType.MESH)
    copy.start()
    return copy


def landed(ref, sem):
    pltpu.make_async_copy(ref, ref, sem).wait()


def enter_all(me, n_dev):
    barrier = pltpu.get_barrier_semaphore()

    @pl.loop(1, n_dev)
    def _(hop):
        pl.semaphore_signal(barrier, inc=1, device_id=(lax.rem(me + hop, n_dev),), device_id_type=pl.DeviceIdType.MESH)

    pl.semaphore_wait(barrier, n_dev - 1)


class CubeGather:
    def __init__(self, me, buf, send_sem, recv_sem, core_sem):
        self.me, self.buf = me, buf
        self.send_sem, self.recv_sem, self.core_sem = send_sem, recv_sem, core_sem
        self.sent = []

    def part(self, dev, p):
        return self.buf.at[dev, pl.ds(PARTS[p][0], PARTS[p][1])]

    def axes(self, p):
        return [CHIP_AXES[(p + i) % 3] for i in range(3)]

    def owner(self, p, index, start=None):
        dev = self.me if start is None else start
        for i, bit in enumerate(self.axes(p)):
            if (index >> i) & 1:
                dev = flip(dev, bit)
        return dev

    def push(self, p, index, axis):
        ref = self.part(self.owner(p, index), p)
        self.sent.append(start_copy(ref, ref, self.send_sem.at[len(self.sent)], self.recv_sem.at[p, index + (1 << axis)], flip(self.me, self.axes(p)[axis])))

    def push_core(self, p, index):
        ref = self.part(self.owner(p, index), p)
        self.sent.append(start_copy(ref, ref, self.send_sem.at[len(self.sent)], self.core_sem.at[p, index], flip(self.me, CORE)))

    def begin(self):
        for axis in range(3):
            for p in range(3):
                self.push(p, 0, axis)
        for p in range(3):
            self.push_core(p, 0)

    def receive(self, index):
        for p in range(3):
            landed(self.part(self.owner(p, index), p), self.recv_sem.at[p, index])
            for axis in range(index.bit_length(), 3):
                self.push(p, index, axis)
            self.push_core(p, index)

    def receive_core(self, index):
        for p in range(3):
            landed(self.part(self.owner(p, index, flip(self.me, CORE)), p), self.core_sem.at[p, index])

    def finish(self):
        for copy in self.sent:
            copy.wait_send()


N_SENDS = 9 + 12 + 24


def gather_proj_kernel(n_dev, x_ref, small_ref, w_ref, u_out, proj_t, small_all, x_buf, u_buf, w_buf, send_sem, recv_sem, core_sem, misc_send, misc_recv, local_sem, u_sem):
    me = lax.axis_index(SEQ_AXIS)
    own = pltpu.make_async_copy(x_ref, x_buf.at[me], local_sem.at[0])
    own.start()
    own_w = pltpu.make_async_copy(w_ref.at[me], w_buf.at[me], local_sem.at[1])
    own_w.start()
    own_small = pltpu.make_async_copy(small_ref, small_all.at[me], local_sem.at[2])
    own_small.start()
    enter_all(me, n_dev)
    own.wait()
    cube = CubeGather(me, x_buf, send_sem, recv_sem, core_sem)
    cube.begin()

    def spread(hop):
        peer = lax.rem(me + hop, n_dev)
        return [
            pltpu.make_async_remote_copy(src_ref=small_ref, dst_ref=small_all.at[me], send_sem=misc_send.at[0, hop], recv_sem=misc_recv.at[0, me], device_id=(peer,), device_id_type=pl.DeviceIdType.MESH),
            pltpu.make_async_remote_copy(src_ref=w_ref.at[peer], dst_ref=w_buf.at[me], send_sem=misc_send.at[1, hop], recv_sem=misc_recv.at[1, me], device_id=(peer,), device_id_type=pl.DeviceIdType.MESH),
        ]

    for kind in range(2):
        @pl.loop(1, n_dev)
        def _(hop, kind=kind):
            spread(hop)[kind].start()

    cube.receive(1)
    cube.receive(2)
    own_w.wait()
    own_small.wait()

    @pl.loop(1, n_dev)
    def _(hop):
        src = lax.rem(me + hop, n_dev)
        landed(small_all.at[src], misc_recv.at[0, src])
        landed(w_buf.at[src], misc_recv.at[1, src])

    width = x_ref.shape[1]
    tok = x_ref.shape[0]
    rows = w_ref.shape[1]
    gain = jnp.concatenate([small_all[d, 0:1, 0:rows] for d in range(n_dev)], axis=1)
    weight = w_buf[...].reshape(width, w_ref.shape[2])
    keep = proj_t.shape[0]
    flushes = []

    def project(dev):
        act = x_buf[dev].astype(F32)
        inv = lax.rsqrt(jnp.mean(act * act, axis=-1, keepdims=True) + RMS_EPS)
        normed = (act * inv * gain).astype(BF16)
        u_buf[dev] = normed
        proj_t[:, pl.ds(pl.multiple_of(dev * tok, tok), tok)] = mm(normed, weight).T[:keep]
        flush = pltpu.make_async_copy(u_buf.at[dev], u_out.at[dev], u_sem.at[len(flushes)])
        flush.start()
        flushes.append(flush)

    other = flip(me, CORE)
    cube.receive_core(0)
    project(me)
    project(other)
    cube.receive(4)
    cube.receive(3)
    for index in (1, 2, 4):
        cube.receive_core(index)
    for bit in CHIP_AXES:
        project(flip(me, bit))
        project(flip(other, bit))
    cube.receive(5)
    cube.receive(6)
    for index in (3, 5, 6):
        cube.receive_core(index)
    for skip in range(3):
        bits = [bit for i, bit in enumerate(CHIP_AXES) if i != skip]
        project(flip(flip(me, bits[0]), bits[1]))
        project(flip(flip(other, bits[0]), bits[1]))
    cube.receive(7)
    cube.receive_core(7)
    far = flip(flip(flip(me, 2), 4), 8)
    project(far)
    project(flip(far, CORE))

    cube.finish()

    @pl.loop(1, n_dev)
    def _(hop):
        for copy in spread(hop):
            copy.wait_send()

    for flush in flushes:
        flush.wait()


def gather_proj(n_dev, x_act, small, w_blocks, qkv):
    tok, width = x_act.shape
    seq = tok * n_dev
    any_spec = pl.BlockSpec(memory_space=pl.ANY)
    vmem_spec = pl.BlockSpec(memory_space=pltpu.VMEM)
    return pl.pallas_call(
        lambda *refs: gather_proj_kernel(n_dev, *refs),
        in_specs=[any_spec, vmem_spec, vmem_spec],
        out_specs=[any_spec, vmem_spec, vmem_spec],
        out_shape=[jax.ShapeDtypeStruct((n_dev, tok, width), BF16), jax.ShapeDtypeStruct((qkv, seq), F32), jax.ShapeDtypeStruct((n_dev,) + small.shape, F32)],
        scratch_shapes=[
            pltpu.VMEM((n_dev, tok, width), BF16),
            pltpu.VMEM((n_dev, tok, width), BF16),
            pltpu.VMEM(w_blocks.shape, BF16),
            pltpu.SemaphoreType.DMA((N_SENDS,)),
            pltpu.SemaphoreType.DMA((3, 8)),
            pltpu.SemaphoreType.DMA((3, 8)),
            pltpu.SemaphoreType.DMA((2, n_dev)),
            pltpu.SemaphoreType.DMA((2, n_dev)),
            pltpu.SemaphoreType.DMA((3,)),
            pltpu.SemaphoreType.DMA((n_dev,)),
        ],
        compiler_params=pltpu.CompilerParams(collective_id=0, has_side_effects=True),
        cost_estimate=pl.CostEstimate(flops=30 * seq * width * width, bytes_accessed=4 * seq * width, transcendentals=0),
        name='gather_proj',
    )(x_act, small, w_blocks)


def gate_backward(d_mixed, gate_pre, up_pre):
    gate_sig = jax.nn.sigmoid(gate_pre)
    d_up = (d_mixed * gate_pre * gate_sig).astype(BF16)
    d_gate = (d_mixed * up_pre * gate_sig * (1.0 + gate_pre * (1.0 - gate_sig))).astype(BF16)
    return d_gate, d_up


def device_step(n_dev, x_act, positions, grad_out, g_attn_s, w_q, w_k, w_v, w_o, g_mlp_s, w_gate, w_up, w_down):
    tok, width = x_act.shape
    seq = tok * n_dev
    rows, heads, head_dim = w_q.shape
    ff = w_gate.shape[1]
    ff_s = ff // n_dev
    qkv = 3 * head_dim

    small = jnp.concatenate([jnp.concatenate([g_attn_s, g_mlp_s]).astype(F32)[None], positions.astype(F32).reshape(-1, 2 * rows)], axis=0)
    small = jnp.pad(small, ((0, 8 - small.shape[0]), (0, 0)))
    w_qkv = jnp.concatenate([w_q, w_k, w_v], axis=2)
    w_blocks = jnp.pad(jnp.transpose(w_qkv, (1, 0, 2)), ((0, 0), (0, 0), (0, 256 - qkv)))
    u_all, proj_t, small_all = gather_proj(n_dev, x_act, small, w_blocks, qkv)
    u_all = u_all.reshape(seq, width)
    g_attn = small_all[:, 0, :rows].reshape(width)
    g_mlp = small_all[:, 0, rows:2 * rows].reshape(width)
    pos_all = small_all[:, 1:1 + tok // (2 * rows)]

    down_groups = [w_down[i:i + rows] for i in range(0, ff_s, rows)]
    down_groups = [jnp.pad(group, ((0, rows - group.shape[0]), (0, 0))) for group in down_groups]
    w_all = gather(jnp.concatenate([w_gate, w_up, w_o[0]] + down_groups + [w_qkv.reshape(rows, heads * qkv)], axis=1))
    w_gu = w_all[:, :2 * ff]
    w_o_all = w_all[:, 2 * ff:2 * ff + width]
    w_down_at = 2 * ff + width
    down_all = [w_all[:, w_down_at + i * width:w_down_at + (i + 1) * width].reshape(n_dev, rows, width) for i in range(len(down_groups))]
    w_down_all = jnp.concatenate(down_all, axis=1)[:, :ff_s].reshape(ff, width)
    w_qkv_all = w_all[:, w_down_at + len(down_groups) * width:]
    me = lax.axis_index(SEQ_AXIS)
    w_cols = jnp.concatenate([lax.dynamic_slice(w_all, (0, at + me * ff_s), (width, ff_s)) for at in (0, ff)], axis=1)

    half = head_dim // 2
    inv_freq = ROPE_BASE ** (-(jnp.arange(half, dtype=F32) * (2.0 / head_dim)))
    angle_t = inv_freq[:, None] * pos_all.reshape(1, seq)
    cos_t, sin_t = jnp.cos(angle_t), jnp.sin(angle_t)

    q_t = (rope_t(proj_t[:head_dim], cos_t, sin_t).astype(BF16).astype(F32) * (head_dim ** -0.5)).astype(BF16)
    k_t = rope_t(proj_t[head_dim:2 * head_dim], cos_t, sin_t).astype(BF16)
    v_t = proj_t[2 * head_dim:].astype(BF16)
    k_in, v_in = k_t.T, v_t.T
    o_blocks, of_t, lse = attention_fwd(q_t, k_in, v_t, n_dev)
    o_loc = exchange(o_blocks).reshape(width, tok)

    hidden = (x_act.astype(F32) + dot(o_loc, w_o_all, 0, 0)).astype(BF16)
    normed_mlp, inv_rms_mlp = rms_norm(hidden, g_mlp)
    a_dy = gather(jnp.concatenate([normed_mlp, grad_out], axis=1))
    pre = dot(normed_mlp, w_gu, 1, 0)
    gate_pre, up_pre = pre[:, :ff], pre[:, ff:]
    mixed = (jax.nn.silu(gate_pre) * up_pre).astype(BF16)
    y_out = (hidden.astype(F32) + dot(mixed, w_down_all, 1, 0)).astype(BF16)

    d_mixed = dot(grad_out, w_down_all, 1, 1).astype(BF16).astype(F32)
    d_gu = jnp.concatenate(gate_backward(d_mixed, gate_pre, up_pre), axis=1)
    d_normed = dot(d_gu, w_gu, 1, 1).astype(BF16)
    d_hid_norm, part_g_mlp = rms_norm_bwd(hidden, g_mlp, inv_rms_mlp, d_normed)
    d_hidden = (grad_out.astype(F32) + d_hid_norm).astype(BF16)
    do_blocks = exchange(dot(w_o_all, d_hidden, 1, 1).astype(BF16).reshape(n_dev, head_dim, tok))
    dh_all = gather(d_hidden)

    do_t = jnp.transpose(do_blocks, (1, 0, 2)).reshape(head_dim, seq)
    d_blocks, d_proj_t = attention_bwd(q_t, do_t, of_t, lse, k_in, k_t, v_in, cos_t, sin_t, n_dev)
    d_proj = exchange(d_blocks)

    a_dy, d_proj_t = lax.optimization_barrier((a_dy, d_proj_t))
    a_all, dy_all = a_dy[:, :width], a_dy[:, width:]
    pre_t = dot(w_cols, a_all, 0, 1)
    gate_t, up_t = pre_t[:ff_s], pre_t[ff_s:]
    d_mixed_t = dot(w_down, dy_all, 1, 1).astype(BF16).astype(F32)
    mixed_t = (jax.nn.silu(gate_t) * up_t).astype(BF16)
    d_gu_t = jnp.concatenate(gate_backward(d_mixed_t, gate_t, up_t), axis=0)
    grad_w_down = dot(mixed_t, dy_all, 1, 0)
    grad_w_gu = dot(a_all, d_gu_t, 0, 1)
    mlp_back = exchange(jnp.concatenate([grad_w_gu, part_g_mlp[:, None]], axis=1).reshape(n_dev, rows, 2 * ff_s + 1))

    d_proj, grad_w_down, d_proj_t = lax.optimization_barrier((d_proj, grad_w_down, d_proj_t))
    d_proj = d_proj.reshape(heads * qkv, tok)
    grad_w_qkv = lax.optimization_barrier(dot(d_proj_t, u_all, 1, 0)).T
    inv_rms = lax.rsqrt(jnp.mean(jnp.square(x_act.astype(F32)), axis=-1, keepdims=True) + RMS_EPS)
    d_u = dot(d_proj, w_qkv_all, 0, 1).astype(BF16)
    d_x_norm, part_g_attn = rms_norm_bwd(x_act, g_attn, inv_rms, d_u)
    grad_x = (d_hidden.astype(F32) + d_x_norm).astype(BF16)
    attn_back = exchange(jnp.concatenate([grad_w_qkv, part_g_attn[:, None]], axis=1).reshape(n_dev, rows, qkv + 1))
    dh_all, grad_x = lax.optimization_barrier((dh_all, grad_x))
    grad_w_o = dot(o_blocks.transpose(1, 0, 2).reshape(head_dim, seq), dh_all, 1, 0)[None]
    grad_g_mlp = jnp.sum(mlp_back[:, :, 2 * ff_s], axis=0)
    grad_g_attn = jnp.sum(attn_back[:, :, qkv], axis=0)
    mlp_rows = jnp.transpose(mlp_back, (1, 0, 2))
    attn_rows = jnp.transpose(attn_back, (1, 0, 2))
    grad_w_gate = mlp_rows[:, :, :ff_s].reshape(rows, ff)
    grad_w_up = mlp_rows[:, :, ff_s:2 * ff_s].reshape(rows, ff)
    grad_w_q, grad_w_k, grad_w_v = (attn_rows[:, :, i * head_dim:(i + 1) * head_dim] for i in range(3))
    return (y_out, grad_x, grad_g_attn, grad_w_q, grad_w_k, grad_w_v, grad_w_o, grad_g_mlp, grad_w_gate, grad_w_up, grad_w_down)


def solution(mesh):
    n_dev = mesh.shape[SEQ_AXIS]
    token_spec = P(SEQ_AXIS, None)
    cube_spec = P(SEQ_AXIS, None, None)
    gain_spec = P(SEQ_AXIS)
    weight_specs = (gain_spec, cube_spec, cube_spec, cube_spec, cube_spec, gain_spec, token_spec, token_spec, token_spec)
    return jax.shard_map(lambda *args: device_step(n_dev, *args), mesh=mesh, in_specs=(token_spec, gain_spec, token_spec) + weight_specs, out_specs=(token_spec, token_spec) + weight_specs, check_vma=False)
```

```python
import jax
import jax.numpy as jnp
from jax import lax
from jax.experimental import pallas as pl
from jax.experimental.pallas import tpu as pltpu
from jax.sharding import PartitionSpec as P

SEQ_AXIS = 'sp'
RMS_EPS = 1e-5
ROPE_BASE = 10000.0
MASK_VALUE = -1e30
TILE = 512
F32 = jnp.float32
BF16 = jnp.bfloat16


def rms_norm(act_in, gain_vec):
    act_f = act_in.astype(F32)
    inv_rms = lax.rsqrt(jnp.mean(act_f * act_f, axis=-1, keepdims=True) + RMS_EPS)
    return (act_f * inv_rms * gain_vec.astype(F32)).astype(BF16), inv_rms


def rms_norm_bwd(act_in, gain_vec, inv_rms, d_normed):
    act_f = act_in.astype(F32)
    d_f = d_normed.astype(F32)
    scaled_d = d_f * gain_vec.astype(F32)
    proj_mean = jnp.mean(scaled_d * act_f, axis=-1, keepdims=True)
    d_act = inv_rms * scaled_d - act_f * (inv_rms * inv_rms * inv_rms) * proj_mean
    d_gain = jnp.sum(d_f * act_f * inv_rms, axis=0)
    return d_act, d_gain


def dot(lhs, rhs, l_dim, r_dim):
    return lax.dot_general(lhs, rhs, (((l_dim,), (r_dim,)), ((), ())), preferred_element_type=F32)


def gather(shard):
    return lax.all_gather(shard, SEQ_AXIS, axis=0, tiled=True)


def exchange(blocks):
    return lax.all_to_all(blocks, SEQ_AXIS, 0, 0, tiled=True)


def rope_t(vals, cos_tab, sin_tab):
    half = vals.shape[0] // 2
    first, second = vals[:half], vals[half:]
    return jnp.concatenate([first * cos_tab - second * sin_tab, second * cos_tab + first * sin_tab], axis=0)


def mm(lhs, rhs):
    return jnp.dot(lhs, rhs, preferred_element_type=F32)


def diag_mask(tile):
    key_at = lax.broadcasted_iota(jnp.int32, (tile, tile), 0)
    query_at = lax.broadcasted_iota(jnp.int32, (tile, tile), 1)
    return key_at <= query_at


def attn_fwd_kernel(tile, q_t, k_ref, v_t, o_ref, of_ref, lse_ref, s_buf):
    step = pl.program_id(0)
    query = q_t[...]

    def scores(j):
        return mm(k_ref[pl.ds(pl.multiple_of(j * tile, tile), tile), :], query)

    def absorb(j, logits, top, total):
        new_top = jnp.maximum(top, jnp.max(logits, axis=0, keepdims=True))
        s_buf[pl.ds(pl.multiple_of(j * tile, tile), tile), :] = logits
        return new_top, total * jnp.exp(top - new_top) + jnp.sum(jnp.exp(logits - new_top), axis=0, keepdims=True)

    top, total = absorb(step, jnp.where(diag_mask(tile), scores(step), MASK_VALUE), jnp.full((1, tile), MASK_VALUE, F32), jnp.zeros((1, tile), F32))
    top, total = lax.fori_loop(0, step, lambda j, c: absorb(j, scores(j), *c), (top, total))
    lse = top + jnp.log(total)

    def weigh(j, acc):
        at = pl.ds(pl.multiple_of(j * tile, tile), tile)
        prob = jnp.exp(s_buf[at, :] - lse).astype(BF16)
        return acc + mm(v_t[:, at], prob)

    out = lax.fori_loop(0, step + 1, weigh, jnp.zeros((v_t.shape[0], tile), F32))
    of_ref[...] = out
    lse_ref[...] = lse
    block = o_ref.shape[2]
    for part in range(tile // block):
        o_ref[part] = out[:, part * block:(part + 1) * block].astype(BF16)


def attention_fwd(q_t, k_in, v_t, n_blocks):
    head_dim, seq = q_t.shape
    block = seq // n_blocks
    per = TILE // block
    return pl.pallas_call(
        lambda *refs: attn_fwd_kernel(TILE, *refs),
        grid=(seq // TILE,),
        in_specs=[pl.BlockSpec((head_dim, TILE), lambda i: (0, i)), pl.BlockSpec((seq, head_dim), lambda i: (0, 0)), pl.BlockSpec((head_dim, seq), lambda i: (0, 0))],
        out_specs=[pl.BlockSpec((per, head_dim, block), lambda i: (i, 0, 0)), pl.BlockSpec((head_dim, TILE), lambda i: (0, i)), pl.BlockSpec((1, TILE), lambda i: (0, i))],
        out_shape=[jax.ShapeDtypeStruct((n_blocks, head_dim, block), BF16), jax.ShapeDtypeStruct((head_dim, seq), F32), jax.ShapeDtypeStruct((1, seq), F32)],
        scratch_shapes=[pltpu.VMEM((seq, TILE), F32)],
        cost_estimate=pl.CostEstimate(flops=8 * seq * seq * head_dim, bytes_accessed=8 * seq * head_dim, transcendentals=seq * seq),
        name='attn_fwd',
    )(q_t, k_in, v_t)


def attn_bwd_kernel(tile, block, q_t, do_t, of_t, lse_ref, cos_ref, sin_ref, k_ref, k_t, v_ref, cos_all, sin_all, d_blocks, d_proj_t, dq_acc, dk_acc, dv_acc):
    step = pl.program_id(0)
    head_dim = q_t.shape[0]
    query_t, d_out_t = q_t[...], do_t[...]
    lse = lse_ref[...]
    delta = jnp.sum(d_out_t.astype(F32) * of_t[...], axis=0, keepdims=True)

    @pl.when(step == 0)
    def _():
        dk_acc[...] = jnp.zeros_like(dk_acc)
        dv_acc[...] = jnp.zeros_like(dv_acc)

    dq_acc[...] = jnp.zeros_like(dq_acc)

    def visit(j, masked):
        at = pl.ds(pl.multiple_of(j * tile, tile), tile)
        prob = jnp.exp(mm(k_ref[at, :], query_t) - lse)
        if masked:
            prob = jnp.where(diag_mask(tile), prob, 0.0)
        d_prob = mm(v_ref[at, :], d_out_t).astype(BF16).astype(F32)
        d_logits = (prob * (d_prob - delta)).astype(BF16)
        dv_acc[:, at] += dot(d_out_t, prob.astype(BF16), 1, 1)
        dk_acc[:, at] += dot(query_t, d_logits, 1, 1)
        dq_acc[...] += mm(k_t[:, at], d_logits)

    visit(step, True)

    @pl.loop(0, step)
    def _(j):
        visit(j, False)

    def put(row, col_block, values):
        rows = slice(row, row + values.shape[0])
        d_proj_t[rows, pl.ds(pl.multiple_of(col_block * block, block), values.shape[1])] = values
        for part in range(values.shape[1] // block):
            d_blocks[col_block + part, rows, :] = values[:, part * block:(part + 1) * block]

    d_q = (dq_acc[...] * (head_dim ** -0.5)).astype(BF16).astype(F32)
    per = tile // block
    put(0, step * per, rope_t(d_q, cos_ref[...], -sin_ref[...]).astype(BF16))

    @pl.when(step == pl.num_programs(0) - 1)
    def _():
        @pl.loop(0, pl.num_programs(0))
        def _(j):
            at = pl.ds(pl.multiple_of(j * tile, tile), tile)
            put(head_dim, j * per, rope_t(dk_acc[:, at].astype(BF16).astype(F32), cos_all[:, at], -sin_all[:, at]).astype(BF16))
            put(2 * head_dim, j * per, dv_acc[:, at].astype(BF16))


def attention_bwd(q_t, do_t, of_t, lse, k_in, k_t, v_in, cos_t, sin_t, n_blocks):
    head_dim, seq = q_t.shape
    block = seq // n_blocks
    cols = pl.BlockSpec((head_dim, TILE), lambda i: (0, i))
    half_cols = pl.BlockSpec((head_dim // 2, TILE), lambda i: (0, i))
    all_rows = pl.BlockSpec((seq, head_dim), lambda i: (0, 0))
    all_cols = pl.BlockSpec((head_dim, seq), lambda i: (0, 0))
    all_half = pl.BlockSpec((head_dim // 2, seq), lambda i: (0, 0))
    return pl.pallas_call(
        lambda *refs: attn_bwd_kernel(TILE, block, *refs),
        grid=(seq // TILE,),
        in_specs=[cols, cols, cols, pl.BlockSpec((1, TILE), lambda i: (0, i)), half_cols, half_cols, all_rows, all_cols, all_rows, all_half, all_half],
        out_specs=[pl.BlockSpec((n_blocks, 3 * head_dim, block), lambda i: (0, 0, 0)), pl.BlockSpec((3 * head_dim, seq), lambda i: (0, 0))],
        out_shape=[jax.ShapeDtypeStruct((n_blocks, 3 * head_dim, block), BF16), jax.ShapeDtypeStruct((3 * head_dim, seq), BF16)],
        scratch_shapes=[pltpu.VMEM((head_dim, TILE), F32), pltpu.VMEM((head_dim, seq), F32), pltpu.VMEM((head_dim, seq), F32)],
        cost_estimate=pl.CostEstimate(flops=20 * seq * seq * head_dim, bytes_accessed=20 * seq * head_dim, transcendentals=seq * seq),
        name='attn_bwd',
    )(q_t, do_t, of_t, lse, cos_t, sin_t, k_in, k_t, v_in, cos_t, sin_t)


PARTS = ((0, 96), (96, 80), (176, 80))
CORE, CHIP_AXES = 1, (2, 4, 8)


def flip(dev, bit):
    return dev + bit * (1 - 2 * ((dev // bit) % 2))


def start_copy(src, dst, send_sem, recv_sem, peer):
    copy = pltpu.make_async_remote_copy(src_ref=src, dst_ref=dst, send_sem=send_sem, recv_sem=recv_sem, device_id=(peer,), device_id_type=pl.DeviceIdType.MESH)
    copy.start()
    return copy


def landed(ref, sem):
    pltpu.make_async_copy(ref, ref, sem).wait()


def enter_all(me, n_dev):
    barrier = pltpu.get_barrier_semaphore()

    @pl.loop(1, n_dev)
    def _(hop):
        pl.semaphore_signal(barrier, inc=1, device_id=(lax.rem(me + hop, n_dev),), device_id_type=pl.DeviceIdType.MESH)

    pl.semaphore_wait(barrier, n_dev - 1)


class CubeGather:
    def __init__(self, me, buf, send_sem, recv_sem, core_sem):
        self.me, self.buf = me, buf
        self.send_sem, self.recv_sem, self.core_sem = send_sem, recv_sem, core_sem
        self.sent = []

    def part(self, dev, p):
        return self.buf.at[dev, pl.ds(PARTS[p][0], PARTS[p][1])]

    def axes(self, p):
        return [CHIP_AXES[(p + i) % 3] for i in range(3)]

    def owner(self, p, index, start=None):
        dev = self.me if start is None else start
        for i, bit in enumerate(self.axes(p)):
            if (index >> i) & 1:
                dev = flip(dev, bit)
        return dev

    def push(self, p, index, axis):
        ref = self.part(self.owner(p, index), p)
        self.sent.append(start_copy(ref, ref, self.send_sem.at[len(self.sent)], self.recv_sem.at[p, index + (1 << axis)], flip(self.me, self.axes(p)[axis])))

    def push_core(self, p, index):
        ref = self.part(self.owner(p, index), p)
        self.sent.append(start_copy(ref, ref, self.send_sem.at[len(self.sent)], self.core_sem.at[p, index], flip(self.me, CORE)))

    def begin(self):
        for axis in range(3):
            for p in range(3):
                self.push(p, 0, axis)
        for p in range(3):
            self.push_core(p, 0)

    def receive(self, index):
        for p in range(3):
            landed(self.part(self.owner(p, index), p), self.recv_sem.at[p, index])
            for axis in range(index.bit_length(), 3):
                self.push(p, index, axis)
            self.push_core(p, index)

    def receive_core(self, index):
        for p in range(3):
            landed(self.part(self.owner(p, index, flip(self.me, CORE)), p), self.core_sem.at[p, index])

    def finish(self):
        for copy in self.sent:
            copy.wait_send()


N_SENDS = 9 + 12 + 24


def gather_proj_kernel(n_dev, x_ref, small_ref, w_ref, u_out, proj_t, small_all, x_buf, u_buf, w_buf, send_sem, recv_sem, core_sem, misc_send, misc_recv, local_sem, u_sem):
    me = lax.axis_index(SEQ_AXIS)
    own = pltpu.make_async_copy(x_ref, x_buf.at[me], local_sem.at[0])
    own.start()
    own_w = pltpu.make_async_copy(w_ref.at[me], w_buf.at[me], local_sem.at[1])
    own_w.start()
    own_small = pltpu.make_async_copy(small_ref, small_all.at[me], local_sem.at[2])
    own_small.start()
    enter_all(me, n_dev)
    own.wait()
    cube = CubeGather(me, x_buf, send_sem, recv_sem, core_sem)
    cube.begin()

    def spread(hop):
        peer = lax.rem(me + hop, n_dev)
        return [
            pltpu.make_async_remote_copy(src_ref=small_ref, dst_ref=small_all.at[me], send_sem=misc_send.at[0, hop], recv_sem=misc_recv.at[0, me], device_id=(peer,), device_id_type=pl.DeviceIdType.MESH),
            pltpu.make_async_remote_copy(src_ref=w_ref.at[peer], dst_ref=w_buf.at[me], send_sem=misc_send.at[1, hop], recv_sem=misc_recv.at[1, me], device_id=(peer,), device_id_type=pl.DeviceIdType.MESH),
        ]

    for kind in range(2):
        @pl.loop(1, n_dev)
        def _(hop, kind=kind):
            spread(hop)[kind].start()

    cube.receive(1)
    cube.receive(2)
    own_w.wait()
    own_small.wait()

    @pl.loop(1, n_dev)
    def _(hop):
        src = lax.rem(me + hop, n_dev)
        landed(small_all.at[src], misc_recv.at[0, src])
        landed(w_buf.at[src], misc_recv.at[1, src])

    width = x_ref.shape[1]
    tok = x_ref.shape[0]
    rows = w_ref.shape[1]
    gain = jnp.concatenate([small_all[d, 0:1, 0:rows] for d in range(n_dev)], axis=1)
    weight = w_buf[...].reshape(width, w_ref.shape[2])
    keep = proj_t.shape[0]
    flushes = []

    def project(dev):
        act = x_buf[dev].astype(F32)
        inv = lax.rsqrt(jnp.mean(act * act, axis=-1, keepdims=True) + RMS_EPS)
        normed = (act * inv * gain).astype(BF16)
        u_buf[dev] = normed
        proj_t[:, pl.ds(pl.multiple_of(dev * tok, tok), tok)] = mm(normed, weight).T[:keep]
        flush = pltpu.make_async_copy(u_buf.at[dev], u_out.at[dev], u_sem.at[len(flushes)])
        flush.start()
        flushes.append(flush)

    other = flip(me, CORE)
    cube.receive_core(0)
    project(me)
    project(other)
    cube.receive(4)
    cube.receive(3)
    for index in (1, 2, 4):
        cube.receive_core(index)
    for bit in CHIP_AXES:
        project(flip(me, bit))
        project(flip(other, bit))
    cube.receive(5)
    cube.receive(6)
    for index in (3, 5, 6):
        cube.receive_core(index)
    for skip in range(3):
        bits = [bit for i, bit in enumerate(CHIP_AXES) if i != skip]
        project(flip(flip(me, bits[0]), bits[1]))
        project(flip(flip(other, bits[0]), bits[1]))
    cube.receive(7)
    cube.receive_core(7)
    far = flip(flip(flip(me, 2), 4), 8)
    project(far)
    project(flip(far, CORE))

    cube.finish()

    @pl.loop(1, n_dev)
    def _(hop):
        for copy in spread(hop):
            copy.wait_send()

    for flush in flushes:
        flush.wait()


def gather_proj(n_dev, x_act, small, w_blocks, qkv):
    tok, width = x_act.shape
    seq = tok * n_dev
    any_spec = pl.BlockSpec(memory_space=pl.ANY)
    vmem_spec = pl.BlockSpec(memory_space=pltpu.VMEM)
    return pl.pallas_call(
        lambda *refs: gather_proj_kernel(n_dev, *refs),
        in_specs=[any_spec, vmem_spec, vmem_spec],
        out_specs=[any_spec, vmem_spec, vmem_spec],
        out_shape=[jax.ShapeDtypeStruct((n_dev, tok, width), BF16), jax.ShapeDtypeStruct((qkv, seq), F32), jax.ShapeDtypeStruct((n_dev,) + small.shape, F32)],
        scratch_shapes=[
            pltpu.VMEM((n_dev, tok, width), BF16),
            pltpu.VMEM((n_dev, tok, width), BF16),
            pltpu.VMEM(w_blocks.shape, BF16),
            pltpu.SemaphoreType.DMA((N_SENDS,)),
            pltpu.SemaphoreType.DMA((3, 8)),
            pltpu.SemaphoreType.DMA((3, 8)),
            pltpu.SemaphoreType.DMA((2, n_dev)),
            pltpu.SemaphoreType.DMA((2, n_dev)),
            pltpu.SemaphoreType.DMA((3,)),
            pltpu.SemaphoreType.DMA((n_dev,)),
        ],
        compiler_params=pltpu.CompilerParams(collective_id=0, has_side_effects=True),
        cost_estimate=pl.CostEstimate(flops=30 * seq * width * width, bytes_accessed=4 * seq * width, transcendentals=0),
        name='gather_proj',
    )(x_act, small, w_blocks)


def gate_backward(d_mixed, gate_pre, up_pre):
    gate_sig = jax.nn.sigmoid(gate_pre)
    d_up = (d_mixed * gate_pre * gate_sig).astype(BF16)
    d_gate = (d_mixed * up_pre * gate_sig * (1.0 + gate_pre * (1.0 - gate_sig))).astype(BF16)
    return d_gate, d_up


def join_columns_kernel(size, src, first, second):
    for i, out in enumerate((first, second)):
        out[...] = jnp.concatenate([src[d, :, i * size:(i + 1) * size] for d in range(src.shape[0])], axis=1)


def join_columns(blocks, size):
    shape = jax.ShapeDtypeStruct((blocks.shape[1], blocks.shape[0] * size), F32)
    return pl.pallas_call(lambda *refs: join_columns_kernel(size, *refs), out_shape=[shape, shape], name='join_columns')(blocks)


def split_heads_kernel(head_dim, src, *outs):
    for i, out in enumerate(outs):
        for d in range(src.shape[0]):
            out[:, d, :] = src[d, :, i * head_dim:(i + 1) * head_dim]


def split_heads(blocks, head_dim):
    shape = jax.ShapeDtypeStruct((blocks.shape[1], blocks.shape[0], head_dim), F32)
    return pl.pallas_call(lambda *refs: split_heads_kernel(head_dim, *refs), out_shape=[shape] * 3, name='split_heads')(blocks)


def device_step(n_dev, x_act, positions, grad_out, g_attn_s, w_q, w_k, w_v, w_o, g_mlp_s, w_gate, w_up, w_down):
    tok, width = x_act.shape
    seq = tok * n_dev
    rows, heads, head_dim = w_q.shape
    ff = w_gate.shape[1]
    ff_s = ff // n_dev
    qkv = 3 * head_dim

    small = jnp.concatenate([jnp.concatenate([g_attn_s, g_mlp_s]).astype(F32)[None], positions.astype(F32).reshape(-1, 2 * rows)], axis=0)
    small = jnp.pad(small, ((0, 8 - small.shape[0]), (0, 0)))
    w_qkv = jnp.concatenate([w_q, w_k, w_v], axis=2)
    w_blocks = jnp.pad(jnp.transpose(w_qkv, (1, 0, 2)), ((0, 0), (0, 0), (0, 256 - qkv)))
    u_all, proj_t, small_all = gather_proj(n_dev, x_act, small, w_blocks, qkv)
    u_all = u_all.reshape(seq, width)
    g_attn = small_all[:, 0, :rows].reshape(width)
    g_mlp = small_all[:, 0, rows:2 * rows].reshape(width)
    pos_all = small_all[:, 1:1 + tok // (2 * rows)]

    down_groups = [w_down[i:i + rows] for i in range(0, ff_s, rows)]
    down_groups = [jnp.pad(group, ((0, rows - group.shape[0]), (0, 0))) for group in down_groups]
    w_all = gather(jnp.concatenate([w_gate, w_up, w_o[0]] + down_groups + [w_qkv.reshape(rows, heads * qkv)], axis=1))
    w_gu = w_all[:, :2 * ff]
    w_o_all = w_all[:, 2 * ff:2 * ff + width]
    w_down_at = 2 * ff + width
    down_all = [w_all[:, w_down_at + i * width:w_down_at + (i + 1) * width].reshape(n_dev, rows, width) for i in range(len(down_groups))]
    w_down_all = jnp.concatenate(down_all, axis=1)[:, :ff_s].reshape(ff, width)
    w_qkv_all = w_all[:, w_down_at + len(down_groups) * width:]
    me = lax.axis_index(SEQ_AXIS)
    w_cols = jnp.concatenate([lax.dynamic_slice(w_all, (0, at + me * ff_s), (width, ff_s)) for at in (0, ff)], axis=1)

    half = head_dim // 2
    inv_freq = ROPE_BASE ** (-(jnp.arange(half, dtype=F32) * (2.0 / head_dim)))
    angle_t = inv_freq[:, None] * pos_all.reshape(1, seq)
    cos_t, sin_t = jnp.cos(angle_t), jnp.sin(angle_t)

    q_t = (rope_t(proj_t[:head_dim], cos_t, sin_t).astype(BF16).astype(F32) * (head_dim ** -0.5)).astype(BF16)
    k_t = rope_t(proj_t[head_dim:2 * head_dim], cos_t, sin_t).astype(BF16)
    v_t = proj_t[2 * head_dim:].astype(BF16)
    k_in, v_in = k_t.T, v_t.T
    o_blocks, of_t, lse = attention_fwd(q_t, k_in, v_t, n_dev)
    o_loc = exchange(o_blocks).reshape(width, tok)

    hidden = (x_act.astype(F32) + dot(o_loc, w_o_all, 0, 0)).astype(BF16)
    normed_mlp, inv_rms_mlp = rms_norm(hidden, g_mlp)
    a_dy = gather(jnp.concatenate([normed_mlp, grad_out], axis=1))
    pre = dot(normed_mlp, w_gu, 1, 0)
    gate_pre, up_pre = pre[:, :ff], pre[:, ff:]
    mixed = (jax.nn.silu(gate_pre) * up_pre).astype(BF16)
    y_out = (hidden.astype(F32) + dot(mixed, w_down_all, 1, 0)).astype(BF16)

    d_mixed = dot(grad_out, w_down_all, 1, 1).astype(BF16).astype(F32)
    d_gu = jnp.concatenate(gate_backward(d_mixed, gate_pre, up_pre), axis=1)
    d_normed = dot(d_gu, w_gu, 1, 1).astype(BF16)
    d_hid_norm, part_g_mlp = rms_norm_bwd(hidden, g_mlp, inv_rms_mlp, d_normed)
    d_hidden = (grad_out.astype(F32) + d_hid_norm).astype(BF16)
    do_blocks = exchange(dot(w_o_all, d_hidden, 1, 1).astype(BF16).reshape(n_dev, head_dim, tok))
    half_n = n_dev // 2
    pairs = [(i, (i + half_n) % n_dev) for i in range(n_dev)]
    near = (me // half_n) * half_n
    o_far = lax.ppermute(lax.dynamic_slice_in_dim(o_blocks, half_n - near, half_n), SEQ_AXIS, pairs)
    o_pair = jnp.concatenate([lax.dynamic_slice_in_dim(o_blocks, near, half_n), o_far], axis=1)
    dh_half = lax.all_gather(d_hidden, SEQ_AXIS, axis=0, tiled=True, axis_index_groups=[list(range(half_n)), list(range(half_n, n_dev))])

    do_t = jnp.transpose(do_blocks, (1, 0, 2)).reshape(head_dim, seq)
    d_blocks, d_proj_t = attention_bwd(q_t, do_t, of_t, lse, k_in, k_t, v_in, cos_t, sin_t, n_dev)
    d_proj = exchange(d_blocks)

    a_dy, d_proj_t = lax.optimization_barrier((a_dy, d_proj_t))
    a_all, dy_all = a_dy[:, :width], a_dy[:, width:]
    pre_t = dot(w_cols, a_all, 0, 1)
    gate_t, up_t = pre_t[:ff_s], pre_t[ff_s:]
    d_mixed_t = dot(w_down, dy_all, 1, 1).astype(BF16).astype(F32)
    mixed_t = (jax.nn.silu(gate_t) * up_t).astype(BF16)
    d_gu_t = jnp.concatenate(gate_backward(d_mixed_t, gate_t, up_t), axis=0)
    grad_w_down = dot(mixed_t, dy_all, 1, 0)
    grad_w_gu = dot(a_all, d_gu_t, 0, 1)
    mlp_send = jnp.concatenate([grad_w_gu, part_g_mlp[:, None]], axis=1).reshape(n_dev, rows, 2 * ff_s + 1)
    d_proj, grad_w_down, d_proj_t, mlp_send = lax.optimization_barrier((d_proj, grad_w_down, d_proj_t, mlp_send))
    mlp_back = exchange(mlp_send)
    d_proj = d_proj.reshape(heads * qkv, tok)
    grad_w_qkv = lax.optimization_barrier(dot(d_proj_t, u_all, 1, 0)).T
    inv_rms = lax.rsqrt(jnp.mean(jnp.square(x_act.astype(F32)), axis=-1, keepdims=True) + RMS_EPS)
    d_u = dot(d_proj, w_qkv_all, 0, 1).astype(BF16)
    d_x_norm, part_g_attn = rms_norm_bwd(x_act, g_attn, inv_rms, d_u)
    grad_x = (d_hidden.astype(F32) + d_x_norm).astype(BF16)
    attn_send = jnp.concatenate([grad_w_qkv, part_g_attn[:, None]], axis=1).reshape(n_dev, rows, qkv + 1)
    mlp_back, attn_send = lax.optimization_barrier((mlp_back, attn_send))
    attn_back = exchange(attn_send)
    dh_half, grad_x = lax.optimization_barrier((dh_half, grad_x))
    part_w_o = dot(o_pair.transpose(1, 0, 2).reshape(2 * head_dim, seq // 2), dh_half, 1, 0)
    grad_w_o = (part_w_o[:head_dim] + lax.ppermute(part_w_o[head_dim:], SEQ_AXIS, pairs))[None]

    grad_g_mlp = jnp.sum(mlp_back[:, :, 2 * ff_s], axis=0)
    grad_g_attn = jnp.sum(attn_back[:, :, qkv], axis=0)
    grad_w_gate, grad_w_up = join_columns(mlp_back, ff_s)
    grad_w_q, grad_w_k, grad_w_v = split_heads(attn_back, head_dim)
    return (y_out, grad_x, grad_g_attn, grad_w_q, grad_w_k, grad_w_v, grad_w_o, grad_g_mlp, grad_w_gate, grad_w_up, grad_w_down)


def solution(mesh):
    n_dev = mesh.shape[SEQ_AXIS]
    token_spec = P(SEQ_AXIS, None)
    cube_spec = P(SEQ_AXIS, None, None)
    gain_spec = P(SEQ_AXIS)
    weight_specs = (gain_spec, cube_spec, cube_spec, cube_spec, cube_spec, gain_spec, token_spec, token_spec, token_spec)
    return jax.shard_map(lambda *args: device_step(n_dev, *args), mesh=mesh, in_specs=(token_spec, gain_spec, token_spec) + weight_specs, out_specs=(token_spec, token_spec) + weight_specs, check_vma=False)
```

```python
import jax
import jax.numpy as jnp
from jax import lax
from jax.experimental import pallas as pl
from jax.experimental.pallas import tpu as pltpu
from jax.sharding import PartitionSpec as P

SEQ_AXIS = 'sp'
RMS_EPS = 1e-5
ROPE_BASE = 10000.0
MASK_VALUE = -1e30
TILE = 512
F32 = jnp.float32
BF16 = jnp.bfloat16


def rms_norm(act_in, gain_vec):
    act_f = act_in.astype(F32)
    inv_rms = lax.rsqrt(jnp.mean(act_f * act_f, axis=-1, keepdims=True) + RMS_EPS)
    return (act_f * inv_rms * gain_vec.astype(F32)).astype(BF16), inv_rms


def rms_norm_bwd(act_in, gain_vec, inv_rms, d_normed):
    act_f = act_in.astype(F32)
    d_f = d_normed.astype(F32)
    scaled_d = d_f * gain_vec.astype(F32)
    proj_mean = jnp.mean(scaled_d * act_f, axis=-1, keepdims=True)
    d_act = inv_rms * scaled_d - act_f * (inv_rms * inv_rms * inv_rms) * proj_mean
    d_gain = jnp.sum(d_f * act_f * inv_rms, axis=0)
    return d_act, d_gain


def dot(lhs, rhs, l_dim, r_dim):
    return lax.dot_general(lhs, rhs, (((l_dim,), (r_dim,)), ((), ())), preferred_element_type=F32)


def gather(shard):
    return lax.all_gather(shard, SEQ_AXIS, axis=0, tiled=True)


def exchange(blocks):
    return lax.all_to_all(blocks, SEQ_AXIS, 0, 0, tiled=True)


def rope_t(vals, cos_tab, sin_tab):
    half = vals.shape[0] // 2
    first, second = vals[:half], vals[half:]
    return jnp.concatenate([first * cos_tab - second * sin_tab, second * cos_tab + first * sin_tab], axis=0)


def mm(lhs, rhs):
    return jnp.dot(lhs, rhs, preferred_element_type=F32)


def diag_mask(tile):
    key_at = lax.broadcasted_iota(jnp.int32, (tile, tile), 0)
    query_at = lax.broadcasted_iota(jnp.int32, (tile, tile), 1)
    return key_at <= query_at


def attn_fwd_kernel(tile, q_t, k_ref, v_t, o_ref, of_ref, lse_ref, s_buf):
    step = pl.program_id(0)
    query = q_t[...]

    def scores(j):
        return mm(k_ref[pl.ds(pl.multiple_of(j * tile, tile), tile), :], query)

    def keep(j, logits, top):
        s_buf[pl.ds(pl.multiple_of(j * tile, tile), tile), :] = logits
        return jnp.maximum(top, jnp.max(logits, axis=0, keepdims=True))

    top = keep(step, jnp.where(diag_mask(tile), scores(step), MASK_VALUE), jnp.full((1, tile), MASK_VALUE, F32))
    top = lax.fori_loop(0, step, lambda j, c: keep(j, scores(j), c), top)

    def weigh(j, carry):
        acc, total = carry
        at = pl.ds(pl.multiple_of(j * tile, tile), tile)
        prob = jnp.exp(s_buf[at, :] - top)
        return acc + mm(v_t[:, at], prob.astype(BF16)), total + jnp.sum(prob, axis=0, keepdims=True)

    out, total = lax.fori_loop(0, step + 1, weigh, (jnp.zeros((v_t.shape[0], tile), F32), jnp.zeros((1, tile), F32)))
    out = out / total
    lse = top + jnp.log(total)
    of_ref[...] = out
    lse_ref[...] = lse
    block = o_ref.shape[2]
    for part in range(tile // block):
        o_ref[part] = out[:, part * block:(part + 1) * block].astype(BF16)


def attention_fwd(q_t, k_in, v_t, n_blocks):
    head_dim, seq = q_t.shape
    block = seq // n_blocks
    per = TILE // block
    return pl.pallas_call(
        lambda *refs: attn_fwd_kernel(TILE, *refs),
        grid=(seq // TILE,),
        in_specs=[pl.BlockSpec((head_dim, TILE), lambda i: (0, i)), pl.BlockSpec((seq, head_dim), lambda i: (0, 0)), pl.BlockSpec((head_dim, seq), lambda i: (0, 0))],
        out_specs=[pl.BlockSpec((per, head_dim, block), lambda i: (i, 0, 0)), pl.BlockSpec((head_dim, TILE), lambda i: (0, i)), pl.BlockSpec((1, TILE), lambda i: (0, i))],
        out_shape=[jax.ShapeDtypeStruct((n_blocks, head_dim, block), BF16), jax.ShapeDtypeStruct((head_dim, seq), F32), jax.ShapeDtypeStruct((1, seq), F32)],
        scratch_shapes=[pltpu.VMEM((seq, TILE), F32)],
        cost_estimate=pl.CostEstimate(flops=8 * seq * seq * head_dim, bytes_accessed=8 * seq * head_dim, transcendentals=seq * seq),
        name='attn_fwd',
    )(q_t, k_in, v_t)


PARTS = ((0, 96), (96, 80), (176, 80))
CORE, CHIP_AXES = 1, (2, 4, 8)


def flip(dev, bit):
    return dev + bit * (1 - 2 * ((dev // bit) % 2))


def start_copy(src, dst, send_sem, recv_sem, peer):
    copy = pltpu.make_async_remote_copy(src_ref=src, dst_ref=dst, send_sem=send_sem, recv_sem=recv_sem, device_id=(peer,), device_id_type=pl.DeviceIdType.MESH)
    copy.start()
    return copy


def landed(ref, sem):
    pltpu.make_async_copy(ref, ref, sem).wait()


def enter_all(me, n_dev):
    barrier = pltpu.get_barrier_semaphore()

    @pl.loop(1, n_dev)
    def _(hop):
        pl.semaphore_signal(barrier, inc=1, device_id=(lax.rem(me + hop, n_dev),), device_id_type=pl.DeviceIdType.MESH)

    pl.semaphore_wait(barrier, n_dev - 1)


class CubeGather:
    def __init__(self, me, part, send_sem, recv_sem, core_sem):
        self.me, self.part = me, part
        self.send_sem, self.recv_sem, self.core_sem = send_sem, recv_sem, core_sem
        self.sent = []

    def axes(self, p):
        return [CHIP_AXES[(p + i) % 3] for i in range(3)]

    def owner(self, p, index, start=None):
        dev = self.me if start is None else start
        for i, bit in enumerate(self.axes(p)):
            if (index >> i) & 1:
                dev = flip(dev, bit)
        return dev

    def push(self, p, index, axis):
        ref = self.part(self.owner(p, index), p)
        start_copy(ref, ref, self.send_sem.at[len(self.sent)], self.recv_sem.at[p, index + (1 << axis)], flip(self.me, self.axes(p)[axis]))
        self.sent.append((p, index))

    def push_core(self, p, index):
        ref = self.part(self.owner(p, index), p)
        start_copy(ref, ref, self.send_sem.at[len(self.sent)], self.core_sem.at[p, index], flip(self.me, CORE))
        self.sent.append((p, index))

    def begin(self):
        for axis in range(3):
            for p in range(3):
                self.push(p, 0, axis)
        for p in range(3):
            self.push_core(p, 0)

    def receive(self, index):
        for p in range(3):
            landed(self.part(self.owner(p, index), p), self.recv_sem.at[p, index])
            for axis in range(index.bit_length(), 3):
                self.push(p, index, axis)
            self.push_core(p, index)

    def receive_core(self, index):
        for p in range(3):
            landed(self.part(self.owner(p, index, flip(self.me, CORE)), p), self.core_sem.at[p, index])

    def finish(self):
        for slot, (p, index) in enumerate(self.sent):
            landed(self.part(self.owner(p, index), p), self.send_sem.at[slot])


N_SENDS = 9 + 12 + 24


def attn_bwd_kernel(n_dev, tile, block, q_t, do_t, of_t, lse_ref, cos_ref, sin_ref, k_ref, k_t, v_ref, cos_all, sin_all, w_ref, d_blocks, d_proj_t, w_out, dq_acc, dk_acc, dv_acc, w_buf, send_sem, recv_sem, core_sem, local_sem):
    step = pl.program_id(0)
    last = pl.num_programs(0) - 1
    me = lax.axis_index(SEQ_AXIS)
    cube = CubeGather(me, lambda dev, p: w_buf.at[p, dev], send_sem, recv_sem, core_sem)

    @pl.when(step == 0)
    def _():
        own = [pltpu.make_async_copy(w_ref.at[p], w_buf.at[p, me], local_sem.at[p]) for p in range(3)]
        for copy in own:
            copy.start()
        enter_all(me, n_dev)
        for copy in own:
            copy.wait()
        cube.begin()

    for at_step, indices in ((4, (1,)), (5, (2,)), (6, (4,)), (7, (3,))):
        @pl.when(step == at_step)
        def _(indices=indices):
            for index in indices:
                cube.receive(index)

    head_dim = q_t.shape[0]
    query_t, d_out_t = q_t[...], do_t[...]
    lse = lse_ref[...]
    delta = jnp.sum(d_out_t.astype(F32) * of_t[...], axis=0, keepdims=True)

    @pl.when(step == 0)
    def _():
        dk_acc[...] = jnp.zeros_like(dk_acc)
        dv_acc[...] = jnp.zeros_like(dv_acc)

    dq_acc[...] = jnp.zeros_like(dq_acc)

    def visit(j, masked):
        at = pl.ds(pl.multiple_of(j * tile, tile), tile)
        prob = jnp.exp(mm(k_ref[at, :], query_t) - lse)
        if masked:
            prob = jnp.where(diag_mask(tile), prob, 0.0)
        d_prob = mm(v_ref[at, :], d_out_t).astype(BF16).astype(F32)
        d_logits = (prob * (d_prob - delta)).astype(BF16)
        dv_acc[:, at] += dot(d_out_t, prob.astype(BF16), 1, 1)
        dk_acc[:, at] += dot(query_t, d_logits, 1, 1)
        dq_acc[...] += mm(k_t[:, at], d_logits)

    visit(step, True)

    @pl.loop(0, step)
    def _(j):
        visit(j, False)

    def put(row, col_block, values):
        rows = slice(row, row + values.shape[0])
        d_proj_t[rows, pl.ds(pl.multiple_of(col_block * block, block), values.shape[1])] = values
        for part in range(values.shape[1] // block):
            d_blocks[col_block + part, rows, :] = values[:, part * block:(part + 1) * block]

    d_q = (dq_acc[...] * (head_dim ** -0.5)).astype(BF16).astype(F32)
    per = tile // block
    put(0, step * per, rope_t(d_q, cos_ref[...], -sin_ref[...]).astype(BF16))

    @pl.when(step == last)
    def _():
        @pl.loop(0, pl.num_programs(0))
        def _(j):
            at = pl.ds(pl.multiple_of(j * tile, tile), tile)
            put(head_dim, j * per, rope_t(dk_acc[:, at].astype(BF16).astype(F32), cos_all[:, at], -sin_all[:, at]).astype(BF16))
            put(2 * head_dim, j * per, dv_acc[:, at].astype(BF16))

        for index in (5, 6, 7):
            cube.receive(index)
        for index in range(8):
            cube.receive_core(index)
        flush = pltpu.make_async_copy(w_buf, w_out, local_sem.at[0])
        flush.start()
        cube.finish()
        flush.wait()


def attention_bwd(q_t, do_t, of_t, lse, k_in, k_t, v_in, cos_t, sin_t, w_parts, n_blocks):
    head_dim, seq = q_t.shape
    block = seq // n_blocks
    cols = pl.BlockSpec((head_dim, TILE), lambda i: (0, i))
    half_cols = pl.BlockSpec((head_dim // 2, TILE), lambda i: (0, i))
    all_rows = pl.BlockSpec((seq, head_dim), lambda i: (0, 0))
    all_cols = pl.BlockSpec((head_dim, seq), lambda i: (0, 0))
    all_half = pl.BlockSpec((head_dim // 2, seq), lambda i: (0, 0))
    w_all_shape = (3, n_blocks) + w_parts.shape[1:]
    return pl.pallas_call(
        lambda *refs: attn_bwd_kernel(n_blocks, TILE, block, *refs),
        grid=(seq // TILE,),
        in_specs=[cols, cols, cols, pl.BlockSpec((1, TILE), lambda i: (0, i)), half_cols, half_cols, all_rows, all_cols, all_rows, all_half, all_half, pl.BlockSpec(memory_space=pl.ANY)],
        out_specs=[pl.BlockSpec((n_blocks, 3 * head_dim, block), lambda i: (0, 0, 0)), pl.BlockSpec((3 * head_dim, seq), lambda i: (0, 0)), pl.BlockSpec(memory_space=pl.ANY)],
        out_shape=[jax.ShapeDtypeStruct((n_blocks, 3 * head_dim, block), BF16), jax.ShapeDtypeStruct((3 * head_dim, seq), BF16), jax.ShapeDtypeStruct(w_all_shape, BF16)],
        scratch_shapes=[
            pltpu.VMEM((head_dim, TILE), F32),
            pltpu.VMEM((head_dim, seq), F32),
            pltpu.VMEM((head_dim, seq), F32),
            pltpu.VMEM(w_all_shape, BF16),
            pltpu.SemaphoreType.DMA((N_SENDS,)),
            pltpu.SemaphoreType.DMA((3, 8)),
            pltpu.SemaphoreType.DMA((3, 8)),
            pltpu.SemaphoreType.DMA((3,)),
        ],
        compiler_params=pltpu.CompilerParams(collective_id=1, has_side_effects=True),
        cost_estimate=pl.CostEstimate(flops=20 * seq * seq * head_dim, bytes_accessed=20 * seq * head_dim, transcendentals=seq * seq),
        name='attn_bwd',
    )(q_t, do_t, of_t, lse, cos_t, sin_t, k_in, k_t, v_in, cos_t, sin_t, w_parts)


def gather_proj_kernel(n_dev, x_ref, small_ref, w_ref, u_out, proj_t, small_all, x_buf, u_buf, w_buf, send_sem, recv_sem, core_sem, misc_send, misc_recv, local_sem, u_sem):
    me = lax.axis_index(SEQ_AXIS)
    own = pltpu.make_async_copy(x_ref, x_buf.at[me], local_sem.at[0])
    own.start()
    own_w = pltpu.make_async_copy(w_ref.at[me], w_buf.at[me], local_sem.at[1])
    own_w.start()
    own_small = pltpu.make_async_copy(small_ref, small_all.at[me], local_sem.at[2])
    own_small.start()
    enter_all(me, n_dev)
    own.wait()
    cube = CubeGather(me, lambda dev, p: x_buf.at[dev, pl.ds(PARTS[p][0], PARTS[p][1])], send_sem, recv_sem, core_sem)
    cube.begin()

    def spread(hop):
        peer = lax.rem(me + hop, n_dev)
        return [
            pltpu.make_async_remote_copy(src_ref=small_ref, dst_ref=small_all.at[me], send_sem=misc_send.at[0, hop], recv_sem=misc_recv.at[0, me], device_id=(peer,), device_id_type=pl.DeviceIdType.MESH),
            pltpu.make_async_remote_copy(src_ref=w_ref.at[peer], dst_ref=w_buf.at[me], send_sem=misc_send.at[1, hop], recv_sem=misc_recv.at[1, me], device_id=(peer,), device_id_type=pl.DeviceIdType.MESH),
        ]

    for kind in range(2):
        @pl.loop(1, n_dev)
        def _(hop, kind=kind):
            spread(hop)[kind].start()

    cube.receive(1)
    cube.receive(2)
    own_w.wait()
    own_small.wait()

    @pl.loop(1, n_dev)
    def _(hop):
        src = lax.rem(me + hop, n_dev)
        landed(small_all.at[src], misc_recv.at[0, src])
        landed(w_buf.at[src], misc_recv.at[1, src])

    width = x_ref.shape[1]
    tok = x_ref.shape[0]
    rows = w_ref.shape[1]
    gain = jnp.concatenate([small_all[d, 0:1, 0:rows] for d in range(n_dev)], axis=1)
    weight = w_buf[...].reshape(width, w_ref.shape[2])
    keep = proj_t.shape[0]
    flushes = []

    def project(dev):
        act = x_buf[dev].astype(F32)
        inv = lax.rsqrt(jnp.mean(act * act, axis=-1, keepdims=True) + RMS_EPS)
        normed = (act * inv * gain).astype(BF16)
        u_buf[dev] = normed
        proj_t[:, pl.ds(pl.multiple_of(dev * tok, tok), tok)] = mm(normed, weight).T[:keep]
        flush = pltpu.make_async_copy(u_buf.at[dev], u_out.at[dev], u_sem.at[len(flushes)])
        flush.start()
        flushes.append(flush)

    other = flip(me, CORE)
    cube.receive_core(0)
    project(me)
    project(other)
    cube.receive(4)
    cube.receive(3)
    for index in (1, 2, 4):
        cube.receive_core(index)
    for bit in CHIP_AXES:
        project(flip(me, bit))
        project(flip(other, bit))
    cube.receive(5)
    cube.receive(6)
    for index in (3, 5, 6):
        cube.receive_core(index)
    for skip in range(3):
        bits = [bit for i, bit in enumerate(CHIP_AXES) if i != skip]
        project(flip(flip(me, bits[0]), bits[1]))
        project(flip(flip(other, bits[0]), bits[1]))
    cube.receive(7)
    cube.receive_core(7)
    far = flip(flip(flip(me, 2), 4), 8)
    project(far)
    project(flip(far, CORE))

    cube.finish()

    @pl.loop(1, n_dev)
    def _(hop):
        for copy in spread(hop):
            copy.wait_send()

    for flush in flushes:
        flush.wait()


def gather_proj(n_dev, x_act, small, w_blocks, qkv):
    tok, width = x_act.shape
    seq = tok * n_dev
    any_spec = pl.BlockSpec(memory_space=pl.ANY)
    vmem_spec = pl.BlockSpec(memory_space=pltpu.VMEM)
    return pl.pallas_call(
        lambda *refs: gather_proj_kernel(n_dev, *refs),
        in_specs=[any_spec, vmem_spec, vmem_spec],
        out_specs=[any_spec, vmem_spec, vmem_spec],
        out_shape=[jax.ShapeDtypeStruct((n_dev, tok, width), BF16), jax.ShapeDtypeStruct((qkv, seq), F32), jax.ShapeDtypeStruct((n_dev,) + small.shape, F32)],
        scratch_shapes=[
            pltpu.VMEM((n_dev, tok, width), BF16),
            pltpu.VMEM((n_dev, tok, width), BF16),
            pltpu.VMEM(w_blocks.shape, BF16),
            pltpu.SemaphoreType.DMA((N_SENDS,)),
            pltpu.SemaphoreType.DMA((3, 8)),
            pltpu.SemaphoreType.DMA((3, 8)),
            pltpu.SemaphoreType.DMA((2, n_dev)),
            pltpu.SemaphoreType.DMA((2, n_dev)),
            pltpu.SemaphoreType.DMA((3,)),
            pltpu.SemaphoreType.DMA((n_dev,)),
        ],
        compiler_params=pltpu.CompilerParams(collective_id=0, has_side_effects=True),
        cost_estimate=pl.CostEstimate(flops=30 * seq * width * width, bytes_accessed=4 * seq * width, transcendentals=0),
        name='gather_proj',
    )(x_act, small, w_blocks)


def gate_backward(d_mixed, gate_pre, up_pre):
    gate_sig = jax.nn.sigmoid(gate_pre)
    d_up = (d_mixed * gate_pre * gate_sig).astype(BF16)
    d_gate = (d_mixed * up_pre * gate_sig * (1.0 + gate_pre * (1.0 - gate_sig))).astype(BF16)
    return d_gate, d_up


def join_columns_kernel(size, src, first, second):
    for i, out in enumerate((first, second)):
        out[...] = jnp.concatenate([src[d, :, i * size:(i + 1) * size] for d in range(src.shape[0])], axis=1)


def join_columns(blocks, size):
    shape = jax.ShapeDtypeStruct((blocks.shape[1], blocks.shape[0] * size), F32)
    return pl.pallas_call(lambda *refs: join_columns_kernel(size, *refs), out_shape=[shape, shape], name='join_columns')(blocks)


def split_heads_kernel(head_dim, src, *outs):
    for i, out in enumerate(outs):
        for d in range(src.shape[0]):
            out[:, d, :] = src[d, :, i * head_dim:(i + 1) * head_dim]


def split_heads(blocks, head_dim):
    shape = jax.ShapeDtypeStruct((blocks.shape[1], blocks.shape[0], head_dim), F32)
    return pl.pallas_call(lambda *refs: split_heads_kernel(head_dim, *refs), out_shape=[shape] * 3, name='split_heads')(blocks)


def device_step(n_dev, x_act, positions, grad_out, g_attn_s, w_q, w_k, w_v, w_o, g_mlp_s, w_gate, w_up, w_down):
    tok, width = x_act.shape
    seq = tok * n_dev
    rows, heads, head_dim = w_q.shape
    ff = w_gate.shape[1]
    ff_s = ff // n_dev
    qkv = 3 * head_dim

    small = jnp.concatenate([jnp.concatenate([g_attn_s, g_mlp_s]).astype(F32)[None], positions.astype(F32).reshape(-1, 2 * rows)], axis=0)
    small = jnp.pad(small, ((0, 8 - small.shape[0]), (0, 0)))
    w_qkv = jnp.concatenate([w_q, w_k, w_v], axis=2)
    w_blocks = jnp.pad(jnp.transpose(w_qkv, (1, 0, 2)), ((0, 0), (0, 0), (0, 256 - qkv)))
    u_all, proj_t, small_all = gather_proj(n_dev, x_act, small, w_blocks, qkv)
    u_all = u_all.reshape(seq, width)
    g_attn = small_all[:, 0, :rows].reshape(width)
    g_mlp = small_all[:, 0, rows:2 * rows].reshape(width)
    pos_all = small_all[:, 1:1 + tok // (2 * rows)]

    down_groups = [w_down[i:i + rows] for i in range(0, ff_s, rows)]
    down_groups = [jnp.pad(group, ((0, rows - group.shape[0]), (0, 0))) for group in down_groups]
    w_all = gather(jnp.concatenate([w_gate, w_up, w_o[0]] + down_groups, axis=1))
    w_gu = w_all[:, :2 * ff]
    w_o_all = w_all[:, 2 * ff:2 * ff + width]
    w_down_at = 2 * ff + width
    down_all = [w_all[:, w_down_at + i * width:w_down_at + (i + 1) * width].reshape(n_dev, rows, width) for i in range(len(down_groups))]
    w_down_all = jnp.concatenate(down_all, axis=1)[:, :ff_s].reshape(ff, width)
    me = lax.axis_index(SEQ_AXIS)
    w_cols = jnp.concatenate([lax.dynamic_slice(w_all, (0, at + me * ff_s), (width, ff_s)) for at in (0, ff)], axis=1)

    half = head_dim // 2
    inv_freq = ROPE_BASE ** (-(jnp.arange(half, dtype=F32) * (2.0 / head_dim)))
    angle_t = inv_freq[:, None] * pos_all.reshape(1, seq)
    cos_t, sin_t = jnp.cos(angle_t), jnp.sin(angle_t)

    q_t = (rope_t(proj_t[:head_dim], cos_t, sin_t).astype(BF16).astype(F32) * (head_dim ** -0.5)).astype(BF16)
    k_t = rope_t(proj_t[head_dim:2 * head_dim], cos_t, sin_t).astype(BF16)
    v_t = proj_t[2 * head_dim:].astype(BF16)
    k_in, v_in = k_t.T, v_t.T
    o_blocks, of_t, lse = attention_fwd(q_t, k_in, v_t, n_dev)
    o_loc = exchange(o_blocks).reshape(width, tok)

    hidden = (x_act.astype(F32) + dot(o_loc, w_o_all, 0, 0)).astype(BF16)
    normed_mlp, inv_rms_mlp = rms_norm(hidden, g_mlp)
    a_dy = gather(jnp.concatenate([normed_mlp, grad_out], axis=1))
    pre = dot(normed_mlp, w_gu, 1, 0)
    gate_pre, up_pre = pre[:, :ff], pre[:, ff:]
    mixed = (jax.nn.silu(gate_pre) * up_pre).astype(BF16)
    y_out = (hidden.astype(F32) + dot(mixed, w_down_all, 1, 0)).astype(BF16)

    d_mixed = dot(grad_out, w_down_all, 1, 1).astype(BF16).astype(F32)
    d_gu = jnp.concatenate(gate_backward(d_mixed, gate_pre, up_pre), axis=1)
    d_normed = dot(d_gu, w_gu, 1, 1).astype(BF16)
    d_hid_norm, part_g_mlp = rms_norm_bwd(hidden, g_mlp, inv_rms_mlp, d_normed)
    d_hidden = (grad_out.astype(F32) + d_hid_norm).astype(BF16)
    do_blocks = exchange(dot(w_o_all, d_hidden, 1, 1).astype(BF16).reshape(n_dev, head_dim, tok))
    half_n = n_dev // 2
    pairs = [(i, (i + half_n) % n_dev) for i in range(n_dev)]
    near = (me // half_n) * half_n
    o_far = lax.ppermute(lax.dynamic_slice_in_dim(o_blocks, half_n - near, half_n), SEQ_AXIS, pairs)
    o_pair = jnp.concatenate([lax.dynamic_slice_in_dim(o_blocks, near, half_n), o_far], axis=1)
    dh_half = lax.all_gather(d_hidden, SEQ_AXIS, axis=0, tiled=True, axis_index_groups=[list(range(half_n)), list(range(half_n, n_dev))])

    do_t = jnp.transpose(do_blocks, (1, 0, 2)).reshape(head_dim, seq)
    w_parts = jnp.stack([w.reshape(rows, heads * head_dim) for w in (w_q, w_k, w_v)])
    d_blocks, d_proj_t, w_qkv_all = attention_bwd(q_t, do_t, of_t, lse, k_in, k_t, v_in, cos_t, sin_t, w_parts, n_dev)
    d_proj = exchange(d_blocks)

    a_dy, d_proj_t = lax.optimization_barrier((a_dy, d_proj_t))
    a_all, dy_all = a_dy[:, :width], a_dy[:, width:]
    pre_t = dot(w_cols, a_all, 0, 1)
    gate_t, up_t = pre_t[:ff_s], pre_t[ff_s:]
    d_mixed_t = dot(w_down, dy_all, 1, 1).astype(BF16).astype(F32)
    mixed_t = (jax.nn.silu(gate_t) * up_t).astype(BF16)
    d_gu_t = jnp.concatenate(gate_backward(d_mixed_t, gate_t, up_t), axis=0)
    grad_w_down = dot(mixed_t, dy_all, 1, 0)
    grad_w_gu = dot(a_all, d_gu_t, 0, 1)
    mlp_send = jnp.concatenate([grad_w_gu, part_g_mlp[:, None]], axis=1).reshape(n_dev, rows, 2 * ff_s + 1)
    d_proj, grad_w_down, d_proj_t, mlp_send = lax.optimization_barrier((d_proj, grad_w_down, d_proj_t, mlp_send))
    mlp_back = exchange(mlp_send)
    d_proj = d_proj.reshape(heads, 3, head_dim, tok)
    grad_w_qkv = lax.optimization_barrier(dot(d_proj_t, u_all, 1, 0)).T
    inv_rms = lax.rsqrt(jnp.mean(jnp.square(x_act.astype(F32)), axis=-1, keepdims=True) + RMS_EPS)
    d_u = sum(dot(d_proj[:, p].reshape(heads * head_dim, tok), w_qkv_all[p].reshape(width, heads * head_dim), 0, 1) for p in range(3)).astype(BF16)
    d_x_norm, part_g_attn = rms_norm_bwd(x_act, g_attn, inv_rms, d_u)
    grad_x = (d_hidden.astype(F32) + d_x_norm).astype(BF16)
    attn_send = jnp.concatenate([grad_w_qkv, part_g_attn[:, None]], axis=1).reshape(n_dev, rows, qkv + 1)
    mlp_back, attn_send = lax.optimization_barrier((mlp_back, attn_send))
    dh_half, attn_send = lax.optimization_barrier((dh_half, attn_send))
    attn_back = exchange(attn_send)
    part_w_o = dot(o_pair.transpose(1, 0, 2).reshape(2 * head_dim, seq // 2), dh_half, 1, 0)
    grad_w_o = (part_w_o[:head_dim] + lax.ppermute(part_w_o[head_dim:], SEQ_AXIS, pairs))[None]

    grad_g_mlp = jnp.sum(mlp_back[:, :, 2 * ff_s], axis=0)
    grad_g_attn = jnp.sum(attn_back[:, :, qkv], axis=0)
    grad_w_gate, grad_w_up = join_columns(mlp_back, ff_s)
    grad_w_q, grad_w_k, grad_w_v = split_heads(attn_back, head_dim)
    return (y_out, grad_x, grad_g_attn, grad_w_q, grad_w_k, grad_w_v, grad_w_o, grad_g_mlp, grad_w_gate, grad_w_up, grad_w_down)


def solution(mesh):
    n_dev = mesh.shape[SEQ_AXIS]
    token_spec = P(SEQ_AXIS, None)
    cube_spec = P(SEQ_AXIS, None, None)
    gain_spec = P(SEQ_AXIS)
    weight_specs = (gain_spec, cube_spec, cube_spec, cube_spec, cube_spec, gain_spec, token_spec, token_spec, token_spec)
    return jax.shard_map(lambda *args: device_step(n_dev, *args), mesh=mesh, in_specs=(token_spec, gain_spec, token_spec) + weight_specs, out_specs=(token_spec, token_spec) + weight_specs, check_vma=False)
```

```python
import jax
import jax.numpy as jnp
from jax import lax
from jax.experimental import pallas as pl
from jax.experimental.pallas import tpu as pltpu
from jax.sharding import PartitionSpec as P

SEQ_AXIS = 'sp'
RMS_EPS = 1e-5
ROPE_BASE = 10000.0
MASK_VALUE = -1e30
TILE = 512
F32 = jnp.float32
BF16 = jnp.bfloat16


def rms_norm(act_in, gain_vec):
    act_f = act_in.astype(F32)
    inv_rms = lax.rsqrt(jnp.mean(act_f * act_f, axis=-1, keepdims=True) + RMS_EPS)
    return (act_f * inv_rms * gain_vec.astype(F32)).astype(BF16), inv_rms


def rms_norm_bwd(act_in, gain_vec, inv_rms, d_normed):
    act_f = act_in.astype(F32)
    d_f = d_normed.astype(F32)
    scaled_d = d_f * gain_vec.astype(F32)
    proj_mean = jnp.mean(scaled_d * act_f, axis=-1, keepdims=True)
    d_act = inv_rms * scaled_d - act_f * (inv_rms * inv_rms * inv_rms) * proj_mean
    d_gain = jnp.sum(d_f * act_f * inv_rms, axis=0)
    return d_act, d_gain


def dot(lhs, rhs, l_dim, r_dim):
    return lax.dot_general(lhs, rhs, (((l_dim,), (r_dim,)), ((), ())), preferred_element_type=F32)


def gather(shard):
    return lax.all_gather(shard, SEQ_AXIS, axis=0, tiled=True)


def exchange(blocks):
    return lax.all_to_all(blocks, SEQ_AXIS, 0, 0, tiled=True)


def rope_t(vals, cos_tab, sin_tab):
    half = vals.shape[0] // 2
    first, second = vals[:half], vals[half:]
    return jnp.concatenate([first * cos_tab - second * sin_tab, second * cos_tab + first * sin_tab], axis=0)


def mm(lhs, rhs):
    return jnp.dot(lhs, rhs, preferred_element_type=F32)


def diag_mask(tile):
    key_at = lax.broadcasted_iota(jnp.int32, (tile, tile), 0)
    query_at = lax.broadcasted_iota(jnp.int32, (tile, tile), 1)
    return key_at <= query_at


def attn_fwd_kernel(tile, q_t, k_ref, v_t, o_ref, of_ref, lse_ref, s_buf):
    step = pl.program_id(0)
    query = q_t[...]

    def scores(j):
        return mm(k_ref[pl.ds(pl.multiple_of(j * tile, tile), tile), :], query)

    def keep(j, logits, top):
        s_buf[pl.ds(pl.multiple_of(j * tile, tile), tile), :] = logits
        return jnp.maximum(top, jnp.max(logits, axis=0, keepdims=True))

    top = keep(step, jnp.where(diag_mask(tile), scores(step), MASK_VALUE), jnp.full((1, tile), MASK_VALUE, F32))
    top = lax.fori_loop(0, step, lambda j, c: keep(j, scores(j), c), top)

    def weigh(j, carry):
        acc, total = carry
        at = pl.ds(pl.multiple_of(j * tile, tile), tile)
        prob = jnp.exp(s_buf[at, :] - top)
        return acc + mm(v_t[:, at], prob.astype(BF16)), total + jnp.sum(prob, axis=0, keepdims=True)

    out, total = lax.fori_loop(0, step + 1, weigh, (jnp.zeros((v_t.shape[0], tile), F32), jnp.zeros((1, tile), F32)))
    out = out / total
    lse = top + jnp.log(total)
    of_ref[...] = out
    lse_ref[...] = lse
    block = o_ref.shape[2]
    for part in range(tile // block):
        o_ref[part] = out[:, part * block:(part + 1) * block].astype(BF16)


def attention_fwd(q_t, k_in, v_t, n_blocks):
    head_dim, seq = q_t.shape
    block = seq // n_blocks
    per = TILE // block
    return pl.pallas_call(
        lambda *refs: attn_fwd_kernel(TILE, *refs),
        grid=(seq // TILE,),
        in_specs=[pl.BlockSpec((head_dim, TILE), lambda i: (0, i)), pl.BlockSpec((seq, head_dim), lambda i: (0, 0)), pl.BlockSpec((head_dim, seq), lambda i: (0, 0))],
        out_specs=[pl.BlockSpec((per, head_dim, block), lambda i: (i, 0, 0)), pl.BlockSpec((head_dim, TILE), lambda i: (0, i)), pl.BlockSpec((1, TILE), lambda i: (0, i))],
        out_shape=[jax.ShapeDtypeStruct((n_blocks, head_dim, block), BF16), jax.ShapeDtypeStruct((head_dim, seq), F32), jax.ShapeDtypeStruct((1, seq), F32)],
        scratch_shapes=[pltpu.VMEM((seq, TILE), F32)],
        cost_estimate=pl.CostEstimate(flops=8 * seq * seq * head_dim, bytes_accessed=8 * seq * head_dim, transcendentals=seq * seq),
        name='attn_fwd',
    )(q_t, k_in, v_t)


PARTS = ((0, 96), (96, 80), (176, 80))
CORE, CHIP_AXES = 1, (2, 4, 8)


def flip(dev, bit):
    return dev + bit * (1 - 2 * ((dev // bit) % 2))


def start_copy(src, dst, send_sem, recv_sem, peer):
    copy = pltpu.make_async_remote_copy(src_ref=src, dst_ref=dst, send_sem=send_sem, recv_sem=recv_sem, device_id=(peer,), device_id_type=pl.DeviceIdType.MESH)
    copy.start()
    return copy


def landed(ref, sem):
    pltpu.make_async_copy(ref, ref, sem).wait()


def enter_all(me, n_dev):
    barrier = pltpu.get_barrier_semaphore()

    @pl.loop(1, n_dev)
    def _(hop):
        pl.semaphore_signal(barrier, inc=1, device_id=(lax.rem(me + hop, n_dev),), device_id_type=pl.DeviceIdType.MESH)

    pl.semaphore_wait(barrier, n_dev - 1)


class CubeGather:
    def __init__(self, me, part, send_sem, recv_sem, core_sem):
        self.me, self.part = me, part
        self.send_sem, self.recv_sem, self.core_sem = send_sem, recv_sem, core_sem
        self.sent = []

    def axes(self, p):
        return [CHIP_AXES[(p + i) % 3] for i in range(3)]

    def owner(self, p, index, start=None):
        dev = self.me if start is None else start
        for i, bit in enumerate(self.axes(p)):
            if (index >> i) & 1:
                dev = flip(dev, bit)
        return dev

    def push(self, p, index, axis):
        ref = self.part(self.owner(p, index), p)
        start_copy(ref, ref, self.send_sem.at[len(self.sent)], self.recv_sem.at[p, index + (1 << axis)], flip(self.me, self.axes(p)[axis]))
        self.sent.append((p, index))

    def push_core(self, p, index):
        ref = self.part(self.owner(p, index), p)
        start_copy(ref, ref, self.send_sem.at[len(self.sent)], self.core_sem.at[p, index], flip(self.me, CORE))
        self.sent.append((p, index))

    def begin(self):
        for axis in range(3):
            for p in range(3):
                self.push(p, 0, axis)
        for p in range(3):
            self.push_core(p, 0)

    def receive(self, index):
        for p in range(3):
            landed(self.part(self.owner(p, index), p), self.recv_sem.at[p, index])
            for axis in range(index.bit_length(), 3):
                self.push(p, index, axis)
            self.push_core(p, index)

    def receive_core(self, index):
        for p in range(3):
            landed(self.part(self.owner(p, index, flip(self.me, CORE)), p), self.core_sem.at[p, index])

    def finish(self):
        for slot, (p, index) in enumerate(self.sent):
            landed(self.part(self.owner(p, index), p), self.send_sem.at[slot])


N_SENDS = 9 + 12 + 24


def attn_bwd_kernel(n_dev, tile, block, q_t, do_t, of_t, lse_ref, cos_ref, sin_ref, k_ref, k_t, v_ref, cos_all, sin_all, w_ref, d_blocks, d_proj_t, w_out_q, w_out_k, w_out_v, dq_acc, dk_acc, dv_acc, w_buf, send_sem, recv_sem, core_sem, local_sem):
    step = pl.program_id(0)
    last = pl.num_programs(0) - 1
    me = lax.axis_index(SEQ_AXIS)
    cube = CubeGather(me, lambda dev, p: w_buf.at[p, dev], send_sem, recv_sem, core_sem)

    @pl.when(step == 0)
    def _():
        own = [pltpu.make_async_copy(w_ref.at[p], w_buf.at[p, me], local_sem.at[p]) for p in range(3)]
        for copy in own:
            copy.start()
        enter_all(me, n_dev)
        for copy in own:
            copy.wait()
        cube.begin()

    for at_step, indices in ((4, (1,)), (5, (2,)), (6, (4,)), (7, (3,))):
        @pl.when(step == at_step)
        def _(indices=indices):
            for index in indices:
                cube.receive(index)

    head_dim = q_t.shape[0]
    query_t, d_out_t = q_t[...], do_t[...]
    lse = lse_ref[...]
    delta = jnp.sum(d_out_t.astype(F32) * of_t[...], axis=0, keepdims=True)

    @pl.when(step == 0)
    def _():
        dk_acc[...] = jnp.zeros_like(dk_acc)
        dv_acc[...] = jnp.zeros_like(dv_acc)

    dq_acc[...] = jnp.zeros_like(dq_acc)

    def visit(j, masked):
        at = pl.ds(pl.multiple_of(j * tile, tile), tile)
        prob = jnp.exp(mm(k_ref[at, :], query_t) - lse)
        if masked:
            prob = jnp.where(diag_mask(tile), prob, 0.0)
        d_prob = mm(v_ref[at, :], d_out_t).astype(BF16).astype(F32)
        d_logits = (prob * (d_prob - delta)).astype(BF16)
        dv_acc[:, at] += dot(d_out_t, prob.astype(BF16), 1, 1)
        dk_acc[:, at] += dot(query_t, d_logits, 1, 1)
        dq_acc[...] += mm(k_t[:, at], d_logits)

    visit(step, True)

    @pl.loop(0, step)
    def _(j):
        visit(j, False)

    def put(row, col_block, values):
        rows = slice(row, row + values.shape[0])
        d_proj_t[rows, pl.ds(pl.multiple_of(col_block * block, block), values.shape[1])] = values
        for part in range(values.shape[1] // block):
            d_blocks[col_block + part, rows, :] = values[:, part * block:(part + 1) * block]

    d_q = (dq_acc[...] * (head_dim ** -0.5)).astype(BF16).astype(F32)
    per = tile // block
    put(0, step * per, rope_t(d_q, cos_ref[...], -sin_ref[...]).astype(BF16))

    @pl.when(step == last)
    def _():
        @pl.loop(0, pl.num_programs(0))
        def _(j):
            at = pl.ds(pl.multiple_of(j * tile, tile), tile)
            put(head_dim, j * per, rope_t(dk_acc[:, at].astype(BF16).astype(F32), cos_all[:, at], -sin_all[:, at]).astype(BF16))
            put(2 * head_dim, j * per, dv_acc[:, at].astype(BF16))

        for index in (5, 6, 7):
            cube.receive(index)
        for index in range(8):
            cube.receive_core(index)
        flushes = [pltpu.make_async_copy(w_buf.at[p], out, local_sem.at[p]) for p, out in enumerate((w_out_q, w_out_k, w_out_v))]
        for flush in flushes:
            flush.start()
        cube.finish()
        for flush in flushes:
            flush.wait()


def attention_bwd(q_t, do_t, of_t, lse, k_in, k_t, v_in, cos_t, sin_t, w_parts, n_blocks):
    head_dim, seq = q_t.shape
    block = seq // n_blocks
    cols = pl.BlockSpec((head_dim, TILE), lambda i: (0, i))
    half_cols = pl.BlockSpec((head_dim // 2, TILE), lambda i: (0, i))
    all_rows = pl.BlockSpec((seq, head_dim), lambda i: (0, 0))
    all_cols = pl.BlockSpec((head_dim, seq), lambda i: (0, 0))
    all_half = pl.BlockSpec((head_dim // 2, seq), lambda i: (0, 0))
    w_all_shape = (3, n_blocks) + w_parts.shape[1:]
    return pl.pallas_call(
        lambda *refs: attn_bwd_kernel(n_blocks, TILE, block, *refs),
        grid=(seq // TILE,),
        in_specs=[cols, cols, cols, pl.BlockSpec((1, TILE), lambda i: (0, i)), half_cols, half_cols, all_rows, all_cols, all_rows, all_half, all_half, pl.BlockSpec(memory_space=pl.ANY)],
        out_specs=[pl.BlockSpec((n_blocks, 3 * head_dim, block), lambda i: (0, 0, 0)), pl.BlockSpec((3 * head_dim, seq), lambda i: (0, 0))] + [pl.BlockSpec(memory_space=pl.ANY)] * 3,
        out_shape=[jax.ShapeDtypeStruct((n_blocks, 3 * head_dim, block), BF16), jax.ShapeDtypeStruct((3 * head_dim, seq), BF16)] + [jax.ShapeDtypeStruct(w_all_shape[1:], BF16)] * 3,
        scratch_shapes=[
            pltpu.VMEM((head_dim, TILE), F32),
            pltpu.VMEM((head_dim, seq), F32),
            pltpu.VMEM((head_dim, seq), F32),
            pltpu.VMEM(w_all_shape, BF16),
            pltpu.SemaphoreType.DMA((N_SENDS,)),
            pltpu.SemaphoreType.DMA((3, 8)),
            pltpu.SemaphoreType.DMA((3, 8)),
            pltpu.SemaphoreType.DMA((3,)),
        ],
        compiler_params=pltpu.CompilerParams(collective_id=1, has_side_effects=True),
        cost_estimate=pl.CostEstimate(flops=20 * seq * seq * head_dim, bytes_accessed=20 * seq * head_dim, transcendentals=seq * seq),
        name='attn_bwd',
    )(q_t, do_t, of_t, lse, cos_t, sin_t, k_in, k_t, v_in, cos_t, sin_t, w_parts)


def gather_proj_kernel(n_dev, x_ref, small_ref, w_ref, u_out, proj_t, small_all, x_buf, u_buf, w_buf, send_sem, recv_sem, core_sem, misc_send, misc_recv, local_sem, u_sem):
    me = lax.axis_index(SEQ_AXIS)
    own = pltpu.make_async_copy(x_ref, x_buf.at[me], local_sem.at[0])
    own.start()
    own_w = pltpu.make_async_copy(w_ref.at[me], w_buf.at[me], local_sem.at[1])
    own_w.start()
    own_small = pltpu.make_async_copy(small_ref, small_all.at[me], local_sem.at[2])
    own_small.start()
    enter_all(me, n_dev)
    own.wait()
    cube = CubeGather(me, lambda dev, p: x_buf.at[dev, pl.ds(PARTS[p][0], PARTS[p][1])], send_sem, recv_sem, core_sem)
    cube.begin()

    def spread(hop):
        peer = lax.rem(me + hop, n_dev)
        return [
            pltpu.make_async_remote_copy(src_ref=small_ref, dst_ref=small_all.at[me], send_sem=misc_send.at[0, hop], recv_sem=misc_recv.at[0, me], device_id=(peer,), device_id_type=pl.DeviceIdType.MESH),
            pltpu.make_async_remote_copy(src_ref=w_ref.at[peer], dst_ref=w_buf.at[me], send_sem=misc_send.at[1, hop], recv_sem=misc_recv.at[1, me], device_id=(peer,), device_id_type=pl.DeviceIdType.MESH),
        ]

    for kind in range(2):
        @pl.loop(1, n_dev)
        def _(hop, kind=kind):
            spread(hop)[kind].start()

    cube.receive(1)
    cube.receive(2)
    own_w.wait()
    own_small.wait()

    @pl.loop(1, n_dev)
    def _(hop):
        src = lax.rem(me + hop, n_dev)
        landed(small_all.at[src], misc_recv.at[0, src])
        landed(w_buf.at[src], misc_recv.at[1, src])

    width = x_ref.shape[1]
    tok = x_ref.shape[0]
    rows = w_ref.shape[1]
    gain = jnp.concatenate([small_all[d, 0:1, 0:rows] for d in range(n_dev)], axis=1)
    weight = w_buf[...].reshape(width, w_ref.shape[2])
    keep = proj_t.shape[0]
    flushes = []

    def project(dev):
        act = x_buf[dev].astype(F32)
        inv = lax.rsqrt(jnp.mean(act * act, axis=-1, keepdims=True) + RMS_EPS)
        normed = (act * inv * gain).astype(BF16)
        u_buf[dev] = normed
        proj_t[:, pl.ds(pl.multiple_of(dev * tok, tok), tok)] = mm(normed, weight).T[:keep]
        flush = pltpu.make_async_copy(u_buf.at[dev], u_out.at[dev], u_sem.at[len(flushes)])
        flush.start()
        flushes.append(flush)

    other = flip(me, CORE)
    cube.receive_core(0)
    project(me)
    project(other)
    cube.receive(4)
    cube.receive(3)
    for index in (1, 2, 4):
        cube.receive_core(index)
    for bit in CHIP_AXES:
        project(flip(me, bit))
        project(flip(other, bit))
    cube.receive(5)
    cube.receive(6)
    for index in (3, 5, 6):
        cube.receive_core(index)
    for skip in range(3):
        bits = [bit for i, bit in enumerate(CHIP_AXES) if i != skip]
        project(flip(flip(me, bits[0]), bits[1]))
        project(flip(flip(other, bits[0]), bits[1]))
    cube.receive(7)
    cube.receive_core(7)
    far = flip(flip(flip(me, 2), 4), 8)
    project(far)
    project(flip(far, CORE))

    cube.finish()

    @pl.loop(1, n_dev)
    def _(hop):
        for copy in spread(hop):
            copy.wait_send()

    for flush in flushes:
        flush.wait()


def gather_proj(n_dev, x_act, small, w_blocks, qkv):
    tok, width = x_act.shape
    seq = tok * n_dev
    any_spec = pl.BlockSpec(memory_space=pl.ANY)
    vmem_spec = pl.BlockSpec(memory_space=pltpu.VMEM)
    return pl.pallas_call(
        lambda *refs: gather_proj_kernel(n_dev, *refs),
        in_specs=[any_spec, vmem_spec, vmem_spec],
        out_specs=[any_spec, vmem_spec, vmem_spec],
        out_shape=[jax.ShapeDtypeStruct((n_dev, tok, width), BF16), jax.ShapeDtypeStruct((qkv, seq), F32), jax.ShapeDtypeStruct((n_dev,) + small.shape, F32)],
        scratch_shapes=[
            pltpu.VMEM((n_dev, tok, width), BF16),
            pltpu.VMEM((n_dev, tok, width), BF16),
            pltpu.VMEM(w_blocks.shape, BF16),
            pltpu.SemaphoreType.DMA((N_SENDS,)),
            pltpu.SemaphoreType.DMA((3, 8)),
            pltpu.SemaphoreType.DMA((3, 8)),
            pltpu.SemaphoreType.DMA((2, n_dev)),
            pltpu.SemaphoreType.DMA((2, n_dev)),
            pltpu.SemaphoreType.DMA((3,)),
            pltpu.SemaphoreType.DMA((n_dev,)),
        ],
        compiler_params=pltpu.CompilerParams(collective_id=0, has_side_effects=True),
        cost_estimate=pl.CostEstimate(flops=30 * seq * width * width, bytes_accessed=4 * seq * width, transcendentals=0),
        name='gather_proj',
    )(x_act, small, w_blocks)


def gate_backward(d_mixed, gate_pre, up_pre):
    gate_sig = jax.nn.sigmoid(gate_pre)
    d_up = (d_mixed * gate_pre * gate_sig).astype(BF16)
    d_gate = (d_mixed * up_pre * gate_sig * (1.0 + gate_pre * (1.0 - gate_sig))).astype(BF16)
    return d_gate, d_up


def join_columns_kernel(size, src, first, second):
    for i, out in enumerate((first, second)):
        out[...] = jnp.concatenate([src[d, :, i * size:(i + 1) * size] for d in range(src.shape[0])], axis=1)


def join_columns(blocks, size):
    shape = jax.ShapeDtypeStruct((blocks.shape[1], blocks.shape[0] * size), F32)
    return pl.pallas_call(lambda *refs: join_columns_kernel(size, *refs), out_shape=[shape, shape], name='join_columns')(blocks)


def split_heads_kernel(head_dim, src, *outs):
    for i, out in enumerate(outs):
        for d in range(src.shape[0]):
            out[:, d, :] = src[d, :, i * head_dim:(i + 1) * head_dim]


def split_heads(blocks, head_dim):
    shape = jax.ShapeDtypeStruct((blocks.shape[1], blocks.shape[0], head_dim), F32)
    return pl.pallas_call(lambda *refs: split_heads_kernel(head_dim, *refs), out_shape=[shape] * 3, name='split_heads')(blocks)


def device_step(n_dev, x_act, positions, grad_out, g_attn_s, w_q, w_k, w_v, w_o, g_mlp_s, w_gate, w_up, w_down):
    tok, width = x_act.shape
    seq = tok * n_dev
    rows, heads, head_dim = w_q.shape
    ff = w_gate.shape[1]
    ff_s = ff // n_dev
    qkv = 3 * head_dim

    small = jnp.concatenate([jnp.concatenate([g_attn_s, g_mlp_s]).astype(F32)[None], positions.astype(F32).reshape(-1, 2 * rows)], axis=0)
    small = jnp.pad(small, ((0, 8 - small.shape[0]), (0, 0)))
    w_qkv = jnp.concatenate([w_q, w_k, w_v], axis=2)
    w_blocks = jnp.pad(jnp.transpose(w_qkv, (1, 0, 2)), ((0, 0), (0, 0), (0, 256 - qkv)))
    u_all, proj_t, small_all = gather_proj(n_dev, x_act, small, w_blocks, qkv)
    u_all = u_all.reshape(seq, width)
    g_attn = small_all[:, 0, :rows].reshape(width)
    g_mlp = small_all[:, 0, rows:2 * rows].reshape(width)
    pos_all = small_all[:, 1:1 + tok // (2 * rows)]

    down_groups = [w_down[i:i + rows] for i in range(0, ff_s, rows)]
    down_groups = [jnp.pad(group, ((0, rows - group.shape[0]), (0, 0))) for group in down_groups]
    w_all = gather(jnp.concatenate([w_gate, w_up, w_o[0]] + down_groups, axis=1))
    w_gu = w_all[:, :2 * ff]
    w_o_all = w_all[:, 2 * ff:2 * ff + width]
    w_down_at = 2 * ff + width
    down_all = [w_all[:, w_down_at + i * width:w_down_at + (i + 1) * width].reshape(n_dev, rows, width) for i in range(len(down_groups))]
    w_down_all = jnp.concatenate(down_all, axis=1)[:, :ff_s].reshape(ff, width)
    me = lax.axis_index(SEQ_AXIS)
    w_cols = jnp.concatenate([lax.dynamic_slice(w_all, (0, at + me * ff_s), (width, ff_s)) for at in (0, ff)], axis=1)

    half = head_dim // 2
    inv_freq = ROPE_BASE ** (-(jnp.arange(half, dtype=F32) * (2.0 / head_dim)))
    angle_t = inv_freq[:, None] * pos_all.reshape(1, seq)
    cos_t, sin_t = jnp.cos(angle_t), jnp.sin(angle_t)

    q_t = (rope_t(proj_t[:head_dim], cos_t, sin_t).astype(BF16).astype(F32) * (head_dim ** -0.5)).astype(BF16)
    k_t = rope_t(proj_t[head_dim:2 * head_dim], cos_t, sin_t).astype(BF16)
    v_t = proj_t[2 * head_dim:].astype(BF16)
    k_in, v_in = k_t.T, v_t.T
    o_blocks, of_t, lse = attention_fwd(q_t, k_in, v_t, n_dev)
    o_loc = exchange(o_blocks).reshape(width, tok)
    w_parts = jnp.stack([w.reshape(rows, heads * head_dim) for w in (w_q, w_k, w_v)])
    o_loc, w_parts, v_in, w_down_all = lax.optimization_barrier((o_loc, w_parts, v_in, w_down_all))

    hidden = (x_act.astype(F32) + dot(o_loc, w_o_all, 0, 0)).astype(BF16)
    normed_mlp, inv_rms_mlp = rms_norm(hidden, g_mlp)
    a_dy = gather(jnp.concatenate([normed_mlp, grad_out], axis=1))
    pre = dot(normed_mlp, w_gu, 1, 0)
    gate_pre, up_pre = pre[:, :ff], pre[:, ff:]
    mixed = (jax.nn.silu(gate_pre) * up_pre).astype(BF16)
    y_out = (hidden.astype(F32) + dot(mixed, w_down_all, 1, 0)).astype(BF16)

    d_mixed = dot(grad_out, w_down_all, 1, 1).astype(BF16).astype(F32)
    d_gu = jnp.concatenate(gate_backward(d_mixed, gate_pre, up_pre), axis=1)
    d_normed = dot(d_gu, w_gu, 1, 1).astype(BF16)
    d_hid_norm, part_g_mlp = rms_norm_bwd(hidden, g_mlp, inv_rms_mlp, d_normed)
    d_hidden = (grad_out.astype(F32) + d_hid_norm).astype(BF16)
    do_blocks = exchange(dot(w_o_all, d_hidden, 1, 1).astype(BF16).reshape(n_dev, head_dim, tok))
    half_n = n_dev // 2
    pairs = [(i, (i + half_n) % n_dev) for i in range(n_dev)]
    near = (me // half_n) * half_n
    o_far = lax.ppermute(lax.dynamic_slice_in_dim(o_blocks, half_n - near, half_n), SEQ_AXIS, pairs)
    do_blocks, y_out = lax.optimization_barrier((do_blocks, y_out))
    dh_half = lax.all_gather(d_hidden, SEQ_AXIS, axis=0, tiled=True, axis_index_groups=[list(range(half_n)), list(range(half_n, n_dev))])

    do_t = jnp.transpose(do_blocks, (1, 0, 2)).reshape(head_dim, seq)
    d_blocks, d_proj_t, *w_qkv_all = attention_bwd(q_t, do_t, of_t, lse, k_in, k_t, v_in, cos_t, sin_t, w_parts, n_dev)
    d_proj = exchange(d_blocks)

    grad_w_qkv = lax.optimization_barrier(dot(d_proj_t, u_all, 1, 0)).T
    attn_send = grad_w_qkv.reshape(n_dev, rows, qkv)
    d_proj, attn_send = lax.optimization_barrier((d_proj, attn_send))
    attn_back = exchange(attn_send)

    a_dy, _ = lax.optimization_barrier((a_dy, d_proj_t))
    a_all, dy_all = a_dy[:, :width], a_dy[:, width:]
    pre_t = dot(w_cols, a_all, 0, 1)
    gate_t, up_t = pre_t[:ff_s], pre_t[ff_s:]
    d_mixed_t = dot(w_down, dy_all, 1, 1).astype(BF16).astype(F32)
    mixed_t = (jax.nn.silu(gate_t) * up_t).astype(BF16)
    d_gu_t = jnp.concatenate(gate_backward(d_mixed_t, gate_t, up_t), axis=0)
    mlp_send = dot(a_all, d_gu_t, 0, 1).reshape(n_dev, rows, 2 * ff_s)
    attn_back, mlp_send = lax.optimization_barrier((attn_back, mlp_send))
    mlp_back = exchange(mlp_send)
    mixed_t, mlp_send = lax.optimization_barrier((mixed_t, mlp_send))
    grad_w_down = dot(mixed_t, dy_all, 1, 0)

    d_proj, mlp_send = lax.optimization_barrier((d_proj, mlp_send))
    d_proj = d_proj.reshape(heads, 3, head_dim, tok)
    inv_rms = lax.rsqrt(jnp.mean(jnp.square(x_act.astype(F32)), axis=-1, keepdims=True) + RMS_EPS)
    d_u = sum(dot(d_proj[:, p].reshape(heads * head_dim, tok), w_qkv_all[p].reshape(width, heads * head_dim), 0, 1) for p in range(3)).astype(BF16)
    d_x_norm, part_g_attn = rms_norm_bwd(x_act, g_attn, inv_rms, d_u)
    grad_x = (d_hidden.astype(F32) + d_x_norm).astype(BF16)
    gain_send = jnp.pad(jnp.concatenate([part_g_attn.reshape(n_dev, 1, rows), part_g_mlp.reshape(n_dev, 1, rows)], axis=2), ((0, 0), (0, 7), (0, 0)))

    o_far, dh_half, o_blocks, gain_send = lax.optimization_barrier((o_far, dh_half, o_blocks, gain_send))
    o_pair = jnp.concatenate([lax.dynamic_slice_in_dim(o_blocks, near, half_n), o_far], axis=1)
    part_w_o = dot(o_pair.transpose(1, 0, 2).reshape(2 * head_dim, seq // 2), dh_half, 1, 0)
    grad_w_o = (part_w_o[:head_dim] + lax.ppermute(part_w_o[head_dim:], SEQ_AXIS, pairs))[None]

    grad_w_q, grad_w_k, grad_w_v = split_heads(attn_back, head_dim)
    mlp_back, gain_send, grad_w_down, grad_w_q, grad_w_k, grad_w_v, grad_w_o = lax.optimization_barrier((mlp_back, gain_send, grad_w_down, grad_w_q, grad_w_k, grad_w_v, grad_w_o))
    gains = jnp.sum(exchange(gain_send)[:, 0], axis=0)
    grad_g_attn, grad_g_mlp = gains[:rows], gains[rows:]
    grad_w_gate, grad_w_up = join_columns(mlp_back, ff_s)
    return (y_out, grad_x, grad_g_attn, grad_w_q, grad_w_k, grad_w_v, grad_w_o, grad_g_mlp, grad_w_gate, grad_w_up, grad_w_down)


def solution(mesh):
    n_dev = mesh.shape[SEQ_AXIS]
    token_spec = P(SEQ_AXIS, None)
    cube_spec = P(SEQ_AXIS, None, None)
    gain_spec = P(SEQ_AXIS)
    weight_specs = (gain_spec, cube_spec, cube_spec, cube_spec, cube_spec, gain_spec, token_spec, token_spec, token_spec)
    return jax.shard_map(lambda *args: device_step(n_dev, *args), mesh=mesh, in_specs=(token_spec, gain_spec, token_spec) + weight_specs, out_specs=(token_spec, token_spec) + weight_specs, check_vma=False)
```

```python
import jax
import jax.numpy as jnp
from jax import lax
from jax.experimental import pallas as pl
from jax.experimental.layout import Layout, with_layout_constraint
from jax.experimental.pallas import tpu as pltpu
from jax.sharding import PartitionSpec as P

SEQ_AXIS = 'sp'
RMS_EPS = 1e-5
ROPE_BASE = 10000.0
MASK_VALUE = -1e30
TILE = 512
F32 = jnp.float32
BF16 = jnp.bfloat16


def rms_norm(act_in, gain_vec):
    act_f = act_in.astype(F32)
    inv_rms = lax.rsqrt(jnp.mean(act_f * act_f, axis=-1, keepdims=True) + RMS_EPS)
    return (act_f * inv_rms * gain_vec.astype(F32)).astype(BF16), inv_rms


def rms_norm_bwd(act_in, gain_vec, inv_rms, d_normed):
    act_f = act_in.astype(F32)
    d_f = d_normed.astype(F32)
    scaled_d = d_f * gain_vec.astype(F32)
    proj_mean = jnp.mean(scaled_d * act_f, axis=-1, keepdims=True)
    d_act = inv_rms * scaled_d - act_f * (inv_rms * inv_rms * inv_rms) * proj_mean
    d_gain = jnp.sum(d_f * act_f * inv_rms, axis=0)
    return d_act, d_gain


def dot(lhs, rhs, l_dim, r_dim):
    return lax.dot_general(lhs, rhs, (((l_dim,), (r_dim,)), ((), ())), preferred_element_type=F32)


def gather(shard):
    return lax.all_gather(shard, SEQ_AXIS, axis=0, tiled=True)


def exchange(blocks):
    return lax.all_to_all(blocks, SEQ_AXIS, 0, 0, tiled=True)


def rope_t(vals, cos_tab, sin_tab):
    half = vals.shape[0] // 2
    first, second = vals[:half], vals[half:]
    return jnp.concatenate([first * cos_tab - second * sin_tab, second * cos_tab + first * sin_tab], axis=0)


def mm(lhs, rhs):
    return jnp.dot(lhs, rhs, preferred_element_type=F32)


def diag_mask(tile):
    key_at = lax.broadcasted_iota(jnp.int32, (tile, tile), 0)
    query_at = lax.broadcasted_iota(jnp.int32, (tile, tile), 1)
    return key_at <= query_at


def attn_fwd_kernel(tile, q_t, k_ref, v_t, o_ref, of_ref, lse_ref, s_buf):
    step = pl.program_id(0)
    query = q_t[...]

    def scores(j):
        return mm(k_ref[pl.ds(pl.multiple_of(j * tile, tile), tile), :], query)

    def keep(j, logits, top):
        s_buf[pl.ds(pl.multiple_of(j * tile, tile), tile), :] = logits
        return jnp.maximum(top, jnp.max(logits, axis=0, keepdims=True))

    top = keep(step, jnp.where(diag_mask(tile), scores(step), MASK_VALUE), jnp.full((1, tile), MASK_VALUE, F32))
    top = lax.fori_loop(0, step, lambda j, c: keep(j, scores(j), c), top)

    def weigh(j, carry):
        acc, total = carry
        at = pl.ds(pl.multiple_of(j * tile, tile), tile)
        prob = jnp.exp(s_buf[at, :] - top)
        return acc + mm(v_t[:, at], prob.astype(BF16)), total + jnp.sum(prob, axis=0, keepdims=True)

    out, total = lax.fori_loop(0, step + 1, weigh, (jnp.zeros((v_t.shape[0], tile), F32), jnp.zeros((1, tile), F32)))
    out = out / total
    lse = top + jnp.log(total)
    of_ref[...] = out
    lse_ref[...] = lse
    block = o_ref.shape[2]
    for part in range(tile // block):
        o_ref[part] = out[:, part * block:(part + 1) * block].astype(BF16)


def attention_fwd(q_t, k_in, v_t, n_blocks):
    head_dim, seq = q_t.shape
    block = seq // n_blocks
    per = TILE // block
    return pl.pallas_call(
        lambda *refs: attn_fwd_kernel(TILE, *refs),
        grid=(seq // TILE,),
        in_specs=[pl.BlockSpec((head_dim, TILE), lambda i: (0, i)), pl.BlockSpec((seq, head_dim), lambda i: (0, 0)), pl.BlockSpec((head_dim, seq), lambda i: (0, 0))],
        out_specs=[pl.BlockSpec((per, head_dim, block), lambda i: (i, 0, 0)), pl.BlockSpec((head_dim, TILE), lambda i: (0, i)), pl.BlockSpec((1, TILE), lambda i: (0, i))],
        out_shape=[jax.ShapeDtypeStruct((n_blocks, head_dim, block), BF16), jax.ShapeDtypeStruct((head_dim, seq), F32), jax.ShapeDtypeStruct((1, seq), F32)],
        scratch_shapes=[pltpu.VMEM((seq, TILE), F32)],
        cost_estimate=pl.CostEstimate(flops=8 * seq * seq * head_dim, bytes_accessed=8 * seq * head_dim, transcendentals=seq * seq),
        name='attn_fwd',
    )(q_t, k_in, v_t)


PARTS = ((0, 96), (96, 80), (176, 80))
CORE, CHIP_AXES = 1, (2, 4, 8)


def flip(dev, bit):
    return dev + bit * (1 - 2 * ((dev // bit) % 2))


def start_copy(src, dst, send_sem, recv_sem, peer):
    copy = pltpu.make_async_remote_copy(src_ref=src, dst_ref=dst, send_sem=send_sem, recv_sem=recv_sem, device_id=(peer,), device_id_type=pl.DeviceIdType.MESH)
    copy.start()
    return copy


def landed(ref, sem):
    pltpu.make_async_copy(ref, ref, sem).wait()


def enter_all(me, n_dev):
    barrier = pltpu.get_barrier_semaphore()

    @pl.loop(1, n_dev)
    def _(hop):
        pl.semaphore_signal(barrier, inc=1, device_id=(lax.rem(me + hop, n_dev),), device_id_type=pl.DeviceIdType.MESH)

    pl.semaphore_wait(barrier, n_dev - 1)


class CubeGather:
    def __init__(self, me, part, send_sem, recv_sem, core_sem):
        self.me, self.part = me, part
        self.send_sem, self.recv_sem, self.core_sem = send_sem, recv_sem, core_sem
        self.sent = []

    def axes(self, p):
        return [CHIP_AXES[(p + i) % 3] for i in range(3)]

    def owner(self, p, index, start=None):
        dev = self.me if start is None else start
        for i, bit in enumerate(self.axes(p)):
            if (index >> i) & 1:
                dev = flip(dev, bit)
        return dev

    def push(self, p, index, axis):
        ref = self.part(self.owner(p, index), p)
        start_copy(ref, ref, self.send_sem.at[len(self.sent)], self.recv_sem.at[p, index + (1 << axis)], flip(self.me, self.axes(p)[axis]))
        self.sent.append((p, index))

    def push_core(self, p, index):
        ref = self.part(self.owner(p, index), p)
        start_copy(ref, ref, self.send_sem.at[len(self.sent)], self.core_sem.at[p, index], flip(self.me, CORE))
        self.sent.append((p, index))

    def begin(self):
        for axis in range(3):
            for p in range(3):
                self.push(p, 0, axis)
        for p in range(3):
            self.push_core(p, 0)

    def receive(self, index):
        for p in range(3):
            landed(self.part(self.owner(p, index), p), self.recv_sem.at[p, index])
            for axis in range(index.bit_length(), 3):
                self.push(p, index, axis)
            self.push_core(p, index)

    def receive_core(self, index):
        for p in range(3):
            landed(self.part(self.owner(p, index, flip(self.me, CORE)), p), self.core_sem.at[p, index])

    def finish(self):
        for slot, (p, index) in enumerate(self.sent):
            landed(self.part(self.owner(p, index), p), self.send_sem.at[slot])


N_SENDS = 9 + 12 + 24


def attn_bwd_kernel(n_dev, tile, block, q_t, do_t, of_t, lse_ref, cos_ref, sin_ref, k_ref, k_t, v_ref, cos_all, sin_all, w_ref, d_blocks, d_proj_t, w_out_q, w_out_k, w_out_v, dq_acc, dk_acc, dv_acc, w_buf, send_sem, recv_sem, core_sem, local_sem):
    step = pl.program_id(0)
    last = pl.num_programs(0) - 1
    me = lax.axis_index(SEQ_AXIS)
    cube = CubeGather(me, lambda dev, p: w_buf.at[p, dev], send_sem, recv_sem, core_sem)

    @pl.when(step == 0)
    def _():
        own = [pltpu.make_async_copy(w_ref.at[p], w_buf.at[p, me], local_sem.at[p]) for p in range(3)]
        for copy in own:
            copy.start()
        enter_all(me, n_dev)
        for copy in own:
            copy.wait()
        cube.begin()

    for at_step, indices in ((4, (1,)), (5, (2,)), (6, (4,)), (7, (3,))):
        @pl.when(step == at_step)
        def _(indices=indices):
            for index in indices:
                cube.receive(index)

    head_dim = q_t.shape[0]
    query_t, d_out_t = q_t[...], do_t[...]
    lse = lse_ref[...]
    delta = jnp.sum(d_out_t.astype(F32) * of_t[...], axis=0, keepdims=True)

    @pl.when(step == 0)
    def _():
        dk_acc[...] = jnp.zeros_like(dk_acc)
        dv_acc[...] = jnp.zeros_like(dv_acc)

    dq_acc[...] = jnp.zeros_like(dq_acc)

    def visit(j, masked):
        at = pl.ds(pl.multiple_of(j * tile, tile), tile)
        prob = jnp.exp(mm(k_ref[at, :], query_t) - lse)
        if masked:
            prob = jnp.where(diag_mask(tile), prob, 0.0)
        d_prob = mm(v_ref[at, :], d_out_t).astype(BF16).astype(F32)
        d_logits = (prob * (d_prob - delta)).astype(BF16)
        dv_acc[:, at] += dot(d_out_t, prob.astype(BF16), 1, 1)
        dk_acc[:, at] += dot(query_t, d_logits, 1, 1)
        dq_acc[...] += mm(k_t[:, at], d_logits)

    visit(step, True)

    @pl.loop(0, step)
    def _(j):
        visit(j, False)

    def put(row, col_block, values):
        rows = slice(row, row + values.shape[0])
        d_proj_t[rows, pl.ds(pl.multiple_of(col_block * block, block), values.shape[1])] = values
        for part in range(values.shape[1] // block):
            d_blocks[col_block + part, rows, :] = values[:, part * block:(part + 1) * block]

    d_q = (dq_acc[...] * (head_dim ** -0.5)).astype(BF16).astype(F32)
    per = tile // block
    put(0, step * per, rope_t(d_q, cos_ref[...], -sin_ref[...]).astype(BF16))

    @pl.when(step == last)
    def _():
        @pl.loop(0, pl.num_programs(0))
        def _(j):
            at = pl.ds(pl.multiple_of(j * tile, tile), tile)
            put(head_dim, j * per, rope_t(dk_acc[:, at].astype(BF16).astype(F32), cos_all[:, at], -sin_all[:, at]).astype(BF16))
            put(2 * head_dim, j * per, dv_acc[:, at].astype(BF16))

        for index in (5, 6, 7):
            cube.receive(index)
        for index in range(8):
            cube.receive_core(index)
        flushes = [pltpu.make_async_copy(w_buf.at[p], out, local_sem.at[p]) for p, out in enumerate((w_out_q, w_out_k, w_out_v))]
        for flush in flushes:
            flush.start()
        cube.finish()
        for flush in flushes:
            flush.wait()


def attention_bwd(q_t, do_t, of_t, lse, k_in, k_t, v_in, cos_t, sin_t, w_parts, n_blocks):
    head_dim, seq = q_t.shape
    block = seq // n_blocks
    cols = pl.BlockSpec((head_dim, TILE), lambda i: (0, i))
    half_cols = pl.BlockSpec((head_dim // 2, TILE), lambda i: (0, i))
    all_rows = pl.BlockSpec((seq, head_dim), lambda i: (0, 0))
    all_cols = pl.BlockSpec((head_dim, seq), lambda i: (0, 0))
    all_half = pl.BlockSpec((head_dim // 2, seq), lambda i: (0, 0))
    w_all_shape = (3, n_blocks) + w_parts.shape[1:]
    return pl.pallas_call(
        lambda *refs: attn_bwd_kernel(n_blocks, TILE, block, *refs),
        grid=(seq // TILE,),
        in_specs=[cols, cols, cols, pl.BlockSpec((1, TILE), lambda i: (0, i)), half_cols, half_cols, all_rows, all_cols, all_rows, all_half, all_half, pl.BlockSpec(memory_space=pl.ANY)],
        out_specs=[pl.BlockSpec((n_blocks, 3 * head_dim, block), lambda i: (0, 0, 0)), pl.BlockSpec((3 * head_dim, seq), lambda i: (0, 0))] + [pl.BlockSpec(memory_space=pl.ANY)] * 3,
        out_shape=[jax.ShapeDtypeStruct((n_blocks, 3 * head_dim, block), BF16), jax.ShapeDtypeStruct((3 * head_dim, seq), BF16)] + [jax.ShapeDtypeStruct(w_all_shape[1:], BF16)] * 3,
        scratch_shapes=[
            pltpu.VMEM((head_dim, TILE), F32),
            pltpu.VMEM((head_dim, seq), F32),
            pltpu.VMEM((head_dim, seq), F32),
            pltpu.VMEM(w_all_shape, BF16),
            pltpu.SemaphoreType.DMA((N_SENDS,)),
            pltpu.SemaphoreType.DMA((3, 8)),
            pltpu.SemaphoreType.DMA((3, 8)),
            pltpu.SemaphoreType.DMA((3,)),
        ],
        compiler_params=pltpu.CompilerParams(collective_id=1, has_side_effects=True),
        cost_estimate=pl.CostEstimate(flops=20 * seq * seq * head_dim, bytes_accessed=20 * seq * head_dim, transcendentals=seq * seq),
        name='attn_bwd',
    )(q_t, do_t, of_t, lse, cos_t, sin_t, k_in, k_t, v_in, cos_t, sin_t, w_parts)


def gather_proj_kernel(n_dev, x_ref, small_ref, w_ref, u_out, proj_t, small_all, x_buf, u_buf, w_buf, send_sem, recv_sem, core_sem, misc_send, misc_recv, local_sem, u_sem):
    me = lax.axis_index(SEQ_AXIS)
    own = pltpu.make_async_copy(x_ref, x_buf.at[me], local_sem.at[0])
    own.start()
    own_w = pltpu.make_async_copy(w_ref.at[me], w_buf.at[me], local_sem.at[1])
    own_w.start()
    own_small = pltpu.make_async_copy(small_ref, small_all.at[me], local_sem.at[2])
    own_small.start()
    enter_all(me, n_dev)
    own.wait()
    cube = CubeGather(me, lambda dev, p: x_buf.at[dev, pl.ds(PARTS[p][0], PARTS[p][1])], send_sem, recv_sem, core_sem)
    cube.begin()

    def spread(hop):
        peer = lax.rem(me + hop, n_dev)
        return [
            pltpu.make_async_remote_copy(src_ref=small_ref, dst_ref=small_all.at[me], send_sem=misc_send.at[0, hop], recv_sem=misc_recv.at[0, me], device_id=(peer,), device_id_type=pl.DeviceIdType.MESH),
            pltpu.make_async_remote_copy(src_ref=w_ref.at[peer], dst_ref=w_buf.at[me], send_sem=misc_send.at[1, hop], recv_sem=misc_recv.at[1, me], device_id=(peer,), device_id_type=pl.DeviceIdType.MESH),
        ]

    for kind in range(2):
        @pl.loop(1, n_dev)
        def _(hop, kind=kind):
            spread(hop)[kind].start()

    cube.receive(1)
    cube.receive(2)
    own_w.wait()
    own_small.wait()

    @pl.loop(1, n_dev)
    def _(hop):
        src = lax.rem(me + hop, n_dev)
        landed(small_all.at[src], misc_recv.at[0, src])
        landed(w_buf.at[src], misc_recv.at[1, src])

    width = x_ref.shape[1]
    tok = x_ref.shape[0]
    rows = w_ref.shape[1]
    gain = jnp.concatenate([small_all[d, 0:1, 0:rows] for d in range(n_dev)], axis=1)
    weight = w_buf[...].reshape(width, w_ref.shape[2])
    keep = proj_t.shape[0]
    flushes = []

    def project(dev):
        act = x_buf[dev].astype(F32)
        inv = lax.rsqrt(jnp.mean(act * act, axis=-1, keepdims=True) + RMS_EPS)
        normed = (act * inv * gain).astype(BF16)
        u_buf[dev] = normed
        proj_t[:, pl.ds(pl.multiple_of(dev * tok, tok), tok)] = mm(normed, weight).T[:keep]
        flush = pltpu.make_async_copy(u_buf.at[dev], u_out.at[dev], u_sem.at[len(flushes)])
        flush.start()
        flushes.append(flush)

    other = flip(me, CORE)
    cube.receive_core(0)
    project(me)
    project(other)
    cube.receive(4)
    cube.receive(3)
    for index in (1, 2, 4):
        cube.receive_core(index)
    for bit in CHIP_AXES:
        project(flip(me, bit))
        project(flip(other, bit))
    cube.receive(5)
    cube.receive(6)
    for index in (3, 5, 6):
        cube.receive_core(index)
    for skip in range(3):
        bits = [bit for i, bit in enumerate(CHIP_AXES) if i != skip]
        project(flip(flip(me, bits[0]), bits[1]))
        project(flip(flip(other, bits[0]), bits[1]))
    cube.receive(7)
    cube.receive_core(7)
    far = flip(flip(flip(me, 2), 4), 8)
    project(far)
    project(flip(far, CORE))

    cube.finish()

    @pl.loop(1, n_dev)
    def _(hop):
        for copy in spread(hop):
            copy.wait_send()

    for flush in flushes:
        flush.wait()


def gather_proj(n_dev, x_act, small, w_blocks, qkv):
    tok, width = x_act.shape
    seq = tok * n_dev
    any_spec = pl.BlockSpec(memory_space=pl.ANY)
    vmem_spec = pl.BlockSpec(memory_space=pltpu.VMEM)
    return pl.pallas_call(
        lambda *refs: gather_proj_kernel(n_dev, *refs),
        in_specs=[any_spec, vmem_spec, vmem_spec],
        out_specs=[any_spec, vmem_spec, vmem_spec],
        out_shape=[jax.ShapeDtypeStruct((n_dev, tok, width), BF16), jax.ShapeDtypeStruct((qkv, seq), F32), jax.ShapeDtypeStruct((n_dev,) + small.shape, F32)],
        scratch_shapes=[
            pltpu.VMEM((n_dev, tok, width), BF16),
            pltpu.VMEM((n_dev, tok, width), BF16),
            pltpu.VMEM(w_blocks.shape, BF16),
            pltpu.SemaphoreType.DMA((N_SENDS,)),
            pltpu.SemaphoreType.DMA((3, 8)),
            pltpu.SemaphoreType.DMA((3, 8)),
            pltpu.SemaphoreType.DMA((2, n_dev)),
            pltpu.SemaphoreType.DMA((2, n_dev)),
            pltpu.SemaphoreType.DMA((3,)),
            pltpu.SemaphoreType.DMA((n_dev,)),
        ],
        compiler_params=pltpu.CompilerParams(collective_id=0, has_side_effects=True),
        cost_estimate=pl.CostEstimate(flops=30 * seq * width * width, bytes_accessed=4 * seq * width, transcendentals=0),
        name='gather_proj',
    )(x_act, small, w_blocks)


def gate_backward(d_mixed, gate_pre, up_pre):
    gate_sig = jax.nn.sigmoid(gate_pre)
    d_up = (d_mixed * gate_pre * gate_sig).astype(BF16)
    d_gate = (d_mixed * up_pre * gate_sig * (1.0 + gate_pre * (1.0 - gate_sig))).astype(BF16)
    return d_gate, d_up


def join_columns_kernel(size, src, first, second):
    for i, out in enumerate((first, second)):
        out[...] = jnp.concatenate([src[d, :, i * size:(i + 1) * size] for d in range(src.shape[0])], axis=1)


def join_columns(blocks, size):
    shape = jax.ShapeDtypeStruct((blocks.shape[1], blocks.shape[0] * size), F32)
    return pl.pallas_call(lambda *refs: join_columns_kernel(size, *refs), out_shape=[shape, shape], name='join_columns')(blocks)


def split_heads_kernel(head_dim, src, *outs):
    for i, out in enumerate(outs):
        for d in range(src.shape[0]):
            out[:, d, :] = src[d, :, i * head_dim:(i + 1) * head_dim]


def split_heads(blocks, head_dim):
    shape = jax.ShapeDtypeStruct((blocks.shape[1], blocks.shape[0], head_dim), F32)
    return pl.pallas_call(lambda *refs: split_heads_kernel(head_dim, *refs), out_shape=[shape] * 3, name='split_heads')(blocks)


def device_step(n_dev, x_act, positions, grad_out, g_attn_s, w_q, w_k, w_v, w_o, g_mlp_s, w_gate, w_up, w_down):
    tok, width = x_act.shape
    seq = tok * n_dev
    rows, heads, head_dim = w_q.shape
    ff = w_gate.shape[1]
    ff_s = ff // n_dev
    qkv = 3 * head_dim

    small = jnp.concatenate([jnp.concatenate([g_attn_s, g_mlp_s]).astype(F32)[None], positions.astype(F32).reshape(-1, 2 * rows)], axis=0)
    small = jnp.pad(small, ((0, 8 - small.shape[0]), (0, 0)))
    w_qkv = jnp.concatenate([w_q, w_k, w_v], axis=2)
    w_blocks = jnp.pad(jnp.transpose(w_qkv, (1, 0, 2)), ((0, 0), (0, 0), (0, 256 - qkv)))
    u_all, proj_t, small_all = gather_proj(n_dev, x_act, small, w_blocks, qkv)
    u_all = u_all.reshape(seq, width)
    g_attn = small_all[:, 0, :rows].reshape(width)
    g_mlp = small_all[:, 0, rows:2 * rows].reshape(width)
    pos_all = small_all[:, 1:1 + tok // (2 * rows)]

    down_groups = [w_down[i:i + rows] for i in range(0, ff_s, rows)]
    down_groups = [jnp.pad(group, ((0, rows - group.shape[0]), (0, 0))) for group in down_groups]
    w_all = gather(jnp.concatenate([w_gate, w_up, w_o[0]] + down_groups, axis=1))
    w_gu = w_all[:, :2 * ff]
    w_o_all = w_all[:, 2 * ff:2 * ff + width]
    w_down_at = 2 * ff + width
    down_all = [w_all[:, w_down_at + i * width:w_down_at + (i + 1) * width].reshape(n_dev, rows, width) for i in range(len(down_groups))]
    w_down_all = jnp.concatenate(down_all, axis=1)[:, :ff_s].reshape(ff, width)
    me = lax.axis_index(SEQ_AXIS)
    w_cols = jnp.concatenate([lax.dynamic_slice(w_all, (0, at + me * ff_s), (width, ff_s)) for at in (0, ff)], axis=1)

    half = head_dim // 2
    inv_freq = ROPE_BASE ** (-(jnp.arange(half, dtype=F32) * (2.0 / head_dim)))
    angle_t = inv_freq[:, None] * pos_all.reshape(1, seq)
    cos_t, sin_t = jnp.cos(angle_t), jnp.sin(angle_t)

    q_t = (rope_t(proj_t[:head_dim], cos_t, sin_t).astype(BF16).astype(F32) * (head_dim ** -0.5)).astype(BF16)
    k_t = rope_t(proj_t[head_dim:2 * head_dim], cos_t, sin_t).astype(BF16)
    v_t = proj_t[2 * head_dim:].astype(BF16)
    k_in, v_in = k_t.T, v_t.T
    o_blocks, of_t, lse = attention_fwd(q_t, k_in, v_t, n_dev)
    o_loc = exchange(o_blocks).reshape(width, tok)
    w_parts = jnp.stack([w.reshape(rows, heads * head_dim) for w in (w_q, w_k, w_v)])
    o_loc, w_parts, v_in, w_down_all = lax.optimization_barrier((o_loc, w_parts, v_in, w_down_all))

    hidden = (x_act.astype(F32) + dot(o_loc, w_o_all, 0, 0)).astype(BF16)
    normed_mlp, inv_rms_mlp = rms_norm(hidden, g_mlp)
    a_dy = jnp.concatenate([normed_mlp, grad_out], axis=1)
    normed_mlp, a_dy = lax.optimization_barrier((normed_mlp, a_dy))
    a_dy = gather(a_dy)
    pre = with_layout_constraint(dot(normed_mlp, w_gu, 1, 0), Layout(major_to_minor=(0, 1)))
    gate_pre, up_pre = pre[:, :ff], pre[:, ff:]
    mixed = (jax.nn.silu(gate_pre) * up_pre).astype(BF16)
    y_out = (hidden.astype(F32) + dot(mixed, w_down_all, 1, 0)).astype(BF16)

    d_mixed = dot(grad_out, w_down_all, 1, 1).astype(BF16).astype(F32)
    d_gu = jnp.concatenate(gate_backward(d_mixed, gate_pre, up_pre), axis=1)
    d_normed = dot(d_gu, w_gu, 1, 1).astype(BF16)
    d_hid_norm, part_g_mlp = rms_norm_bwd(hidden, g_mlp, inv_rms_mlp, d_normed)
    d_hidden = (grad_out.astype(F32) + d_hid_norm).astype(BF16)
    do_blocks = exchange(dot(w_o_all, d_hidden, 1, 1).astype(BF16).reshape(n_dev, head_dim, tok))
    half_n = n_dev // 2
    pairs = [(i, (i + half_n) % n_dev) for i in range(n_dev)]
    near = (me // half_n) * half_n
    o_far = lax.ppermute(lax.dynamic_slice_in_dim(o_blocks, half_n - near, half_n), SEQ_AXIS, pairs)
    do_blocks, y_out = lax.optimization_barrier((do_blocks, y_out))
    dh_half = lax.all_gather(d_hidden, SEQ_AXIS, axis=0, tiled=True, axis_index_groups=[list(range(half_n)), list(range(half_n, n_dev))])

    do_t = jnp.transpose(do_blocks, (1, 0, 2)).reshape(head_dim, seq)
    d_blocks, d_proj_t, *w_qkv_all = attention_bwd(q_t, do_t, of_t, lse, k_in, k_t, v_in, cos_t, sin_t, w_parts, n_dev)
    d_proj = exchange(d_blocks)

    grad_w_qkv = lax.optimization_barrier(dot(d_proj_t, u_all, 1, 0)).T
    attn_send = grad_w_qkv.reshape(n_dev, rows, qkv)
    d_proj, attn_send = lax.optimization_barrier((d_proj, attn_send))
    attn_back = exchange(attn_send)

    a_dy, _ = lax.optimization_barrier((a_dy, d_proj_t))
    a_all, dy_all = a_dy[:, :width], a_dy[:, width:]
    pre_t = dot(w_cols, a_all, 0, 1)
    gate_t, up_t = pre_t[:ff_s], pre_t[ff_s:]
    d_mixed_t = dot(w_down, dy_all, 1, 1).astype(BF16).astype(F32)
    mixed_t = (jax.nn.silu(gate_t) * up_t).astype(BF16)
    d_gu_t = jnp.concatenate(gate_backward(d_mixed_t, gate_t, up_t), axis=0)
    mlp_send = dot(a_all, d_gu_t, 0, 1).reshape(n_dev, rows, 2 * ff_s)
    attn_back, mlp_send = lax.optimization_barrier((attn_back, mlp_send))
    mlp_back = exchange(mlp_send)
    mixed_t, mlp_send = lax.optimization_barrier((mixed_t, mlp_send))
    grad_w_down = dot(mixed_t, dy_all, 1, 0)

    d_proj, mlp_send = lax.optimization_barrier((d_proj, mlp_send))
    d_proj = d_proj.reshape(heads, 3, head_dim, tok)
    inv_rms = lax.rsqrt(jnp.mean(jnp.square(x_act.astype(F32)), axis=-1, keepdims=True) + RMS_EPS)
    d_u = sum(dot(d_proj[:, p].reshape(heads * head_dim, tok), w_qkv_all[p].reshape(width, heads * head_dim), 0, 1) for p in range(3)).astype(BF16)
    d_x_norm, part_g_attn = rms_norm_bwd(x_act, g_attn, inv_rms, d_u)
    grad_x = (d_hidden.astype(F32) + d_x_norm).astype(BF16)
    gain_send = jnp.pad(jnp.concatenate([part_g_attn.reshape(n_dev, 1, rows), part_g_mlp.reshape(n_dev, 1, rows)], axis=2), ((0, 0), (0, 7), (0, 0)))

    o_far, dh_half, o_blocks, grad_w_down = lax.optimization_barrier((o_far, dh_half, o_blocks, grad_w_down))
    o_pair = jnp.concatenate([lax.dynamic_slice_in_dim(o_blocks, near, half_n), o_far], axis=1)
    part_w_o = dot(o_pair.transpose(1, 0, 2).reshape(2 * head_dim, seq // 2), dh_half, 1, 0)
    grad_w_o = (part_w_o[:head_dim] + lax.ppermute(part_w_o[head_dim:], SEQ_AXIS, pairs))[None]

    grad_w_q, grad_w_k, grad_w_v = split_heads(attn_back, head_dim)
    mlp_back, gain_send, grad_w_down, grad_w_q, grad_w_k, grad_w_v, grad_w_o = lax.optimization_barrier((mlp_back, gain_send, grad_w_down, grad_w_q, grad_w_k, grad_w_v, grad_w_o))
    gains = jnp.sum(exchange(gain_send)[:, 0], axis=0)
    grad_g_attn, grad_g_mlp = gains[:rows], gains[rows:]
    grad_w_gate, grad_w_up = join_columns(mlp_back, ff_s)
    return (y_out, grad_x, grad_g_attn, grad_w_q, grad_w_k, grad_w_v, grad_w_o, grad_g_mlp, grad_w_gate, grad_w_up, grad_w_down)


def solution(mesh):
    n_dev = mesh.shape[SEQ_AXIS]
    token_spec = P(SEQ_AXIS, None)
    cube_spec = P(SEQ_AXIS, None, None)
    gain_spec = P(SEQ_AXIS)
    weight_specs = (gain_spec, cube_spec, cube_spec, cube_spec, cube_spec, gain_spec, token_spec, token_spec, token_spec)
    return jax.shard_map(lambda *args: device_step(n_dev, *args), mesh=mesh, in_specs=(token_spec, gain_spec, token_spec) + weight_specs, out_specs=(token_spec, token_spec) + weight_specs, check_vma=False)
```

```python
import jax
import jax.numpy as jnp
from jax import lax
from jax.experimental import pallas as pl
from jax.experimental.layout import Layout, with_layout_constraint
from jax.experimental.pallas import tpu as pltpu
from jax.sharding import PartitionSpec as P

SEQ_AXIS = 'sp'
RMS_EPS = 1e-5
ROPE_BASE = 10000.0
MASK_VALUE = -1e30
TILE = 512
F32 = jnp.float32
BF16 = jnp.bfloat16


def rms_norm(act_in, gain_vec):
    act_f = act_in.astype(F32)
    inv_rms = lax.rsqrt(jnp.mean(act_f * act_f, axis=-1, keepdims=True) + RMS_EPS)
    return (act_f * inv_rms * gain_vec.astype(F32)).astype(BF16), inv_rms


def rms_norm_bwd(act_in, gain_vec, inv_rms, d_normed):
    act_f = act_in.astype(F32)
    d_f = d_normed.astype(F32)
    scaled_d = d_f * gain_vec.astype(F32)
    proj_mean = jnp.mean(scaled_d * act_f, axis=-1, keepdims=True)
    d_act = inv_rms * scaled_d - act_f * (inv_rms * inv_rms * inv_rms) * proj_mean
    d_gain = jnp.sum(d_f * act_f * inv_rms, axis=0)
    return d_act, d_gain


def dot(lhs, rhs, l_dim, r_dim):
    return lax.dot_general(lhs, rhs, (((l_dim,), (r_dim,)), ((), ())), preferred_element_type=F32)


def gather(shard):
    return lax.all_gather(shard, SEQ_AXIS, axis=0, tiled=True)


def exchange(blocks):
    return lax.all_to_all(blocks, SEQ_AXIS, 0, 0, tiled=True)


def rope_t(vals, cos_tab, sin_tab):
    half = vals.shape[0] // 2
    first, second = vals[:half], vals[half:]
    return jnp.concatenate([first * cos_tab - second * sin_tab, second * cos_tab + first * sin_tab], axis=0)


def mm(lhs, rhs):
    return jnp.dot(lhs, rhs, preferred_element_type=F32)


def diag_mask(tile):
    key_at = lax.broadcasted_iota(jnp.int32, (tile, tile), 0)
    query_at = lax.broadcasted_iota(jnp.int32, (tile, tile), 1)
    return key_at <= query_at


def attn_fwd_kernel(tile, q_t, k_ref, v_t, o_ref, of_ref, lse_ref, s_buf):
    step = pl.program_id(0)
    query = q_t[...]

    def scores(j):
        return mm(k_ref[pl.ds(pl.multiple_of(j * tile, tile), tile), :], query)

    def keep(j, logits, top):
        s_buf[pl.ds(pl.multiple_of(j * tile, tile), tile), :] = logits
        return jnp.maximum(top, jnp.max(logits, axis=0, keepdims=True))

    top = keep(step, jnp.where(diag_mask(tile), scores(step), MASK_VALUE), jnp.full((1, tile), MASK_VALUE, F32))
    top = lax.fori_loop(0, step, lambda j, c: keep(j, scores(j), c), top)

    def weigh(j, carry):
        acc, total = carry
        at = pl.ds(pl.multiple_of(j * tile, tile), tile)
        prob = jnp.exp(s_buf[at, :] - top)
        return acc + mm(v_t[:, at], prob.astype(BF16)), total + jnp.sum(prob, axis=0, keepdims=True)

    out, total = lax.fori_loop(0, step + 1, weigh, (jnp.zeros((v_t.shape[0], tile), F32), jnp.zeros((1, tile), F32)))
    out = out / total
    lse = top + jnp.log(total)
    of_ref[...] = out
    lse_ref[...] = lse
    block = o_ref.shape[2]
    for part in range(tile // block):
        o_ref[part] = out[:, part * block:(part + 1) * block].astype(BF16)


def attention_fwd(q_t, k_in, v_t, n_blocks):
    head_dim, seq = q_t.shape
    block = seq // n_blocks
    per = TILE // block
    return pl.pallas_call(
        lambda *refs: attn_fwd_kernel(TILE, *refs),
        grid=(seq // TILE,),
        in_specs=[pl.BlockSpec((head_dim, TILE), lambda i: (0, i)), pl.BlockSpec((seq, head_dim), lambda i: (0, 0)), pl.BlockSpec((head_dim, seq), lambda i: (0, 0))],
        out_specs=[pl.BlockSpec((per, head_dim, block), lambda i: (i, 0, 0)), pl.BlockSpec((head_dim, TILE), lambda i: (0, i)), pl.BlockSpec((1, TILE), lambda i: (0, i))],
        out_shape=[jax.ShapeDtypeStruct((n_blocks, head_dim, block), BF16), jax.ShapeDtypeStruct((head_dim, seq), F32), jax.ShapeDtypeStruct((1, seq), F32)],
        scratch_shapes=[pltpu.VMEM((seq, TILE), F32)],
        cost_estimate=pl.CostEstimate(flops=8 * seq * seq * head_dim, bytes_accessed=8 * seq * head_dim, transcendentals=seq * seq),
        name='attn_fwd',
    )(q_t, k_in, v_t)


PARTS = ((0, 96), (96, 80), (176, 80))
CORE, CHIP_AXES = 1, (2, 4, 8)


def flip(dev, bit):
    return dev + bit * (1 - 2 * ((dev // bit) % 2))


def start_copy(src, dst, send_sem, recv_sem, peer):
    copy = pltpu.make_async_remote_copy(src_ref=src, dst_ref=dst, send_sem=send_sem, recv_sem=recv_sem, device_id=(peer,), device_id_type=pl.DeviceIdType.MESH)
    copy.start()
    return copy


def landed(ref, sem):
    pltpu.make_async_copy(ref, ref, sem).wait()


def enter_all(me, n_dev):
    barrier = pltpu.get_barrier_semaphore()

    @pl.loop(1, n_dev)
    def _(hop):
        pl.semaphore_signal(barrier, inc=1, device_id=(lax.rem(me + hop, n_dev),), device_id_type=pl.DeviceIdType.MESH)

    pl.semaphore_wait(barrier, n_dev - 1)


class CubeGather:
    def __init__(self, me, part, send_sem, recv_sem, core_sem):
        self.me, self.part = me, part
        self.send_sem, self.recv_sem, self.core_sem = send_sem, recv_sem, core_sem
        self.sent = []

    def axes(self, p):
        return [CHIP_AXES[(p + i) % 3] for i in range(3)]

    def owner(self, p, index, start=None):
        dev = self.me if start is None else start
        for i, bit in enumerate(self.axes(p)):
            if (index >> i) & 1:
                dev = flip(dev, bit)
        return dev

    def push(self, p, index, axis):
        ref = self.part(self.owner(p, index), p)
        start_copy(ref, ref, self.send_sem.at[len(self.sent)], self.recv_sem.at[p, index + (1 << axis)], flip(self.me, self.axes(p)[axis]))
        self.sent.append((p, index))

    def push_core(self, p, index):
        ref = self.part(self.owner(p, index), p)
        start_copy(ref, ref, self.send_sem.at[len(self.sent)], self.core_sem.at[p, index], flip(self.me, CORE))
        self.sent.append((p, index))

    def begin(self):
        for axis in range(3):
            for p in range(3):
                self.push(p, 0, axis)
        for p in range(3):
            self.push_core(p, 0)

    def receive(self, index):
        for p in range(3):
            landed(self.part(self.owner(p, index), p), self.recv_sem.at[p, index])
            for axis in range(index.bit_length(), 3):
                self.push(p, index, axis)
            self.push_core(p, index)

    def receive_core(self, index):
        for p in range(3):
            landed(self.part(self.owner(p, index, flip(self.me, CORE)), p), self.core_sem.at[p, index])

    def finish(self):
        for slot, (p, index) in enumerate(self.sent):
            landed(self.part(self.owner(p, index), p), self.send_sem.at[slot])


N_SENDS = 9 + 12 + 24


def attn_bwd_kernel(n_dev, tile, block, q_t, do_t, of_t, lse_ref, cos_ref, sin_ref, k_ref, k_t, v_ref, cos_all, sin_all, w_ref, d_blocks, d_proj_t, w_out_q, w_out_k, w_out_v, dq_acc, dk_acc, dv_acc, w_buf, send_sem, recv_sem, core_sem, local_sem):
    step = pl.program_id(0)
    last = pl.num_programs(0) - 1
    me = lax.axis_index(SEQ_AXIS)
    cube = CubeGather(me, lambda dev, p: w_buf.at[p, dev], send_sem, recv_sem, core_sem)

    @pl.when(step == 0)
    def _():
        own = [pltpu.make_async_copy(w_ref.at[p], w_buf.at[p, me], local_sem.at[p]) for p in range(3)]
        for copy in own:
            copy.start()
        enter_all(me, n_dev)
        for copy in own:
            copy.wait()
        cube.begin()

    for at_step, indices in ((4, (1,)), (5, (2,)), (6, (4,)), (7, (3,))):
        @pl.when(step == at_step)
        def _(indices=indices):
            for index in indices:
                cube.receive(index)

    head_dim = q_t.shape[0]
    query_t, d_out_t = q_t[...], do_t[...]
    lse = lse_ref[...]
    delta = jnp.sum(d_out_t.astype(F32) * of_t[...], axis=0, keepdims=True)

    @pl.when(step == 0)
    def _():
        dk_acc[...] = jnp.zeros_like(dk_acc)
        dv_acc[...] = jnp.zeros_like(dv_acc)

    dq_acc[...] = jnp.zeros_like(dq_acc)

    def visit(j, masked):
        at = pl.ds(pl.multiple_of(j * tile, tile), tile)
        prob = jnp.exp(mm(k_ref[at, :], query_t) - lse)
        if masked:
            prob = jnp.where(diag_mask(tile), prob, 0.0)
        d_prob = mm(v_ref[at, :], d_out_t).astype(BF16).astype(F32)
        d_logits = (prob * (d_prob - delta)).astype(BF16)
        dv_acc[:, at] += dot(d_out_t, prob.astype(BF16), 1, 1)
        dk_acc[:, at] += dot(query_t, d_logits, 1, 1)
        dq_acc[...] += mm(k_t[:, at], d_logits)

    visit(step, True)

    @pl.loop(0, step)
    def _(j):
        visit(j, False)

    def put(row, col_block, values):
        rows = slice(row, row + values.shape[0])
        d_proj_t[rows, pl.ds(pl.multiple_of(col_block * block, block), values.shape[1])] = values
        for part in range(values.shape[1] // block):
            d_blocks[col_block + part, rows, :] = values[:, part * block:(part + 1) * block]

    d_q = (dq_acc[...] * (head_dim ** -0.5)).astype(BF16).astype(F32)
    per = tile // block
    put(0, step * per, rope_t(d_q, cos_ref[...], -sin_ref[...]).astype(BF16))

    @pl.when(step == last)
    def _():
        @pl.loop(0, pl.num_programs(0))
        def _(j):
            at = pl.ds(pl.multiple_of(j * tile, tile), tile)
            put(head_dim, j * per, rope_t(dk_acc[:, at].astype(BF16).astype(F32), cos_all[:, at], -sin_all[:, at]).astype(BF16))
            put(2 * head_dim, j * per, dv_acc[:, at].astype(BF16))

        for index in (5, 6, 7):
            cube.receive(index)
        for index in range(8):
            cube.receive_core(index)
        flushes = [pltpu.make_async_copy(w_buf.at[p], out, local_sem.at[p]) for p, out in enumerate((w_out_q, w_out_k, w_out_v))]
        for flush in flushes:
            flush.start()
        cube.finish()
        for flush in flushes:
            flush.wait()


def attention_bwd(q_t, do_t, of_t, lse, k_in, k_t, v_in, cos_t, sin_t, w_parts, n_blocks):
    head_dim, seq = q_t.shape
    block = seq // n_blocks
    cols = pl.BlockSpec((head_dim, TILE), lambda i: (0, i))
    half_cols = pl.BlockSpec((head_dim // 2, TILE), lambda i: (0, i))
    all_rows = pl.BlockSpec((seq, head_dim), lambda i: (0, 0))
    all_cols = pl.BlockSpec((head_dim, seq), lambda i: (0, 0))
    all_half = pl.BlockSpec((head_dim // 2, seq), lambda i: (0, 0))
    w_all_shape = (3, n_blocks) + w_parts.shape[1:]
    return pl.pallas_call(
        lambda *refs: attn_bwd_kernel(n_blocks, TILE, block, *refs),
        grid=(seq // TILE,),
        in_specs=[cols, cols, cols, pl.BlockSpec((1, TILE), lambda i: (0, i)), half_cols, half_cols, all_rows, all_cols, all_rows, all_half, all_half, pl.BlockSpec(memory_space=pl.ANY)],
        out_specs=[pl.BlockSpec((n_blocks, 3 * head_dim, block), lambda i: (0, 0, 0)), pl.BlockSpec((3 * head_dim, seq), lambda i: (0, 0))] + [pl.BlockSpec(memory_space=pl.ANY)] * 3,
        out_shape=[jax.ShapeDtypeStruct((n_blocks, 3 * head_dim, block), BF16), jax.ShapeDtypeStruct((3 * head_dim, seq), BF16)] + [jax.ShapeDtypeStruct(w_all_shape[1:], BF16)] * 3,
        scratch_shapes=[
            pltpu.VMEM((head_dim, TILE), F32),
            pltpu.VMEM((head_dim, seq), F32),
            pltpu.VMEM((head_dim, seq), F32),
            pltpu.VMEM(w_all_shape, BF16),
            pltpu.SemaphoreType.DMA((N_SENDS,)),
            pltpu.SemaphoreType.DMA((3, 8)),
            pltpu.SemaphoreType.DMA((3, 8)),
            pltpu.SemaphoreType.DMA((3,)),
        ],
        compiler_params=pltpu.CompilerParams(collective_id=1, has_side_effects=True),
        cost_estimate=pl.CostEstimate(flops=20 * seq * seq * head_dim, bytes_accessed=20 * seq * head_dim, transcendentals=seq * seq),
        name='attn_bwd',
    )(q_t, do_t, of_t, lse, cos_t, sin_t, k_in, k_t, v_in, cos_t, sin_t, w_parts)


def gather_proj_kernel(n_dev, x_ref, small_ref, w_ref, freq_ref, u_out, q_t, k_t, v_t, k_out, v_out, cos_ref, sin_ref, small_all, x_buf, u_buf, w_buf, send_sem, recv_sem, core_sem, misc_send, misc_recv, local_sem, u_sem):
    me = lax.axis_index(SEQ_AXIS)
    own = pltpu.make_async_copy(x_ref, x_buf.at[me], local_sem.at[0])
    own.start()
    own_w = pltpu.make_async_copy(w_ref.at[me], w_buf.at[me], local_sem.at[1])
    own_w.start()
    own_small = pltpu.make_async_copy(small_ref, small_all.at[me], local_sem.at[2])
    own_small.start()
    enter_all(me, n_dev)
    own.wait()
    cube = CubeGather(me, lambda dev, p: x_buf.at[dev, pl.ds(PARTS[p][0], PARTS[p][1])], send_sem, recv_sem, core_sem)
    cube.begin()

    def spread(hop):
        peer = lax.rem(me + hop, n_dev)
        return [
            pltpu.make_async_remote_copy(src_ref=small_ref, dst_ref=small_all.at[me], send_sem=misc_send.at[0, hop], recv_sem=misc_recv.at[0, me], device_id=(peer,), device_id_type=pl.DeviceIdType.MESH),
            pltpu.make_async_remote_copy(src_ref=w_ref.at[peer], dst_ref=w_buf.at[me], send_sem=misc_send.at[1, hop], recv_sem=misc_recv.at[1, me], device_id=(peer,), device_id_type=pl.DeviceIdType.MESH),
        ]

    for kind in range(2):
        @pl.loop(1, n_dev)
        def _(hop, kind=kind):
            spread(hop)[kind].start()

    cube.receive(1)
    cube.receive(2)
    own_w.wait()
    own_small.wait()

    @pl.loop(1, n_dev)
    def _(hop):
        src = lax.rem(me + hop, n_dev)
        landed(small_all.at[src], misc_recv.at[0, src])
        landed(w_buf.at[src], misc_recv.at[1, src])

    width = x_ref.shape[1]
    tok = x_ref.shape[0]
    rows = w_ref.shape[1]
    gain = jnp.concatenate([small_all[d, 0:1, 0:rows] for d in range(n_dev)], axis=1)
    weight = w_buf[...].reshape(width, w_ref.shape[2])
    head_dim = q_t.shape[0]
    freq = freq_ref[:, 0:1]
    flushes = []

    @pl.loop(0, n_dev)
    def _(dev):
        at = pl.ds(pl.multiple_of(dev * tok, tok), tok)
        angle = freq * jnp.concatenate([small_all[dev, 1:2, :], small_all[dev, 2:3, :]], axis=1)
        cos_ref[:, at] = jnp.cos(angle)
        sin_ref[:, at] = jnp.sin(angle)

    def project(dev):
        act = x_buf[dev].astype(F32)
        inv = lax.rsqrt(jnp.mean(act * act, axis=-1, keepdims=True) + RMS_EPS)
        normed = (act * inv * gain).astype(BF16)
        u_buf[dev] = normed
        at = pl.ds(pl.multiple_of(dev * tok, tok), tok)
        proj = mm(normed, weight)
        proj_t = proj.T
        cos_tab, sin_tab = cos_ref[:, at], sin_ref[:, at]
        query = rope_t(proj_t[:head_dim], cos_tab, sin_tab).astype(BF16).astype(F32)
        key = rope_t(proj_t[head_dim:2 * head_dim], cos_tab, sin_tab)
        q_t[:, at] = (query * (head_dim ** -0.5)).astype(BF16)
        k_t[:, at] = key.astype(BF16)
        v_t[:, at] = proj_t[2 * head_dim:3 * head_dim].astype(BF16)
        k_out[at, :] = key.T.astype(BF16)
        v_out[at, :] = proj[:, 2 * head_dim:3 * head_dim].astype(BF16)
        flush = pltpu.make_async_copy(u_buf.at[dev], u_out.at[dev], u_sem.at[len(flushes)])
        flush.start()
        flushes.append(flush)

    other = flip(me, CORE)
    cube.receive_core(0)
    project(me)
    project(other)
    cube.receive(4)
    cube.receive(3)
    for index in (1, 2, 4):
        cube.receive_core(index)
    for bit in CHIP_AXES:
        project(flip(me, bit))
        project(flip(other, bit))
    cube.receive(5)
    cube.receive(6)
    for index in (3, 5, 6):
        cube.receive_core(index)
    for skip in range(3):
        bits = [bit for i, bit in enumerate(CHIP_AXES) if i != skip]
        project(flip(flip(me, bits[0]), bits[1]))
        project(flip(flip(other, bits[0]), bits[1]))
    cube.receive(7)
    cube.receive_core(7)
    far = flip(flip(flip(me, 2), 4), 8)
    project(far)
    project(flip(far, CORE))

    cube.finish()

    @pl.loop(1, n_dev)
    def _(hop):
        for copy in spread(hop):
            copy.wait_send()

    for flush in flushes:
        flush.wait()


def gather_proj(n_dev, x_act, small, w_blocks, inv_freq, head_dim):
    tok, width = x_act.shape
    seq = tok * n_dev
    any_spec = pl.BlockSpec(memory_space=pl.ANY)
    vmem_spec = pl.BlockSpec(memory_space=pltpu.VMEM)
    return pl.pallas_call(
        lambda *refs: gather_proj_kernel(n_dev, *refs),
        in_specs=[any_spec, vmem_spec, vmem_spec, vmem_spec],
        out_specs=[any_spec] + [vmem_spec] * 8,
        out_shape=[jax.ShapeDtypeStruct((n_dev, tok, width), BF16)]
        + [jax.ShapeDtypeStruct((head_dim, seq), BF16)] * 3
        + [jax.ShapeDtypeStruct((seq, head_dim), BF16)] * 2
        + [jax.ShapeDtypeStruct((head_dim // 2, seq), F32)] * 2
        + [jax.ShapeDtypeStruct((n_dev,) + small.shape, F32)],
        scratch_shapes=[
            pltpu.VMEM((n_dev, tok, width), BF16),
            pltpu.VMEM((n_dev, tok, width), BF16),
            pltpu.VMEM(w_blocks.shape, BF16),
            pltpu.SemaphoreType.DMA((N_SENDS,)),
            pltpu.SemaphoreType.DMA((3, 8)),
            pltpu.SemaphoreType.DMA((3, 8)),
            pltpu.SemaphoreType.DMA((2, n_dev)),
            pltpu.SemaphoreType.DMA((2, n_dev)),
            pltpu.SemaphoreType.DMA((3,)),
            pltpu.SemaphoreType.DMA((n_dev,)),
        ],
        compiler_params=pltpu.CompilerParams(collective_id=0, has_side_effects=True),
        cost_estimate=pl.CostEstimate(flops=30 * seq * width * width, bytes_accessed=4 * seq * width, transcendentals=0),
        name='gather_proj',
    )(x_act, small, w_blocks, jnp.broadcast_to(inv_freq[:, None], (head_dim // 2, 128)))


def gate_backward(d_mixed, gate_pre, up_pre):
    gate_sig = jax.nn.sigmoid(gate_pre)
    d_up = (d_mixed * gate_pre * gate_sig).astype(BF16)
    d_gate = (d_mixed * up_pre * gate_sig * (1.0 + gate_pre * (1.0 - gate_sig))).astype(BF16)
    return d_gate, d_up


def join_columns_kernel(size, src, first, second):
    for i, out in enumerate((first, second)):
        out[...] = jnp.concatenate([src[d, :, i * size:(i + 1) * size] for d in range(src.shape[0])], axis=1)


def join_columns(blocks, size):
    shape = jax.ShapeDtypeStruct((blocks.shape[1], blocks.shape[0] * size), F32)
    return pl.pallas_call(lambda *refs: join_columns_kernel(size, *refs), out_shape=[shape, shape], name='join_columns')(blocks)


def split_heads_kernel(head_dim, src, *outs):
    for i, out in enumerate(outs):
        for d in range(src.shape[0]):
            out[:, d, :] = src[d, :, i * head_dim:(i + 1) * head_dim]


def split_heads(blocks, head_dim):
    shape = jax.ShapeDtypeStruct((blocks.shape[1], blocks.shape[0], head_dim), F32)
    return pl.pallas_call(lambda *refs: split_heads_kernel(head_dim, *refs), out_shape=[shape] * 3, name='split_heads')(blocks)


def device_step(n_dev, x_act, positions, grad_out, g_attn_s, w_q, w_k, w_v, w_o, g_mlp_s, w_gate, w_up, w_down):
    tok, width = x_act.shape
    seq = tok * n_dev
    rows, heads, head_dim = w_q.shape
    ff = w_gate.shape[1]
    ff_s = ff // n_dev
    qkv = 3 * head_dim

    small = jnp.concatenate([jnp.concatenate([g_attn_s, g_mlp_s]).astype(F32)[None], positions.astype(F32).reshape(-1, 2 * rows)], axis=0)
    small = jnp.pad(small, ((0, 8 - small.shape[0]), (0, 0)))
    w_qkv = jnp.concatenate([w_q, w_k, w_v], axis=2)
    w_blocks = jnp.pad(jnp.transpose(w_qkv, (1, 0, 2)), ((0, 0), (0, 0), (0, 256 - qkv)))
    inv_freq = ROPE_BASE ** (-(jnp.arange(head_dim // 2, dtype=F32) * (2.0 / head_dim)))
    u_all, q_t, k_t, v_t, k_in, v_in, cos_t, sin_t, small_all = gather_proj(n_dev, x_act, small, w_blocks, inv_freq, head_dim)
    u_all = u_all.reshape(seq, width)
    g_attn = small_all[:, 0, :rows].reshape(width)
    g_mlp = small_all[:, 0, rows:2 * rows].reshape(width)

    down_groups = [w_down[i:i + rows] for i in range(0, ff_s, rows)]
    down_groups = [jnp.pad(group, ((0, rows - group.shape[0]), (0, 0))) for group in down_groups]
    w_all = gather(jnp.concatenate([w_gate, w_up, w_o[0]] + down_groups, axis=1))
    w_gu = w_all[:, :2 * ff]
    w_o_all = w_all[:, 2 * ff:2 * ff + width]
    w_down_at = 2 * ff + width
    down_all = [w_all[:, w_down_at + i * width:w_down_at + (i + 1) * width].reshape(n_dev, rows, width) for i in range(len(down_groups))]
    w_down_all = jnp.concatenate(down_all, axis=1)[:, :ff_s].reshape(ff, width)
    me = lax.axis_index(SEQ_AXIS)
    w_cols = jnp.concatenate([lax.dynamic_slice(w_all, (0, at + me * ff_s), (width, ff_s)) for at in (0, ff)], axis=1)

    o_blocks, of_t, lse = attention_fwd(q_t, k_in, v_t, n_dev)
    o_loc = exchange(o_blocks).reshape(width, tok)
    w_parts = jnp.stack([w.reshape(rows, heads * head_dim) for w in (w_q, w_k, w_v)])
    o_loc, w_parts, w_down_all = lax.optimization_barrier((o_loc, w_parts, w_down_all))

    hidden = (x_act.astype(F32) + dot(o_loc, w_o_all, 0, 0)).astype(BF16)
    normed_mlp, inv_rms_mlp = rms_norm(hidden, g_mlp)
    a_dy = jnp.concatenate([normed_mlp, grad_out], axis=1)
    normed_mlp, a_dy = lax.optimization_barrier((normed_mlp, a_dy))
    a_dy = gather(a_dy)
    pre = with_layout_constraint(dot(normed_mlp, w_gu, 1, 0), Layout(major_to_minor=(0, 1)))
    gate_pre, up_pre = pre[:, :ff], pre[:, ff:]
    mixed = (jax.nn.silu(gate_pre) * up_pre).astype(BF16)
    y_out = (hidden.astype(F32) + dot(mixed, w_down_all, 1, 0)).astype(BF16)

    d_mixed = dot(grad_out, w_down_all, 1, 1).astype(BF16).astype(F32)
    d_gu = jnp.concatenate(gate_backward(d_mixed, gate_pre, up_pre), axis=1)
    d_normed = dot(d_gu, w_gu, 1, 1).astype(BF16)
    d_hid_norm, part_g_mlp = rms_norm_bwd(hidden, g_mlp, inv_rms_mlp, d_normed)
    d_hidden = (grad_out.astype(F32) + d_hid_norm).astype(BF16)
    do_blocks = exchange(dot(w_o_all, d_hidden, 1, 1).astype(BF16).reshape(n_dev, head_dim, tok))
    half_n = n_dev // 2
    pairs = [(i, (i + half_n) % n_dev) for i in range(n_dev)]
    near = (me // half_n) * half_n
    o_far = lax.ppermute(lax.dynamic_slice_in_dim(o_blocks, half_n - near, half_n), SEQ_AXIS, pairs)
    do_blocks, y_out = lax.optimization_barrier((do_blocks, y_out))
    dh_half = lax.all_gather(d_hidden, SEQ_AXIS, axis=0, tiled=True, axis_index_groups=[list(range(half_n)), list(range(half_n, n_dev))])

    do_t = jnp.transpose(do_blocks, (1, 0, 2)).reshape(head_dim, seq)
    d_blocks, d_proj_t, *w_qkv_all = attention_bwd(q_t, do_t, of_t, lse, k_in, k_t, v_in, cos_t, sin_t, w_parts, n_dev)
    d_proj = exchange(d_blocks)

    grad_w_qkv = lax.optimization_barrier(dot(d_proj_t, u_all, 1, 0)).T
    attn_send = grad_w_qkv.reshape(n_dev, rows, qkv)
    d_proj, attn_send = lax.optimization_barrier((d_proj, attn_send))
    attn_back = exchange(attn_send)

    a_all, dy_all = a_dy[:, :width], a_dy[:, width:]
    pre_t = dot(w_cols, a_all, 0, 1)
    gate_t, up_t = pre_t[:ff_s], pre_t[ff_s:]
    d_mixed_t = dot(w_down, dy_all, 1, 1).astype(BF16).astype(F32)
    mixed_t = (jax.nn.silu(gate_t) * up_t).astype(BF16)
    d_gu_t = jnp.concatenate(gate_backward(d_mixed_t, gate_t, up_t), axis=0)
    mlp_send = dot(a_all, d_gu_t, 0, 1).reshape(n_dev, rows, 2 * ff_s)
    attn_back, mlp_send, mixed_t, d_proj = lax.optimization_barrier((attn_back, mlp_send, mixed_t, d_proj))
    mlp_back = exchange(mlp_send)
    grad_w_down = dot(mixed_t, dy_all, 1, 0)

    d_proj = d_proj.reshape(heads, 3, head_dim, tok)
    inv_rms = lax.rsqrt(jnp.mean(jnp.square(x_act.astype(F32)), axis=-1, keepdims=True) + RMS_EPS)
    d_u = sum(dot(d_proj[:, p].reshape(heads * head_dim, tok), w_qkv_all[p].reshape(width, heads * head_dim), 0, 1) for p in range(3)).astype(BF16)
    d_x_norm, part_g_attn = rms_norm_bwd(x_act, g_attn, inv_rms, d_u)
    grad_x = (d_hidden.astype(F32) + d_x_norm).astype(BF16)
    gain_send = jnp.pad(jnp.concatenate([part_g_attn.reshape(n_dev, 1, rows), part_g_mlp.reshape(n_dev, 1, rows)], axis=2), ((0, 0), (0, 7), (0, 0)))

    o_far, dh_half, o_blocks, grad_w_down = lax.optimization_barrier((o_far, dh_half, o_blocks, grad_w_down))
    o_pair = jnp.concatenate([lax.dynamic_slice_in_dim(o_blocks, near, half_n), o_far], axis=1)
    part_w_o = dot(o_pair.transpose(1, 0, 2).reshape(2 * head_dim, seq // 2), dh_half, 1, 0)
    grad_w_o = (part_w_o[:head_dim] + lax.ppermute(part_w_o[head_dim:], SEQ_AXIS, pairs))[None]

    grad_w_q, grad_w_k, grad_w_v = split_heads(attn_back, head_dim)
    mlp_back, gain_send, grad_w_down, grad_w_q, grad_w_k, grad_w_v, grad_w_o = lax.optimization_barrier((mlp_back, gain_send, grad_w_down, grad_w_q, grad_w_k, grad_w_v, grad_w_o))
    gains = jnp.sum(exchange(gain_send)[:, 0], axis=0)
    grad_g_attn, grad_g_mlp = gains[:rows], gains[rows:]
    grad_w_gate, grad_w_up = join_columns(mlp_back, ff_s)
    return (y_out, grad_x, grad_g_attn, grad_w_q, grad_w_k, grad_w_v, grad_w_o, grad_g_mlp, grad_w_gate, grad_w_up, grad_w_down)


def solution(mesh):
    n_dev = mesh.shape[SEQ_AXIS]
    token_spec = P(SEQ_AXIS, None)
    cube_spec = P(SEQ_AXIS, None, None)
    gain_spec = P(SEQ_AXIS)
    weight_specs = (gain_spec, cube_spec, cube_spec, cube_spec, cube_spec, gain_spec, token_spec, token_spec, token_spec)
    return jax.shard_map(lambda *args: device_step(n_dev, *args), mesh=mesh, in_specs=(token_spec, gain_spec, token_spec) + weight_specs, out_specs=(token_spec, token_spec) + weight_specs, check_vma=False)
```

```python
import jax
import jax.numpy as jnp
from jax import lax
from jax.experimental import pallas as pl
from jax.experimental.layout import Layout, with_layout_constraint
from jax.experimental.pallas import tpu as pltpu
from jax.sharding import PartitionSpec as P

SEQ_AXIS = 'sp'
RMS_EPS = 1e-5
ROPE_BASE = 10000.0
MASK_VALUE = -1e30
TILE = 512
F32 = jnp.float32
BF16 = jnp.bfloat16


def rms_norm(act_in, gain_vec):
    act_f = act_in.astype(F32)
    inv_rms = lax.rsqrt(jnp.mean(act_f * act_f, axis=-1, keepdims=True) + RMS_EPS)
    return (act_f * inv_rms * gain_vec.astype(F32)).astype(BF16), inv_rms


def rms_norm_bwd(act_in, gain_vec, inv_rms, d_normed):
    act_f = act_in.astype(F32)
    d_f = d_normed.astype(F32)
    scaled_d = d_f * gain_vec.astype(F32)
    proj_mean = jnp.mean(scaled_d * act_f, axis=-1, keepdims=True)
    d_act = inv_rms * scaled_d - act_f * (inv_rms * inv_rms * inv_rms) * proj_mean
    d_gain = jnp.sum(d_f * act_f * inv_rms, axis=0)
    return d_act, d_gain


def dot(lhs, rhs, l_dim, r_dim):
    return lax.dot_general(lhs, rhs, (((l_dim,), (r_dim,)), ((), ())), preferred_element_type=F32)


def gather(shard):
    return lax.all_gather(shard, SEQ_AXIS, axis=0, tiled=True)


def exchange(blocks):
    return lax.all_to_all(blocks, SEQ_AXIS, 0, 0, tiled=True)


def rope_t(vals, cos_tab, sin_tab):
    half = vals.shape[0] // 2
    first, second = vals[:half], vals[half:]
    return jnp.concatenate([first * cos_tab - second * sin_tab, second * cos_tab + first * sin_tab], axis=0)


def mm(lhs, rhs):
    return jnp.dot(lhs, rhs, preferred_element_type=F32)


def diag_mask(tile):
    key_at = lax.broadcasted_iota(jnp.int32, (tile, tile), 0)
    query_at = lax.broadcasted_iota(jnp.int32, (tile, tile), 1)
    return key_at <= query_at


def attn_fwd_kernel(tile, q_t, k_ref, v_t, o_ref, of_ref, lse_ref, s_buf):
    step = pl.program_id(0)
    query = q_t[...]

    def scores(j):
        return mm(k_ref[pl.ds(pl.multiple_of(j * tile, tile), tile), :], query)

    def keep(j, logits, top):
        s_buf[pl.ds(pl.multiple_of(j * tile, tile), tile), :] = logits
        return jnp.maximum(top, jnp.max(logits, axis=0, keepdims=True))

    top = keep(step, jnp.where(diag_mask(tile), scores(step), MASK_VALUE), jnp.full((1, tile), MASK_VALUE, F32))
    top = lax.fori_loop(0, step, lambda j, c: keep(j, scores(j), c), top)

    def weigh(j, carry):
        acc, total = carry
        at = pl.ds(pl.multiple_of(j * tile, tile), tile)
        prob = jnp.exp(s_buf[at, :] - top)
        return acc + mm(v_t[:, at], prob.astype(BF16)), total + jnp.sum(prob, axis=0, keepdims=True)

    out, total = lax.fori_loop(0, step + 1, weigh, (jnp.zeros((v_t.shape[0], tile), F32), jnp.zeros((1, tile), F32)))
    out = out / total
    lse = top + jnp.log(total)
    of_ref[...] = out
    lse_ref[...] = lse
    block = o_ref.shape[2]
    for part in range(tile // block):
        o_ref[part] = out[:, part * block:(part + 1) * block].astype(BF16)


def attention_fwd(q_t, k_in, v_t, n_blocks):
    head_dim, seq = q_t.shape
    block = seq // n_blocks
    per = TILE // block
    return pl.pallas_call(
        lambda *refs: attn_fwd_kernel(TILE, *refs),
        grid=(seq // TILE,),
        in_specs=[pl.BlockSpec((head_dim, TILE), lambda i: (0, i)), pl.BlockSpec((seq, head_dim), lambda i: (0, 0)), pl.BlockSpec((head_dim, seq), lambda i: (0, 0))],
        out_specs=[pl.BlockSpec((per, head_dim, block), lambda i: (i, 0, 0)), pl.BlockSpec((head_dim, TILE), lambda i: (0, i)), pl.BlockSpec((1, TILE), lambda i: (0, i))],
        out_shape=[jax.ShapeDtypeStruct((n_blocks, head_dim, block), BF16), jax.ShapeDtypeStruct((head_dim, seq), F32), jax.ShapeDtypeStruct((1, seq), F32)],
        scratch_shapes=[pltpu.VMEM((seq, TILE), F32)],
        cost_estimate=pl.CostEstimate(flops=8 * seq * seq * head_dim, bytes_accessed=8 * seq * head_dim, transcendentals=seq * seq),
        name='attn_fwd',
    )(q_t, k_in, v_t)


PARTS = ((0, 96), (96, 80), (176, 80))
CORE, CHIP_AXES = 1, (2, 4, 8)


def flip(dev, bit):
    return dev + bit * (1 - 2 * ((dev // bit) % 2))


def start_copy(src, dst, send_sem, recv_sem, peer):
    copy = pltpu.make_async_remote_copy(src_ref=src, dst_ref=dst, send_sem=send_sem, recv_sem=recv_sem, device_id=(peer,), device_id_type=pl.DeviceIdType.MESH)
    copy.start()
    return copy


def landed(ref, sem):
    pltpu.make_async_copy(ref, ref, sem).wait()


def enter_all(me, n_dev):
    barrier = pltpu.get_barrier_semaphore()

    @pl.loop(1, n_dev)
    def _(hop):
        pl.semaphore_signal(barrier, inc=1, device_id=(lax.rem(me + hop, n_dev),), device_id_type=pl.DeviceIdType.MESH)

    pl.semaphore_wait(barrier, n_dev - 1)


class CubeGather:
    def __init__(self, me, part, send_sem, recv_sem, core_sem):
        self.me, self.part = me, part
        self.send_sem, self.recv_sem, self.core_sem = send_sem, recv_sem, core_sem
        self.sent = []

    def axes(self, p):
        return [CHIP_AXES[(p + i) % 3] for i in range(3)]

    def owner(self, p, index, start=None):
        dev = self.me if start is None else start
        for i, bit in enumerate(self.axes(p)):
            if (index >> i) & 1:
                dev = flip(dev, bit)
        return dev

    def push(self, p, index, axis):
        ref = self.part(self.owner(p, index), p)
        start_copy(ref, ref, self.send_sem.at[len(self.sent)], self.recv_sem.at[p, index + (1 << axis)], flip(self.me, self.axes(p)[axis]))
        self.sent.append((p, index))

    def push_core(self, p, index):
        ref = self.part(self.owner(p, index), p)
        start_copy(ref, ref, self.send_sem.at[len(self.sent)], self.core_sem.at[p, index], flip(self.me, CORE))
        self.sent.append((p, index))

    def begin(self):
        for axis in range(3):
            for p in range(3):
                self.push(p, 0, axis)
        for p in range(3):
            self.push_core(p, 0)

    def receive(self, index):
        for p in range(3):
            landed(self.part(self.owner(p, index), p), self.recv_sem.at[p, index])
            for axis in range(index.bit_length(), 3):
                self.push(p, index, axis)
            self.push_core(p, index)

    def receive_core(self, index):
        for p in range(3):
            landed(self.part(self.owner(p, index, flip(self.me, CORE)), p), self.core_sem.at[p, index])

    def finish(self):
        for slot, (p, index) in enumerate(self.sent):
            landed(self.part(self.owner(p, index), p), self.send_sem.at[slot])


N_SENDS = 9 + 12 + 24


def attn_bwd_kernel(n_dev, tile, block, q_t, do_t, of_t, lse_ref, cos_ref, sin_ref, k_ref, k_t, v_ref, cos_all, sin_all, w_ref, d_blocks, d_proj_t, w_out_q, w_out_k, w_out_v, dq_acc, dk_acc, dv_acc, w_buf, send_sem, recv_sem, core_sem, local_sem):
    step = pl.program_id(0)
    last = pl.num_programs(0) - 1
    me = lax.axis_index(SEQ_AXIS)
    cube = CubeGather(me, lambda dev, p: w_buf.at[p, dev], send_sem, recv_sem, core_sem)

    @pl.when(step == 0)
    def _():
        own = [pltpu.make_async_copy(w_ref.at[p], w_buf.at[p, me], local_sem.at[p]) for p in range(3)]
        for copy in own:
            copy.start()
        enter_all(me, n_dev)
        for copy in own:
            copy.wait()
        cube.begin()

    for at_step, indices in ((4, (1,)), (5, (2,)), (6, (4,)), (7, (3,))):
        @pl.when(step == at_step)
        def _(indices=indices):
            for index in indices:
                cube.receive(index)

    head_dim = q_t.shape[0]
    query_t, d_out_t = q_t[...], do_t[...]
    lse = lse_ref[...]
    delta = jnp.sum(d_out_t.astype(F32) * of_t[...], axis=0, keepdims=True)

    @pl.when(step == 0)
    def _():
        dk_acc[...] = jnp.zeros_like(dk_acc)
        dv_acc[...] = jnp.zeros_like(dv_acc)

    dq_acc[...] = jnp.zeros_like(dq_acc)

    def visit(j, masked):
        at = pl.ds(pl.multiple_of(j * tile, tile), tile)
        prob = jnp.exp(mm(k_ref[at, :], query_t) - lse)
        if masked:
            prob = jnp.where(diag_mask(tile), prob, 0.0)
        d_prob = mm(v_ref[at, :], d_out_t).astype(BF16).astype(F32)
        d_logits = (prob * (d_prob - delta)).astype(BF16)
        dv_acc[:, at] += dot(d_out_t, prob.astype(BF16), 1, 1)
        dk_acc[:, at] += dot(query_t, d_logits, 1, 1)
        dq_acc[...] += mm(k_t[:, at], d_logits)

    visit(step, True)

    @pl.loop(0, step)
    def _(j):
        visit(j, False)

    def put(row, col_block, values):
        rows = slice(row, row + values.shape[0])
        d_proj_t[rows, pl.ds(pl.multiple_of(col_block * block, block), values.shape[1])] = values
        for part in range(values.shape[1] // block):
            d_blocks[col_block + part, rows, :] = values[:, part * block:(part + 1) * block]

    d_q = (dq_acc[...] * (head_dim ** -0.5)).astype(BF16).astype(F32)
    per = tile // block
    put(0, step * per, rope_t(d_q, cos_ref[...], -sin_ref[...]).astype(BF16))

    @pl.when(step == last)
    def _():
        @pl.loop(0, pl.num_programs(0))
        def _(j):
            at = pl.ds(pl.multiple_of(j * tile, tile), tile)
            put(head_dim, j * per, rope_t(dk_acc[:, at].astype(BF16).astype(F32), cos_all[:, at], -sin_all[:, at]).astype(BF16))
            put(2 * head_dim, j * per, dv_acc[:, at].astype(BF16))

        for index in (5, 6, 7):
            cube.receive(index)
        for index in range(8):
            cube.receive_core(index)
        flushes = [pltpu.make_async_copy(w_buf.at[p], out, local_sem.at[p]) for p, out in enumerate((w_out_q, w_out_k, w_out_v))]
        for flush in flushes:
            flush.start()
        cube.finish()
        for flush in flushes:
            flush.wait()


def attention_bwd(q_t, do_t, of_t, lse, k_in, k_t, v_in, cos_t, sin_t, w_parts, n_blocks):
    head_dim, seq = q_t.shape
    block = seq // n_blocks
    cols = pl.BlockSpec((head_dim, TILE), lambda i: (0, i))
    half_cols = pl.BlockSpec((head_dim // 2, TILE), lambda i: (0, i))
    all_rows = pl.BlockSpec((seq, head_dim), lambda i: (0, 0))
    all_cols = pl.BlockSpec((head_dim, seq), lambda i: (0, 0))
    all_half = pl.BlockSpec((head_dim // 2, seq), lambda i: (0, 0))
    w_all_shape = (3, n_blocks) + w_parts.shape[1:]
    return pl.pallas_call(
        lambda *refs: attn_bwd_kernel(n_blocks, TILE, block, *refs),
        grid=(seq // TILE,),
        in_specs=[cols, cols, cols, pl.BlockSpec((1, TILE), lambda i: (0, i)), half_cols, half_cols, all_rows, all_cols, all_rows, all_half, all_half, pl.BlockSpec(memory_space=pl.ANY)],
        out_specs=[pl.BlockSpec((n_blocks, 3 * head_dim, block), lambda i: (0, 0, 0)), pl.BlockSpec((3 * head_dim, seq), lambda i: (0, 0))] + [pl.BlockSpec(memory_space=pl.ANY)] * 3,
        out_shape=[jax.ShapeDtypeStruct((n_blocks, 3 * head_dim, block), BF16), jax.ShapeDtypeStruct((3 * head_dim, seq), BF16)] + [jax.ShapeDtypeStruct(w_all_shape[1:], BF16)] * 3,
        scratch_shapes=[
            pltpu.VMEM((head_dim, TILE), F32),
            pltpu.VMEM((head_dim, seq), F32),
            pltpu.VMEM((head_dim, seq), F32),
            pltpu.VMEM(w_all_shape, BF16),
            pltpu.SemaphoreType.DMA((N_SENDS,)),
            pltpu.SemaphoreType.DMA((3, 8)),
            pltpu.SemaphoreType.DMA((3, 8)),
            pltpu.SemaphoreType.DMA((3,)),
        ],
        compiler_params=pltpu.CompilerParams(collective_id=1, has_side_effects=True),
        cost_estimate=pl.CostEstimate(flops=20 * seq * seq * head_dim, bytes_accessed=20 * seq * head_dim, transcendentals=seq * seq),
        name='attn_bwd',
    )(q_t, do_t, of_t, lse, cos_t, sin_t, k_in, k_t, v_in, cos_t, sin_t, w_parts)


def gather_proj_kernel(n_dev, x_ref, small_ref, w_ref, freq_ref, u_out, q_t, k_t, v_t, k_out, v_out, cos_ref, sin_ref, small_all, x_buf, u_buf, w_buf, send_sem, recv_sem, core_sem, misc_send, misc_recv, local_sem, u_sem):
    me = lax.axis_index(SEQ_AXIS)
    own = pltpu.make_async_copy(x_ref, x_buf.at[me], local_sem.at[0])
    own.start()
    own_w = pltpu.make_async_copy(w_ref.at[me], w_buf.at[me], local_sem.at[1])
    own_w.start()
    own_small = pltpu.make_async_copy(small_ref, small_all.at[me], local_sem.at[2])
    own_small.start()
    enter_all(me, n_dev)
    own.wait()
    cube = CubeGather(me, lambda dev, p: x_buf.at[dev, pl.ds(PARTS[p][0], PARTS[p][1])], send_sem, recv_sem, core_sem)
    cube.begin()

    def spread(hop):
        peer = lax.rem(me + hop, n_dev)
        return [
            pltpu.make_async_remote_copy(src_ref=small_ref, dst_ref=small_all.at[me], send_sem=misc_send.at[0, hop], recv_sem=misc_recv.at[0, me], device_id=(peer,), device_id_type=pl.DeviceIdType.MESH),
            pltpu.make_async_remote_copy(src_ref=w_ref.at[peer], dst_ref=w_buf.at[me], send_sem=misc_send.at[1, hop], recv_sem=misc_recv.at[1, me], device_id=(peer,), device_id_type=pl.DeviceIdType.MESH),
        ]

    for kind in range(2):
        @pl.loop(1, n_dev)
        def _(hop, kind=kind):
            spread(hop)[kind].start()

    cube.receive(1)
    cube.receive(2)
    own_w.wait()
    own_small.wait()

    @pl.loop(1, n_dev)
    def _(hop):
        src = lax.rem(me + hop, n_dev)
        landed(small_all.at[src], misc_recv.at[0, src])
        landed(w_buf.at[src], misc_recv.at[1, src])

    width = x_ref.shape[1]
    tok = x_ref.shape[0]
    rows = w_ref.shape[1]
    gain = jnp.concatenate([small_all[d, 0:1, 0:rows] for d in range(n_dev)], axis=1)
    weight = w_buf[...].reshape(width, w_ref.shape[2])
    head_dim = q_t.shape[0]
    freq = freq_ref[:, 0:1]
    flushes = []

    @pl.loop(0, n_dev)
    def _(dev):
        at = pl.ds(pl.multiple_of(dev * tok, tok), tok)
        angle = freq * jnp.concatenate([small_all[dev, 1:2, :], small_all[dev, 2:3, :]], axis=1)
        cos_ref[:, at] = jnp.cos(angle)
        sin_ref[:, at] = jnp.sin(angle)

    def project(dev):
        act = x_buf[dev].astype(F32)
        inv = lax.rsqrt(jnp.mean(act * act, axis=-1, keepdims=True) + RMS_EPS)
        normed = (act * inv * gain).astype(BF16)
        u_buf[dev] = normed
        at = pl.ds(pl.multiple_of(dev * tok, tok), tok)
        proj = mm(normed, weight)
        proj_t = jnp.concatenate([proj, jnp.zeros((tok, 4 * head_dim - proj.shape[1]), F32)], axis=1).T
        cos_tab, sin_tab = cos_ref[:, at], sin_ref[:, at]
        query = rope_t(proj_t[:head_dim], cos_tab, sin_tab).astype(BF16).astype(F32)
        key = rope_t(proj_t[head_dim:2 * head_dim], cos_tab, sin_tab)
        q_t[:, at] = (query * (head_dim ** -0.5)).astype(BF16)
        k_t[:, at] = key.astype(BF16)
        v_t[:, at] = proj_t[2 * head_dim:3 * head_dim].astype(BF16)
        k_out[at, :] = key.T.astype(BF16)
        v_out[at, :] = proj[:, 2 * head_dim:3 * head_dim].astype(BF16)
        flush = pltpu.make_async_copy(u_buf.at[dev], u_out.at[dev], u_sem.at[len(flushes)])
        flush.start()
        flushes.append(flush)

    other = flip(me, CORE)
    cube.receive_core(0)
    project(me)
    project(other)
    cube.receive(4)
    cube.receive(3)
    for index in (1, 2, 4):
        cube.receive_core(index)
    for bit in CHIP_AXES:
        project(flip(me, bit))
        project(flip(other, bit))
    cube.receive(5)
    cube.receive(6)
    for index in (3, 5, 6):
        cube.receive_core(index)
    for skip in range(3):
        bits = [bit for i, bit in enumerate(CHIP_AXES) if i != skip]
        project(flip(flip(me, bits[0]), bits[1]))
        project(flip(flip(other, bits[0]), bits[1]))
    cube.receive(7)
    cube.receive_core(7)
    far = flip(flip(flip(me, 2), 4), 8)
    project(far)
    project(flip(far, CORE))

    cube.finish()

    @pl.loop(1, n_dev)
    def _(hop):
        for copy in spread(hop):
            copy.wait_send()

    for flush in flushes:
        flush.wait()


def gather_proj(n_dev, x_act, small, w_blocks, inv_freq, head_dim):
    tok, width = x_act.shape
    seq = tok * n_dev
    any_spec = pl.BlockSpec(memory_space=pl.ANY)
    vmem_spec = pl.BlockSpec(memory_space=pltpu.VMEM)
    return pl.pallas_call(
        lambda *refs: gather_proj_kernel(n_dev, *refs),
        in_specs=[any_spec, vmem_spec, vmem_spec, vmem_spec],
        out_specs=[any_spec] + [vmem_spec] * 8,
        out_shape=[jax.ShapeDtypeStruct((n_dev, tok, width), BF16)]
        + [jax.ShapeDtypeStruct((head_dim, seq), BF16)] * 3
        + [jax.ShapeDtypeStruct((seq, head_dim), BF16)] * 2
        + [jax.ShapeDtypeStruct((head_dim // 2, seq), F32)] * 2
        + [jax.ShapeDtypeStruct((n_dev,) + small.shape, F32)],
        scratch_shapes=[
            pltpu.VMEM((n_dev, tok, width), BF16),
            pltpu.VMEM((n_dev, tok, width), BF16),
            pltpu.VMEM(w_blocks.shape, BF16),
            pltpu.SemaphoreType.DMA((N_SENDS,)),
            pltpu.SemaphoreType.DMA((3, 8)),
            pltpu.SemaphoreType.DMA((3, 8)),
            pltpu.SemaphoreType.DMA((2, n_dev)),
            pltpu.SemaphoreType.DMA((2, n_dev)),
            pltpu.SemaphoreType.DMA((3,)),
            pltpu.SemaphoreType.DMA((n_dev,)),
        ],
        compiler_params=pltpu.CompilerParams(collective_id=0, has_side_effects=True),
        cost_estimate=pl.CostEstimate(flops=30 * seq * width * width, bytes_accessed=4 * seq * width, transcendentals=0),
        name='gather_proj',
    )(x_act, small, w_blocks, jnp.broadcast_to(inv_freq[:, None], (head_dim // 2, 128)))


def gate_backward(d_mixed, gate_pre, up_pre):
    gate_sig = jax.nn.sigmoid(gate_pre)
    d_up = (d_mixed * gate_pre * gate_sig).astype(BF16)
    d_gate = (d_mixed * up_pre * gate_sig * (1.0 + gate_pre * (1.0 - gate_sig))).astype(BF16)
    return d_gate, d_up


def join_columns_kernel(size, src, first, second):
    for i, out in enumerate((first, second)):
        out[...] = jnp.concatenate([src[d, :, i * size:(i + 1) * size] for d in range(src.shape[0])], axis=1)


def join_columns(blocks, size):
    shape = jax.ShapeDtypeStruct((blocks.shape[1], blocks.shape[0] * size), F32)
    return pl.pallas_call(lambda *refs: join_columns_kernel(size, *refs), out_shape=[shape, shape], name='join_columns')(blocks)


def split_heads_kernel(head_dim, src, *outs):
    for i, out in enumerate(outs):
        for d in range(src.shape[0]):
            out[:, d, :] = src[d, :, i * head_dim:(i + 1) * head_dim]


def split_heads(blocks, head_dim):
    shape = jax.ShapeDtypeStruct((blocks.shape[1], blocks.shape[0], head_dim), F32)
    return pl.pallas_call(lambda *refs: split_heads_kernel(head_dim, *refs), out_shape=[shape] * 3, name='split_heads')(blocks)


def device_step(n_dev, x_act, positions, grad_out, g_attn_s, w_q, w_k, w_v, w_o, g_mlp_s, w_gate, w_up, w_down):
    tok, width = x_act.shape
    seq = tok * n_dev
    rows, heads, head_dim = w_q.shape
    ff = w_gate.shape[1]
    ff_s = ff // n_dev
    qkv = 3 * head_dim

    small = jnp.concatenate([jnp.concatenate([g_attn_s, g_mlp_s]).astype(F32)[None], positions.astype(F32).reshape(-1, 2 * rows)], axis=0)
    small = jnp.pad(small, ((0, 8 - small.shape[0]), (0, 0)))
    w_qkv = jnp.concatenate([w_q, w_k, w_v], axis=2)
    w_blocks = jnp.transpose(w_qkv, (1, 0, 2))
    inv_freq = ROPE_BASE ** (-(jnp.arange(head_dim // 2, dtype=F32) * (2.0 / head_dim)))
    u_all, q_t, k_t, v_t, k_in, v_in, cos_t, sin_t, small_all = gather_proj(n_dev, x_act, small, w_blocks, inv_freq, head_dim)
    u_all = u_all.reshape(seq, width)
    g_attn = small_all[:, 0, :rows].reshape(width)
    g_mlp = small_all[:, 0, rows:2 * rows].reshape(width)

    down_groups = [w_down[i:i + rows] for i in range(0, ff_s, rows)]
    down_groups = [jnp.pad(group, ((0, rows - group.shape[0]), (0, 0))) for group in down_groups]
    w_all = gather(jnp.concatenate([w_gate, w_up, w_o[0]] + down_groups, axis=1))
    w_gu = w_all[:, :2 * ff]
    w_o_all = w_all[:, 2 * ff:2 * ff + width]
    w_down_at = 2 * ff + width
    down_all = [w_all[:, w_down_at + i * width:w_down_at + (i + 1) * width].reshape(n_dev, rows, width) for i in range(len(down_groups))]
    w_down_all = jnp.concatenate(down_all, axis=1)[:, :ff_s].reshape(ff, width)
    me = lax.axis_index(SEQ_AXIS)
    w_cols = jnp.concatenate([lax.dynamic_slice(w_all, (0, at + me * ff_s), (width, ff_s)) for at in (0, ff)], axis=1)

    o_blocks, of_t, lse = attention_fwd(q_t, k_in, v_t, n_dev)
    o_loc = exchange(o_blocks).reshape(width, tok)
    w_parts = jnp.stack([w.reshape(rows, heads * head_dim) for w in (w_q, w_k, w_v)])
    o_loc, w_parts = lax.optimization_barrier((o_loc, w_parts))

    hidden = (x_act.astype(F32) + dot(o_loc, w_o_all, 0, 0)).astype(BF16)
    normed_mlp, inv_rms_mlp = rms_norm(hidden, g_mlp)
    a_dy = jnp.concatenate([normed_mlp, grad_out], axis=1)
    normed_mlp, a_dy = lax.optimization_barrier((normed_mlp, a_dy))
    a_dy = gather(a_dy)
    pre = with_layout_constraint(dot(normed_mlp, w_gu, 1, 0), Layout(major_to_minor=(0, 1)))
    gate_pre, up_pre = pre[:, :ff], pre[:, ff:]
    mixed = (jax.nn.silu(gate_pre) * up_pre).astype(BF16)
    y_out = (hidden.astype(F32) + dot(mixed, w_down_all, 1, 0)).astype(BF16)

    d_mixed = dot(grad_out, w_down_all, 1, 1).astype(BF16).astype(F32)
    d_gu = jnp.concatenate(gate_backward(d_mixed, gate_pre, up_pre), axis=1)
    d_normed = dot(d_gu, w_gu, 1, 1).astype(BF16)
    d_hid_norm, part_g_mlp = rms_norm_bwd(hidden, g_mlp, inv_rms_mlp, d_normed)
    d_hidden = (grad_out.astype(F32) + d_hid_norm).astype(BF16)
    do_blocks = exchange(dot(w_o_all, d_hidden, 1, 1).astype(BF16).reshape(n_dev, head_dim, tok))
    half_n = n_dev // 2
    pairs = [(i, (i + half_n) % n_dev) for i in range(n_dev)]
    near = (me // half_n) * half_n
    o_far = lax.ppermute(lax.dynamic_slice_in_dim(o_blocks, half_n - near, half_n), SEQ_AXIS, pairs)
    do_blocks, y_out = lax.optimization_barrier((do_blocks, y_out))
    dh_half = lax.all_gather(d_hidden, SEQ_AXIS, axis=0, tiled=True, axis_index_groups=[list(range(half_n)), list(range(half_n, n_dev))])

    do_t = jnp.transpose(do_blocks, (1, 0, 2)).reshape(head_dim, seq)
    d_blocks, d_proj_t, *w_qkv_all = attention_bwd(q_t, do_t, of_t, lse, k_in, k_t, v_in, cos_t, sin_t, w_parts, n_dev)
    d_proj = exchange(d_blocks)

    grad_w_qkv = lax.optimization_barrier(dot(d_proj_t, u_all, 1, 0)).T
    attn_send = grad_w_qkv.reshape(n_dev, rows, qkv)

    a_all, dy_all = a_dy[:, :width], a_dy[:, width:]
    pre_t = dot(w_cols, a_all, 0, 1)
    d_proj, attn_send, pre_t = lax.optimization_barrier((d_proj, attn_send, pre_t))
    attn_back = exchange(attn_send)
    gate_t, up_t = pre_t[:ff_s], pre_t[ff_s:]
    d_mixed_t = dot(w_down, dy_all, 1, 1).astype(BF16).astype(F32)
    mixed_t = (jax.nn.silu(gate_t) * up_t).astype(BF16)
    d_gu_t = jnp.concatenate(gate_backward(d_mixed_t, gate_t, up_t), axis=0)
    mlp_send = dot(a_all, d_gu_t, 0, 1).reshape(n_dev, rows, 2 * ff_s)
    attn_back, mlp_send, mixed_t, d_proj = lax.optimization_barrier((attn_back, mlp_send, mixed_t, d_proj))
    mlp_back = exchange(mlp_send)
    grad_w_down = dot(mixed_t, dy_all, 1, 0)

    d_proj = d_proj.reshape(heads, 3, head_dim, tok)
    inv_rms = lax.rsqrt(jnp.mean(jnp.square(x_act.astype(F32)), axis=-1, keepdims=True) + RMS_EPS)
    d_u = sum(dot(d_proj[:, p].reshape(heads * head_dim, tok), w_qkv_all[p].reshape(width, heads * head_dim), 0, 1) for p in range(3)).astype(BF16)
    d_x_norm, part_g_attn = rms_norm_bwd(x_act, g_attn, inv_rms, d_u)
    grad_x = (d_hidden.astype(F32) + d_x_norm).astype(BF16)
    gain_send = jnp.pad(jnp.concatenate([part_g_attn.reshape(n_dev, 1, rows), part_g_mlp.reshape(n_dev, 1, rows)], axis=2), ((0, 0), (0, 7), (0, 0)))

    o_far, dh_half, o_blocks, gain_send = lax.optimization_barrier((o_far, dh_half, o_blocks, gain_send))
    o_pair = jnp.concatenate([lax.dynamic_slice_in_dim(o_blocks, near, half_n), o_far], axis=1)
    part_w_o = dot(o_pair.transpose(1, 0, 2).reshape(2 * head_dim, seq // 2), dh_half, 1, 0)
    grad_w_o = (part_w_o[:head_dim] + lax.ppermute(part_w_o[head_dim:], SEQ_AXIS, pairs))[None]

    grad_w_q, grad_w_k, grad_w_v = split_heads(attn_back, head_dim)
    mlp_back, gain_send, grad_w_down, grad_w_q, grad_w_k, grad_w_v, grad_w_o = lax.optimization_barrier((mlp_back, gain_send, grad_w_down, grad_w_q, grad_w_k, grad_w_v, grad_w_o))
    gains = jnp.sum(exchange(gain_send)[:, 0], axis=0)
    grad_g_attn, grad_g_mlp = gains[:rows], gains[rows:]
    grad_w_gate, grad_w_up = join_columns(mlp_back, ff_s)
    return (y_out, grad_x, grad_g_attn, grad_w_q, grad_w_k, grad_w_v, grad_w_o, grad_g_mlp, grad_w_gate, grad_w_up, grad_w_down)


def solution(mesh):
    n_dev = mesh.shape[SEQ_AXIS]
    token_spec = P(SEQ_AXIS, None)
    cube_spec = P(SEQ_AXIS, None, None)
    gain_spec = P(SEQ_AXIS)
    weight_specs = (gain_spec, cube_spec, cube_spec, cube_spec, cube_spec, gain_spec, token_spec, token_spec, token_spec)
    return jax.shard_map(lambda *args: device_step(n_dev, *args), mesh=mesh, in_specs=(token_spec, gain_spec, token_spec) + weight_specs, out_specs=(token_spec, token_spec) + weight_specs, check_vma=False)
```

```python
import jax
import jax.numpy as jnp
from jax import lax
from jax.experimental import pallas as pl
from jax.experimental.layout import Layout, with_layout_constraint
from jax.experimental.pallas import tpu as pltpu
from jax.sharding import PartitionSpec as P

SEQ_AXIS = 'sp'
RMS_EPS = 1e-5
ROPE_BASE = 10000.0
MASK_VALUE = -1e30
TILE = 512
F32 = jnp.float32
BF16 = jnp.bfloat16


def rms_norm(act_in, gain_vec):
    act_f = act_in.astype(F32)
    inv_rms = lax.rsqrt(jnp.mean(act_f * act_f, axis=-1, keepdims=True) + RMS_EPS)
    return (act_f * inv_rms * gain_vec.astype(F32)).astype(BF16), inv_rms


def rms_norm_bwd(act_in, gain_vec, inv_rms, d_normed):
    act_f = act_in.astype(F32)
    d_f = d_normed.astype(F32)
    scaled_d = d_f * gain_vec.astype(F32)
    proj_mean = jnp.mean(scaled_d * act_f, axis=-1, keepdims=True)
    d_act = inv_rms * scaled_d - act_f * (inv_rms * inv_rms * inv_rms) * proj_mean
    d_gain = jnp.sum(d_f * act_f * inv_rms, axis=0)
    return d_act, d_gain


def dot(lhs, rhs, l_dim, r_dim):
    return lax.dot_general(lhs, rhs, (((l_dim,), (r_dim,)), ((), ())), preferred_element_type=F32)


def gather(shard):
    return lax.all_gather(shard, SEQ_AXIS, axis=0, tiled=True)


def exchange(blocks):
    return lax.all_to_all(blocks, SEQ_AXIS, 0, 0, tiled=True)


def rope_t(vals, cos_tab, sin_tab):
    half = vals.shape[0] // 2
    first, second = vals[:half], vals[half:]
    return jnp.concatenate([first * cos_tab - second * sin_tab, second * cos_tab + first * sin_tab], axis=0)


def mm(lhs, rhs):
    return jnp.dot(lhs, rhs, preferred_element_type=F32)


def diag_mask(tile):
    key_at = lax.broadcasted_iota(jnp.int32, (tile, tile), 0)
    query_at = lax.broadcasted_iota(jnp.int32, (tile, tile), 1)
    return key_at <= query_at


def attn_fwd_kernel(tile, q_t, k_ref, v_t, o_ref, of_ref, lse_ref, s_buf):
    step = pl.program_id(0)
    query = q_t[...]

    def scores(j):
        return mm(k_ref[pl.ds(pl.multiple_of(j * tile, tile), tile), :], query)

    def keep(j, logits, top):
        s_buf[pl.ds(pl.multiple_of(j * tile, tile), tile), :] = logits
        return jnp.maximum(top, jnp.max(logits, axis=0, keepdims=True))

    top = keep(step, jnp.where(diag_mask(tile), scores(step), MASK_VALUE), jnp.full((1, tile), MASK_VALUE, F32))
    top = lax.fori_loop(0, step, lambda j, c: keep(j, scores(j), c), top)

    def weigh(j, carry):
        acc, total = carry
        at = pl.ds(pl.multiple_of(j * tile, tile), tile)
        prob = jnp.exp(s_buf[at, :] - top)
        return acc + mm(v_t[:, at], prob.astype(BF16)), total + jnp.sum(prob, axis=0, keepdims=True)

    out, total = lax.fori_loop(0, step + 1, weigh, (jnp.zeros((v_t.shape[0], tile), F32), jnp.zeros((1, tile), F32)))
    out = out / total
    lse = top + jnp.log(total)
    of_ref[...] = out
    lse_ref[...] = lse
    block = o_ref.shape[2]
    for part in range(tile // block):
        o_ref[part] = out[:, part * block:(part + 1) * block].astype(BF16)


def attention_fwd(q_t, k_in, v_t, n_blocks):
    head_dim, seq = q_t.shape
    block = seq // n_blocks
    per = TILE // block
    return pl.pallas_call(
        lambda *refs: attn_fwd_kernel(TILE, *refs),
        grid=(seq // TILE,),
        in_specs=[pl.BlockSpec((head_dim, TILE), lambda i: (0, i)), pl.BlockSpec((seq, head_dim), lambda i: (0, 0)), pl.BlockSpec((head_dim, seq), lambda i: (0, 0))],
        out_specs=[pl.BlockSpec((per, head_dim, block), lambda i: (i, 0, 0)), pl.BlockSpec((head_dim, TILE), lambda i: (0, i)), pl.BlockSpec((1, TILE), lambda i: (0, i))],
        out_shape=[jax.ShapeDtypeStruct((n_blocks, head_dim, block), BF16), jax.ShapeDtypeStruct((head_dim, seq), F32), jax.ShapeDtypeStruct((1, seq), F32)],
        scratch_shapes=[pltpu.VMEM((seq, TILE), F32)],
        cost_estimate=pl.CostEstimate(flops=8 * seq * seq * head_dim, bytes_accessed=8 * seq * head_dim, transcendentals=seq * seq),
        name='attn_fwd',
    )(q_t, k_in, v_t)


PARTS = ((0, 96), (96, 80), (176, 80))
CORE, CHIP_AXES = 1, (2, 4, 8)


def flip(dev, bit):
    return dev + bit * (1 - 2 * ((dev // bit) % 2))


def start_copy(src, dst, send_sem, recv_sem, peer):
    copy = pltpu.make_async_remote_copy(src_ref=src, dst_ref=dst, send_sem=send_sem, recv_sem=recv_sem, device_id=(peer,), device_id_type=pl.DeviceIdType.MESH)
    copy.start()
    return copy


def landed(ref, sem):
    pltpu.make_async_copy(ref, ref, sem).wait()


def enter_all(me, n_dev):
    barrier = pltpu.get_barrier_semaphore()

    @pl.loop(1, n_dev)
    def _(hop):
        pl.semaphore_signal(barrier, inc=1, device_id=(lax.rem(me + hop, n_dev),), device_id_type=pl.DeviceIdType.MESH)

    pl.semaphore_wait(barrier, n_dev - 1)


class CubeGather:
    def __init__(self, me, part, send_sem, recv_sem, core_sem):
        self.me, self.part = me, part
        self.send_sem, self.recv_sem, self.core_sem = send_sem, recv_sem, core_sem
        self.sent = []

    def axes(self, p):
        return [CHIP_AXES[(p + i) % 3] for i in range(3)]

    def owner(self, p, index, start=None):
        dev = self.me if start is None else start
        for i, bit in enumerate(self.axes(p)):
            if (index >> i) & 1:
                dev = flip(dev, bit)
        return dev

    def push(self, p, index, axis):
        ref = self.part(self.owner(p, index), p)
        start_copy(ref, ref, self.send_sem.at[len(self.sent)], self.recv_sem.at[p, index + (1 << axis)], flip(self.me, self.axes(p)[axis]))
        self.sent.append((p, index))

    def push_core(self, p, index):
        ref = self.part(self.owner(p, index), p)
        start_copy(ref, ref, self.send_sem.at[len(self.sent)], self.core_sem.at[p, index], flip(self.me, CORE))
        self.sent.append((p, index))

    def begin(self):
        for axis in range(3):
            for p in range(3):
                self.push(p, 0, axis)
        for p in range(3):
            self.push_core(p, 0)

    def receive(self, index):
        for p in range(3):
            landed(self.part(self.owner(p, index), p), self.recv_sem.at[p, index])
            for axis in range(index.bit_length(), 3):
                self.push(p, index, axis)
            self.push_core(p, index)

    def receive_core(self, index):
        for p in range(3):
            landed(self.part(self.owner(p, index, flip(self.me, CORE)), p), self.core_sem.at[p, index])

    def finish(self):
        for slot, (p, index) in enumerate(self.sent):
            landed(self.part(self.owner(p, index), p), self.send_sem.at[slot])


N_SENDS = 9 + 12 + 24


def attn_bwd_kernel(n_dev, tile, block, q_t, do_t, of_t, lse_ref, cos_ref, sin_ref, k_ref, k_t, v_ref, cos_all, sin_all, w_ref, d_blocks, d_proj_t, w_out_q, w_out_k, w_out_v, dq_acc, dk_acc, dv_acc, w_buf, send_sem, recv_sem, core_sem, local_sem):
    step = pl.program_id(0)
    last = pl.num_programs(0) - 1
    me = lax.axis_index(SEQ_AXIS)
    cube = CubeGather(me, lambda dev, p: w_buf.at[p, dev], send_sem, recv_sem, core_sem)

    @pl.when(step == 0)
    def _():
        own = [pltpu.make_async_copy(w_ref.at[p], w_buf.at[p, me], local_sem.at[p]) for p in range(3)]
        for copy in own:
            copy.start()
        enter_all(me, n_dev)
        for copy in own:
            copy.wait()
        cube.begin()

    for at_step, indices in ((4, (1,)), (5, (2,)), (6, (4,)), (7, (3,))):
        @pl.when(step == at_step)
        def _(indices=indices):
            for index in indices:
                cube.receive(index)

    head_dim = q_t.shape[0]
    query_t, d_out_t = q_t[...], do_t[...]
    lse = lse_ref[...]
    delta = jnp.sum(d_out_t.astype(F32) * of_t[...], axis=0, keepdims=True)

    @pl.when(step == 0)
    def _():
        dk_acc[...] = jnp.zeros_like(dk_acc)
        dv_acc[...] = jnp.zeros_like(dv_acc)

    dq_acc[...] = jnp.zeros_like(dq_acc)

    def visit(j, masked):
        at = pl.ds(pl.multiple_of(j * tile, tile), tile)
        prob = jnp.exp(mm(k_ref[at, :], query_t) - lse)
        if masked:
            prob = jnp.where(diag_mask(tile), prob, 0.0)
        d_prob = mm(v_ref[at, :], d_out_t).astype(BF16).astype(F32)
        d_logits = (prob * (d_prob - delta)).astype(BF16)
        dv_acc[:, at] += dot(d_out_t, prob.astype(BF16), 1, 1)
        dk_acc[:, at] += dot(query_t, d_logits, 1, 1)
        dq_acc[...] += mm(k_t[:, at], d_logits)

    visit(step, True)

    @pl.loop(0, step)
    def _(j):
        visit(j, False)

    def put(row, col_block, values):
        rows = slice(row, row + values.shape[0])
        d_proj_t[rows, pl.ds(pl.multiple_of(col_block * block, block), values.shape[1])] = values
        for part in range(values.shape[1] // block):
            d_blocks[col_block + part, rows, :] = values[:, part * block:(part + 1) * block]

    d_q = (dq_acc[...] * (head_dim ** -0.5)).astype(BF16).astype(F32)
    per = tile // block
    put(0, step * per, rope_t(d_q, cos_ref[...], -sin_ref[...]).astype(BF16))

    @pl.when(step == last)
    def _():
        @pl.loop(0, pl.num_programs(0))
        def _(j):
            at = pl.ds(pl.multiple_of(j * tile, tile), tile)
            put(head_dim, j * per, rope_t(dk_acc[:, at].astype(BF16).astype(F32), cos_all[:, at], -sin_all[:, at]).astype(BF16))
            put(2 * head_dim, j * per, dv_acc[:, at].astype(BF16))

        for index in (5, 6, 7):
            cube.receive(index)
        for index in range(8):
            cube.receive_core(index)
        flushes = [pltpu.make_async_copy(w_buf.at[p], out, local_sem.at[p]) for p, out in enumerate((w_out_q, w_out_k, w_out_v))]
        for flush in flushes:
            flush.start()
        cube.finish()
        for flush in flushes:
            flush.wait()


def attention_bwd(q_t, do_t, of_t, lse, k_in, k_t, v_in, cos_t, sin_t, w_parts, n_blocks):
    head_dim, seq = q_t.shape
    block = seq // n_blocks
    cols = pl.BlockSpec((head_dim, TILE), lambda i: (0, i))
    half_cols = pl.BlockSpec((head_dim // 2, TILE), lambda i: (0, i))
    all_rows = pl.BlockSpec((seq, head_dim), lambda i: (0, 0))
    all_cols = pl.BlockSpec((head_dim, seq), lambda i: (0, 0))
    all_half = pl.BlockSpec((head_dim // 2, seq), lambda i: (0, 0))
    w_all_shape = (3, n_blocks) + w_parts.shape[1:]
    return pl.pallas_call(
        lambda *refs: attn_bwd_kernel(n_blocks, TILE, block, *refs),
        grid=(seq // TILE,),
        in_specs=[cols, cols, cols, pl.BlockSpec((1, TILE), lambda i: (0, i)), half_cols, half_cols, all_rows, all_cols, all_rows, all_half, all_half, pl.BlockSpec(memory_space=pl.ANY)],
        out_specs=[pl.BlockSpec((n_blocks, 3 * head_dim, block), lambda i: (0, 0, 0)), pl.BlockSpec((3 * head_dim, seq), lambda i: (0, 0))] + [pl.BlockSpec(memory_space=pl.ANY)] * 3,
        out_shape=[jax.ShapeDtypeStruct((n_blocks, 3 * head_dim, block), BF16), jax.ShapeDtypeStruct((3 * head_dim, seq), BF16)] + [jax.ShapeDtypeStruct(w_all_shape[1:], BF16)] * 3,
        scratch_shapes=[
            pltpu.VMEM((head_dim, TILE), F32),
            pltpu.VMEM((head_dim, seq), F32),
            pltpu.VMEM((head_dim, seq), F32),
            pltpu.VMEM(w_all_shape, BF16),
            pltpu.SemaphoreType.DMA((N_SENDS,)),
            pltpu.SemaphoreType.DMA((3, 8)),
            pltpu.SemaphoreType.DMA((3, 8)),
            pltpu.SemaphoreType.DMA((3,)),
        ],
        compiler_params=pltpu.CompilerParams(collective_id=1, has_side_effects=True),
        cost_estimate=pl.CostEstimate(flops=20 * seq * seq * head_dim, bytes_accessed=20 * seq * head_dim, transcendentals=seq * seq),
        name='attn_bwd',
    )(q_t, do_t, of_t, lse, cos_t, sin_t, k_in, k_t, v_in, cos_t, sin_t, w_parts)


def gather_proj_kernel(n_dev, x_ref, small_ref, w_ref, freq_ref, u_out, q_t, k_t, v_t, k_out, v_out, cos_ref, sin_ref, small_all, x_buf, u_buf, w_buf, send_sem, recv_sem, core_sem, misc_send, misc_recv, local_sem, u_sem):
    me = lax.axis_index(SEQ_AXIS)
    own = pltpu.make_async_copy(x_ref, x_buf.at[me], local_sem.at[0])
    own.start()
    own_w = pltpu.make_async_copy(w_ref.at[me], w_buf.at[me], local_sem.at[1])
    own_w.start()
    own_small = pltpu.make_async_copy(small_ref, small_all.at[me], local_sem.at[2])
    own_small.start()
    enter_all(me, n_dev)
    own.wait()
    cube = CubeGather(me, lambda dev, p: x_buf.at[dev, pl.ds(PARTS[p][0], PARTS[p][1])], send_sem, recv_sem, core_sem)
    cube.begin()

    def spread(hop):
        peer = lax.rem(me + hop, n_dev)
        return [
            pltpu.make_async_remote_copy(src_ref=small_ref, dst_ref=small_all.at[me], send_sem=misc_send.at[0, hop], recv_sem=misc_recv.at[0, me], device_id=(peer,), device_id_type=pl.DeviceIdType.MESH),
            pltpu.make_async_remote_copy(src_ref=w_ref.at[peer], dst_ref=w_buf.at[me], send_sem=misc_send.at[1, hop], recv_sem=misc_recv.at[1, me], device_id=(peer,), device_id_type=pl.DeviceIdType.MESH),
        ]

    for kind in range(2):
        @pl.loop(1, n_dev)
        def _(hop, kind=kind):
            spread(hop)[kind].start()

    cube.receive(1)
    cube.receive(2)
    own_w.wait()
    own_small.wait()

    @pl.loop(1, n_dev)
    def _(hop):
        src = lax.rem(me + hop, n_dev)
        landed(small_all.at[src], misc_recv.at[0, src])
        landed(w_buf.at[src], misc_recv.at[1, src])

    width = x_ref.shape[1]
    tok = x_ref.shape[0]
    rows = w_ref.shape[1]
    gain = jnp.concatenate([small_all[d, 0:1, 0:rows] for d in range(n_dev)], axis=1)
    weight = w_buf[...].reshape(width, w_ref.shape[2])
    head_dim = q_t.shape[0]
    freq = freq_ref[:, 0:1]
    flushes = []

    @pl.loop(0, n_dev)
    def _(dev):
        at = pl.ds(pl.multiple_of(dev * tok, tok), tok)
        angle = freq * jnp.concatenate([small_all[dev, 1:2, :], small_all[dev, 2:3, :]], axis=1)
        cos_ref[:, at] = jnp.cos(angle)
        sin_ref[:, at] = jnp.sin(angle)

    def project(dev):
        act = x_buf[dev].astype(F32)
        inv = lax.rsqrt(jnp.mean(act * act, axis=-1, keepdims=True) + RMS_EPS)
        normed = (act * inv * gain).astype(BF16)
        u_buf[dev] = normed
        at = pl.ds(pl.multiple_of(dev * tok, tok), tok)
        proj = mm(normed, weight)
        proj_t = jnp.concatenate([proj, jnp.zeros((tok, 4 * head_dim - proj.shape[1]), F32)], axis=1).T
        cos_tab, sin_tab = cos_ref[:, at], sin_ref[:, at]
        query = rope_t(proj_t[:head_dim], cos_tab, sin_tab).astype(BF16).astype(F32)
        key = rope_t(proj_t[head_dim:2 * head_dim], cos_tab, sin_tab)
        q_t[:, at] = (query * (head_dim ** -0.5)).astype(BF16)
        k_t[:, at] = key.astype(BF16)
        v_t[:, at] = proj_t[2 * head_dim:3 * head_dim].astype(BF16)
        k_out[at, :] = key.T.astype(BF16)
        v_out[at, :] = proj[:, 2 * head_dim:3 * head_dim].astype(BF16)
        flush = pltpu.make_async_copy(u_buf.at[dev], u_out.at[dev], u_sem.at[len(flushes)])
        flush.start()
        flushes.append(flush)

    other = flip(me, CORE)
    cube.receive_core(0)
    project(me)
    project(other)
    cube.receive(4)
    cube.receive(3)
    for index in (1, 2, 4):
        cube.receive_core(index)
    for bit in CHIP_AXES:
        project(flip(me, bit))
        project(flip(other, bit))
    cube.receive(5)
    cube.receive(6)
    for index in (3, 5, 6):
        cube.receive_core(index)
    for skip in range(3):
        bits = [bit for i, bit in enumerate(CHIP_AXES) if i != skip]
        project(flip(flip(me, bits[0]), bits[1]))
        project(flip(flip(other, bits[0]), bits[1]))
    cube.receive(7)
    cube.receive_core(7)
    far = flip(flip(flip(me, 2), 4), 8)
    project(far)
    project(flip(far, CORE))

    cube.finish()

    @pl.loop(1, n_dev)
    def _(hop):
        for copy in spread(hop):
            copy.wait_send()

    for flush in flushes:
        flush.wait()


def gather_proj(n_dev, x_act, small, w_blocks, inv_freq, head_dim):
    tok, width = x_act.shape
    seq = tok * n_dev
    any_spec = pl.BlockSpec(memory_space=pl.ANY)
    vmem_spec = pl.BlockSpec(memory_space=pltpu.VMEM)
    return pl.pallas_call(
        lambda *refs: gather_proj_kernel(n_dev, *refs),
        in_specs=[any_spec, vmem_spec, vmem_spec, vmem_spec],
        out_specs=[any_spec] + [vmem_spec] * 8,
        out_shape=[jax.ShapeDtypeStruct((n_dev, tok, width), BF16)]
        + [jax.ShapeDtypeStruct((head_dim, seq), BF16)] * 3
        + [jax.ShapeDtypeStruct((seq, head_dim), BF16)] * 2
        + [jax.ShapeDtypeStruct((head_dim // 2, seq), F32)] * 2
        + [jax.ShapeDtypeStruct((n_dev,) + small.shape, F32)],
        scratch_shapes=[
            pltpu.VMEM((n_dev, tok, width), BF16),
            pltpu.VMEM((n_dev, tok, width), BF16),
            pltpu.VMEM(w_blocks.shape, BF16),
            pltpu.SemaphoreType.DMA((N_SENDS,)),
            pltpu.SemaphoreType.DMA((3, 8)),
            pltpu.SemaphoreType.DMA((3, 8)),
            pltpu.SemaphoreType.DMA((2, n_dev)),
            pltpu.SemaphoreType.DMA((2, n_dev)),
            pltpu.SemaphoreType.DMA((3,)),
            pltpu.SemaphoreType.DMA((n_dev,)),
        ],
        compiler_params=pltpu.CompilerParams(collective_id=0, has_side_effects=True),
        cost_estimate=pl.CostEstimate(flops=30 * seq * width * width, bytes_accessed=4 * seq * width, transcendentals=0),
        name='gather_proj',
    )(x_act, small, w_blocks, jnp.broadcast_to(inv_freq[:, None], (head_dim // 2, 128)))


def gate_backward(d_mixed, gate_pre, up_pre):
    gate_sig = jax.nn.sigmoid(gate_pre)
    d_up = (d_mixed * gate_pre * gate_sig).astype(BF16)
    d_gate = (d_mixed * up_pre * gate_sig * (1.0 + gate_pre * (1.0 - gate_sig))).astype(BF16)
    return d_gate, d_up


def join_columns_kernel(size, src, first, second):
    turned = [src[d, :size, :].T for d in range(src.shape[0])]
    rows = first.shape[0]
    first[...] = jnp.concatenate([block[:rows] for block in turned], axis=1)
    second[...] = jnp.concatenate([block[rows:] for block in turned], axis=1)


def join_columns(blocks, size):
    shape = jax.ShapeDtypeStruct((blocks.shape[2] // 2, blocks.shape[0] * size), F32)
    return pl.pallas_call(lambda *refs: join_columns_kernel(size, *refs), out_shape=[shape, shape], name='join_columns')(blocks)


def split_heads_kernel(head_dim, src, first, second, third):
    half = head_dim // 2
    for d in range(src.shape[0]):
        turned = src[d].T
        low, high = turned[:head_dim], turned[head_dim:]
        first[:, d, :] = low[:, :head_dim]
        second[:, d, :] = jnp.concatenate([low[:, head_dim:], high[:, :half]], axis=1)
        third[:, d, :] = high[:, half:]


def split_heads(blocks, head_dim):
    shape = jax.ShapeDtypeStruct((blocks.shape[2] // 2, blocks.shape[0], head_dim), F32)
    return pl.pallas_call(lambda *refs: split_heads_kernel(head_dim, *refs), out_shape=[shape] * 3, name='split_heads')(blocks)


def pack_pairs_kernel(rows, grad_t, *refs):
    out = refs[-1]
    half = grad_t.shape[0] // 2
    for d in range(out.shape[0]):
        at = slice(d * rows, (d + 1) * rows)
        out[d, :half, :] = jnp.concatenate([grad_t[:half, at], grad_t[half:, at]], axis=1)
        if len(refs) > 1:
            out[d, half:, :] = refs[0][d]


def pack_pairs(grad_t, n_dev, rows, *tail):
    height = grad_t.shape[0] // 2 + sum(part.shape[1] for part in tail)
    shape = jax.ShapeDtypeStruct((n_dev, height, 2 * rows), F32)
    return pl.pallas_call(lambda *refs: pack_pairs_kernel(rows, *refs), out_shape=shape, name='pack_pairs')(grad_t, *tail)


def device_step(n_dev, x_act, positions, grad_out, g_attn_s, w_q, w_k, w_v, w_o, g_mlp_s, w_gate, w_up, w_down):
    tok, width = x_act.shape
    seq = tok * n_dev
    rows, heads, head_dim = w_q.shape
    ff = w_gate.shape[1]
    ff_s = ff // n_dev

    small = jnp.concatenate([jnp.concatenate([g_attn_s, g_mlp_s]).astype(F32)[None], positions.astype(F32).reshape(-1, 2 * rows)], axis=0)
    small = jnp.pad(small, ((0, 8 - small.shape[0]), (0, 0)))
    w_qkv = jnp.concatenate([w_q, w_k, w_v], axis=2)
    w_blocks = jnp.transpose(w_qkv, (1, 0, 2))
    inv_freq = ROPE_BASE ** (-(jnp.arange(head_dim // 2, dtype=F32) * (2.0 / head_dim)))
    u_all, q_t, k_t, v_t, k_in, v_in, cos_t, sin_t, small_all = gather_proj(n_dev, x_act, small, w_blocks, inv_freq, head_dim)
    u_all = u_all.reshape(seq, width)
    g_attn = small_all[:, 0, :rows].reshape(width)
    g_mlp = small_all[:, 0, rows:2 * rows].reshape(width)

    down_groups = [w_down[i:i + rows] for i in range(0, ff_s, rows)]
    down_groups = [jnp.pad(group, ((0, rows - group.shape[0]), (0, 0))) for group in down_groups]
    w_all = gather(jnp.concatenate([w_gate, w_up, w_o[0]] + down_groups, axis=1))
    w_gu = w_all[:, :2 * ff]
    w_o_all = w_all[:, 2 * ff:2 * ff + width]
    w_down_at = 2 * ff + width
    down_all = [w_all[:, w_down_at + i * width:w_down_at + (i + 1) * width].reshape(n_dev, rows, width) for i in range(len(down_groups))]
    w_down_all = jnp.concatenate(down_all, axis=1)[:, :ff_s].reshape(ff, width)
    me = lax.axis_index(SEQ_AXIS)
    w_cols = jnp.concatenate([lax.dynamic_slice(w_all, (0, at + me * ff_s), (width, ff_s)) for at in (0, ff)], axis=1)

    o_blocks, of_t, lse = attention_fwd(q_t, k_in, v_t, n_dev)
    o_loc = exchange(o_blocks).reshape(width, tok)
    w_parts = jnp.stack([w.reshape(rows, heads * head_dim) for w in (w_q, w_k, w_v)])
    o_loc, w_parts = lax.optimization_barrier((o_loc, w_parts))

    hidden = (x_act.astype(F32) + dot(o_loc, w_o_all, 0, 0)).astype(BF16)
    normed_mlp, inv_rms_mlp = rms_norm(hidden, g_mlp)
    a_dy = jnp.concatenate([normed_mlp, grad_out], axis=1)
    normed_mlp, a_dy = lax.optimization_barrier((normed_mlp, a_dy))
    a_dy = gather(a_dy)
    pre = with_layout_constraint(dot(normed_mlp, w_gu, 1, 0), Layout(major_to_minor=(0, 1)))
    gate_pre, up_pre = pre[:, :ff], pre[:, ff:]
    mixed = (jax.nn.silu(gate_pre) * up_pre).astype(BF16)
    y_out = (hidden.astype(F32) + dot(mixed, w_down_all, 1, 0)).astype(BF16)

    d_mixed = dot(grad_out, w_down_all, 1, 1).astype(BF16).astype(F32)
    d_gu = jnp.concatenate(gate_backward(d_mixed, gate_pre, up_pre), axis=1)
    d_normed = dot(d_gu, w_gu, 1, 1).astype(BF16)
    d_hid_norm, part_g_mlp = rms_norm_bwd(hidden, g_mlp, inv_rms_mlp, d_normed)
    d_hidden = (grad_out.astype(F32) + d_hid_norm).astype(BF16)
    do_blocks = exchange(dot(w_o_all, d_hidden, 1, 1).astype(BF16).reshape(n_dev, head_dim, tok))
    half_n = n_dev // 2
    pairs = [(i, (i + half_n) % n_dev) for i in range(n_dev)]
    near = (me // half_n) * half_n
    o_far = lax.ppermute(lax.dynamic_slice_in_dim(o_blocks, half_n - near, half_n), SEQ_AXIS, pairs)
    do_blocks, y_out = lax.optimization_barrier((do_blocks, y_out))
    dh_half = lax.all_gather(d_hidden, SEQ_AXIS, axis=0, tiled=True, axis_index_groups=[list(range(half_n)), list(range(half_n, n_dev))])

    do_t = jnp.transpose(do_blocks, (1, 0, 2)).reshape(head_dim, seq)
    d_blocks, d_proj_t, *w_qkv_all = attention_bwd(q_t, do_t, of_t, lse, k_in, k_t, v_in, cos_t, sin_t, w_parts, n_dev)
    d_proj = exchange(d_blocks)

    attn_send = pack_pairs(dot(d_proj_t, u_all, 1, 0), n_dev, rows)
    d_proj, attn_send = lax.optimization_barrier((d_proj, attn_send))
    attn_back = exchange(attn_send)
    d_proj = d_proj.reshape(heads, 3, head_dim, tok)
    inv_rms = lax.rsqrt(jnp.mean(jnp.square(x_act.astype(F32)), axis=-1, keepdims=True) + RMS_EPS)
    d_u = sum(dot(d_proj[:, p].reshape(heads * head_dim, tok), w_qkv_all[p].reshape(width, heads * head_dim), 0, 1) for p in range(3)).astype(BF16)
    d_x_norm, part_g_attn = rms_norm_bwd(x_act, g_attn, inv_rms, d_u)
    grad_x = (d_hidden.astype(F32) + d_x_norm).astype(BF16)
    gain_send = jnp.concatenate([part_g_attn.reshape(n_dev, 1, rows), part_g_mlp.reshape(n_dev, 1, rows)], axis=2)

    a_all, dy_all = a_dy[:, :width], a_dy[:, width:]
    pre_t = dot(w_cols, a_all, 0, 1)
    gate_t, up_t = pre_t[:ff_s], pre_t[ff_s:]
    d_mixed_t = dot(w_down, dy_all, 1, 1).astype(BF16).astype(F32)
    mixed_t = (jax.nn.silu(gate_t) * up_t).astype(BF16)
    d_gu_t = jnp.concatenate(gate_backward(d_mixed_t, gate_t, up_t), axis=0)
    mlp_send = pack_pairs(dot(d_gu_t, a_all, 1, 0), n_dev, rows, jnp.pad(gain_send, ((0, 0), (0, 7), (0, 0))))
    attn_back, mlp_send, mixed_t = lax.optimization_barrier((attn_back, mlp_send, mixed_t))
    mlp_back = exchange(mlp_send)
    grad_w_down = dot(mixed_t, dy_all, 1, 0)

    o_far, dh_half, o_blocks, grad_w_down = lax.optimization_barrier((o_far, dh_half, o_blocks, grad_w_down))
    o_pair = jnp.concatenate([lax.dynamic_slice_in_dim(o_blocks, near, half_n), o_far], axis=1)
    part_w_o = dot(o_pair.transpose(1, 0, 2).reshape(2 * head_dim, seq // 2), dh_half, 1, 0)
    grad_w_o = (part_w_o[:head_dim] + lax.ppermute(part_w_o[head_dim:], SEQ_AXIS, pairs))[None]

    grad_w_q, grad_w_k, grad_w_v = split_heads(attn_back, head_dim)
    mlp_back, grad_w_down, grad_w_q, grad_w_k, grad_w_v, grad_w_o = lax.optimization_barrier((mlp_back, grad_w_down, grad_w_q, grad_w_k, grad_w_v, grad_w_o))
    gains = jnp.sum(mlp_back[:, ff_s], axis=0)
    grad_g_attn, grad_g_mlp = gains[:rows], gains[rows:]
    grad_w_gate, grad_w_up = join_columns(mlp_back, ff_s)
    return (y_out, grad_x, grad_g_attn, grad_w_q, grad_w_k, grad_w_v, grad_w_o, grad_g_mlp, grad_w_gate, grad_w_up, grad_w_down)


def solution(mesh):
    n_dev = mesh.shape[SEQ_AXIS]
    token_spec = P(SEQ_AXIS, None)
    cube_spec = P(SEQ_AXIS, None, None)
    gain_spec = P(SEQ_AXIS)
    weight_specs = (gain_spec, cube_spec, cube_spec, cube_spec, cube_spec, gain_spec, token_spec, token_spec, token_spec)
    return jax.shard_map(lambda *args: device_step(n_dev, *args), mesh=mesh, in_specs=(token_spec, gain_spec, token_spec) + weight_specs, out_specs=(token_spec, token_spec) + weight_specs, check_vma=False)
```

```python
import jax
import jax.numpy as jnp
from jax import lax
from jax.experimental import pallas as pl
from jax.experimental.layout import Layout, with_layout_constraint
from jax.experimental.pallas import tpu as pltpu
from jax.sharding import PartitionSpec as P

SEQ_AXIS = 'sp'
RMS_EPS = 1e-5
ROPE_BASE = 10000.0
MASK_VALUE = -1e30
TILE = 512
F32 = jnp.float32
BF16 = jnp.bfloat16


def rms_norm(act_in, gain_vec):
    act_f = act_in.astype(F32)
    inv_rms = lax.rsqrt(jnp.mean(act_f * act_f, axis=-1, keepdims=True) + RMS_EPS)
    return (act_f * inv_rms * gain_vec.astype(F32)).astype(BF16), inv_rms


def rms_norm_bwd(act_in, gain_vec, inv_rms, d_normed):
    act_f = act_in.astype(F32)
    d_f = d_normed.astype(F32)
    scaled_d = d_f * gain_vec.astype(F32)
    proj_mean = jnp.mean(scaled_d * act_f, axis=-1, keepdims=True)
    d_act = inv_rms * scaled_d - act_f * (inv_rms * inv_rms * inv_rms) * proj_mean
    d_gain = jnp.sum(d_f * act_f * inv_rms, axis=0)
    return d_act, d_gain


def dot(lhs, rhs, l_dim, r_dim):
    return lax.dot_general(lhs, rhs, (((l_dim,), (r_dim,)), ((), ())), preferred_element_type=F32)


def gather(shard):
    return lax.all_gather(shard, SEQ_AXIS, axis=0, tiled=True)


def exchange(blocks):
    return lax.all_to_all(blocks, SEQ_AXIS, 0, 0, tiled=True)


def rope_t(vals, cos_tab, sin_tab):
    half = vals.shape[0] // 2
    first, second = vals[:half], vals[half:]
    return jnp.concatenate([first * cos_tab - second * sin_tab, second * cos_tab + first * sin_tab], axis=0)


def mm(lhs, rhs):
    return jnp.dot(lhs, rhs, preferred_element_type=F32)


def diag_mask(tile):
    key_at = lax.broadcasted_iota(jnp.int32, (tile, tile), 0)
    query_at = lax.broadcasted_iota(jnp.int32, (tile, tile), 1)
    return key_at <= query_at


def attn_fwd_kernel(tile, q_t, k_ref, v_t, o_ref, of_ref, lse_ref, s_buf):
    step = pl.program_id(0)
    query = q_t[...]

    def scores(j):
        return mm(k_ref[pl.ds(pl.multiple_of(j * tile, tile), tile), :], query)

    def keep(j, logits, top):
        s_buf[pl.ds(pl.multiple_of(j * tile, tile), tile), :] = logits
        return jnp.maximum(top, jnp.max(logits, axis=0, keepdims=True))

    top = keep(step, jnp.where(diag_mask(tile), scores(step), MASK_VALUE), jnp.full((1, tile), MASK_VALUE, F32))
    top = lax.fori_loop(0, step, lambda j, c: keep(j, scores(j), c), top)

    def weigh(j, carry):
        acc, total = carry
        at = pl.ds(pl.multiple_of(j * tile, tile), tile)
        prob = jnp.exp(s_buf[at, :] - top)
        return acc + mm(v_t[:, at], prob.astype(BF16)), total + jnp.sum(prob, axis=0, keepdims=True)

    out, total = lax.fori_loop(0, step + 1, weigh, (jnp.zeros((v_t.shape[0], tile), F32), jnp.zeros((1, tile), F32)))
    out = out / total
    lse = top + jnp.log(total)
    of_ref[...] = out
    lse_ref[...] = lse
    block = o_ref.shape[2]
    for part in range(tile // block):
        o_ref[part] = out[:, part * block:(part + 1) * block].astype(BF16)


def attention_fwd(q_t, k_in, v_t, n_blocks):
    head_dim, seq = q_t.shape
    block = seq // n_blocks
    per = TILE // block
    return pl.pallas_call(
        lambda *refs: attn_fwd_kernel(TILE, *refs),
        grid=(seq // TILE,),
        in_specs=[pl.BlockSpec((head_dim, TILE), lambda i: (0, i)), pl.BlockSpec((seq, head_dim), lambda i: (0, 0)), pl.BlockSpec((head_dim, seq), lambda i: (0, 0))],
        out_specs=[pl.BlockSpec((per, head_dim, block), lambda i: (i, 0, 0)), pl.BlockSpec((head_dim, TILE), lambda i: (0, i)), pl.BlockSpec((1, TILE), lambda i: (0, i))],
        out_shape=[jax.ShapeDtypeStruct((n_blocks, head_dim, block), BF16), jax.ShapeDtypeStruct((head_dim, seq), F32), jax.ShapeDtypeStruct((1, seq), F32)],
        scratch_shapes=[pltpu.VMEM((seq, TILE), F32)],
        cost_estimate=pl.CostEstimate(flops=8 * seq * seq * head_dim, bytes_accessed=8 * seq * head_dim, transcendentals=seq * seq),
        name='attn_fwd',
    )(q_t, k_in, v_t)


PARTS = ((0, 96), (96, 80), (176, 80))
CORE, CHIP_AXES = 1, (2, 4, 8)


def flip(dev, bit):
    return dev + bit * (1 - 2 * ((dev // bit) % 2))


def start_copy(src, dst, send_sem, recv_sem, peer):
    copy = pltpu.make_async_remote_copy(src_ref=src, dst_ref=dst, send_sem=send_sem, recv_sem=recv_sem, device_id=(peer,), device_id_type=pl.DeviceIdType.MESH)
    copy.start()
    return copy


def landed(ref, sem):
    pltpu.make_async_copy(ref, ref, sem).wait()


def enter_all(me, n_dev):
    barrier = pltpu.get_barrier_semaphore()

    @pl.loop(1, n_dev)
    def _(hop):
        pl.semaphore_signal(barrier, inc=1, device_id=(lax.rem(me + hop, n_dev),), device_id_type=pl.DeviceIdType.MESH)

    pl.semaphore_wait(barrier, n_dev - 1)


class CubeGather:
    def __init__(self, me, part, send_sem, recv_sem, core_sem):
        self.me, self.part = me, part
        self.send_sem, self.recv_sem, self.core_sem = send_sem, recv_sem, core_sem
        self.sent = []

    def axes(self, p):
        return [CHIP_AXES[(p + i) % 3] for i in range(3)]

    def owner(self, p, index, start=None):
        dev = self.me if start is None else start
        for i, bit in enumerate(self.axes(p)):
            if (index >> i) & 1:
                dev = flip(dev, bit)
        return dev

    def push(self, p, index, axis):
        ref = self.part(self.owner(p, index), p)
        start_copy(ref, ref, self.send_sem.at[len(self.sent)], self.recv_sem.at[p, index + (1 << axis)], flip(self.me, self.axes(p)[axis]))
        self.sent.append((p, index))

    def push_core(self, p, index):
        ref = self.part(self.owner(p, index), p)
        start_copy(ref, ref, self.send_sem.at[len(self.sent)], self.core_sem.at[p, index], flip(self.me, CORE))
        self.sent.append((p, index))

    def begin(self):
        for axis in range(3):
            for p in range(3):
                self.push(p, 0, axis)
        for p in range(3):
            self.push_core(p, 0)

    def receive(self, index):
        for p in range(3):
            landed(self.part(self.owner(p, index), p), self.recv_sem.at[p, index])
            for axis in range(index.bit_length(), 3):
                self.push(p, index, axis)
            self.push_core(p, index)

    def receive_core(self, index):
        for p in range(3):
            landed(self.part(self.owner(p, index, flip(self.me, CORE)), p), self.core_sem.at[p, index])

    def finish(self):
        for slot, (p, index) in enumerate(self.sent):
            landed(self.part(self.owner(p, index), p), self.send_sem.at[slot])


N_SENDS = 9 + 12 + 24


def attn_bwd_kernel(n_dev, tile, block, q_t, do_t, of_t, lse_ref, cos_ref, sin_ref, k_ref, k_t, v_ref, cos_all, sin_all, w_ref, d_blocks, d_proj_t, w_out_q, w_out_k, w_out_v, dq_acc, dk_acc, dv_acc, w_buf, send_sem, recv_sem, core_sem, local_sem):
    step = pl.program_id(0)
    last = pl.num_programs(0) - 1
    me = lax.axis_index(SEQ_AXIS)
    cube = CubeGather(me, lambda dev, p: w_buf.at[p, dev], send_sem, recv_sem, core_sem)

    @pl.when(step == 0)
    def _():
        own = [pltpu.make_async_copy(w_ref.at[p], w_buf.at[p, me], local_sem.at[p]) for p in range(3)]
        for copy in own:
            copy.start()
        enter_all(me, n_dev)
        for copy in own:
            copy.wait()
        cube.begin()

    for at_step, indices in ((4, (1,)), (5, (2,)), (6, (4,)), (7, (3,))):
        @pl.when(step == at_step)
        def _(indices=indices):
            for index in indices:
                cube.receive(index)

    head_dim = q_t.shape[0]
    query_t, d_out_t = q_t[...], do_t[...]
    lse = lse_ref[...]
    delta = jnp.sum(d_out_t.astype(F32) * of_t[...], axis=0, keepdims=True)

    @pl.when(step == 0)
    def _():
        dk_acc[...] = jnp.zeros_like(dk_acc)
        dv_acc[...] = jnp.zeros_like(dv_acc)

    dq_acc[...] = jnp.zeros_like(dq_acc)

    def visit(j, masked):
        at = pl.ds(pl.multiple_of(j * tile, tile), tile)
        prob = jnp.exp(mm(k_ref[at, :], query_t) - lse)
        if masked:
            prob = jnp.where(diag_mask(tile), prob, 0.0)
        d_prob = mm(v_ref[at, :], d_out_t).astype(BF16).astype(F32)
        d_logits = (prob * (d_prob - delta)).astype(BF16)
        dv_acc[:, at] += dot(d_out_t, prob.astype(BF16), 1, 1)
        dk_acc[:, at] += dot(query_t, d_logits, 1, 1)
        dq_acc[...] += mm(k_t[:, at], d_logits)

    visit(step, True)

    @pl.loop(0, step)
    def _(j):
        visit(j, False)

    def put(row, col_block, values):
        rows = slice(row, row + values.shape[0])
        d_proj_t[rows, pl.ds(pl.multiple_of(col_block * block, block), values.shape[1])] = values
        for part in range(values.shape[1] // block):
            d_blocks[col_block + part, rows, :] = values[:, part * block:(part + 1) * block]

    d_q = (dq_acc[...] * (head_dim ** -0.5)).astype(BF16).astype(F32)
    per = tile // block
    put(0, step * per, rope_t(d_q, cos_ref[...], -sin_ref[...]).astype(BF16))

    @pl.when(step == last)
    def _():
        @pl.loop(0, pl.num_programs(0))
        def _(j):
            at = pl.ds(pl.multiple_of(j * tile, tile), tile)
            put(head_dim, j * per, rope_t(dk_acc[:, at].astype(BF16).astype(F32), cos_all[:, at], -sin_all[:, at]).astype(BF16))
            put(2 * head_dim, j * per, dv_acc[:, at].astype(BF16))

        for index in (5, 6, 7):
            cube.receive(index)
        for index in range(8):
            cube.receive_core(index)
        flushes = [pltpu.make_async_copy(w_buf.at[p], out, local_sem.at[p]) for p, out in enumerate((w_out_q, w_out_k, w_out_v))]
        for flush in flushes:
            flush.start()
        cube.finish()
        for flush in flushes:
            flush.wait()


def attention_bwd(q_t, do_t, of_t, lse, k_in, k_t, v_in, cos_t, sin_t, w_parts, n_blocks):
    head_dim, seq = q_t.shape
    block = seq // n_blocks
    cols = pl.BlockSpec((head_dim, TILE), lambda i: (0, i))
    half_cols = pl.BlockSpec((head_dim // 2, TILE), lambda i: (0, i))
    all_rows = pl.BlockSpec((seq, head_dim), lambda i: (0, 0))
    all_cols = pl.BlockSpec((head_dim, seq), lambda i: (0, 0))
    all_half = pl.BlockSpec((head_dim // 2, seq), lambda i: (0, 0))
    w_all_shape = (3, n_blocks) + w_parts.shape[1:]
    return pl.pallas_call(
        lambda *refs: attn_bwd_kernel(n_blocks, TILE, block, *refs),
        grid=(seq // TILE,),
        in_specs=[cols, cols, cols, pl.BlockSpec((1, TILE), lambda i: (0, i)), half_cols, half_cols, all_rows, all_cols, all_rows, all_half, all_half, pl.BlockSpec(memory_space=pl.ANY)],
        out_specs=[pl.BlockSpec((n_blocks, 3 * head_dim, block), lambda i: (0, 0, 0)), pl.BlockSpec((3 * head_dim, seq), lambda i: (0, 0))] + [pl.BlockSpec(memory_space=pl.ANY)] * 3,
        out_shape=[jax.ShapeDtypeStruct((n_blocks, 3 * head_dim, block), BF16), jax.ShapeDtypeStruct((3 * head_dim, seq), BF16)] + [jax.ShapeDtypeStruct(w_all_shape[1:], BF16)] * 3,
        scratch_shapes=[
            pltpu.VMEM((head_dim, TILE), F32),
            pltpu.VMEM((head_dim, seq), F32),
            pltpu.VMEM((head_dim, seq), F32),
            pltpu.VMEM(w_all_shape, BF16),
            pltpu.SemaphoreType.DMA((N_SENDS,)),
            pltpu.SemaphoreType.DMA((3, 8)),
            pltpu.SemaphoreType.DMA((3, 8)),
            pltpu.SemaphoreType.DMA((3,)),
        ],
        compiler_params=pltpu.CompilerParams(collective_id=1, has_side_effects=True),
        cost_estimate=pl.CostEstimate(flops=20 * seq * seq * head_dim, bytes_accessed=20 * seq * head_dim, transcendentals=seq * seq),
        name='attn_bwd',
    )(q_t, do_t, of_t, lse, cos_t, sin_t, k_in, k_t, v_in, cos_t, sin_t, w_parts)


def gather_proj_kernel(n_dev, x_ref, small_ref, w_ref, u_out, proj_t, small_all, x_buf, u_buf, w_buf, send_sem, recv_sem, core_sem, misc_send, misc_recv, local_sem, u_sem):
    me = lax.axis_index(SEQ_AXIS)
    own = pltpu.make_async_copy(x_ref, x_buf.at[me], local_sem.at[0])
    own.start()
    own_w = pltpu.make_async_copy(w_ref.at[me], w_buf.at[me], local_sem.at[1])
    own_w.start()
    own_small = pltpu.make_async_copy(small_ref, small_all.at[me], local_sem.at[2])
    own_small.start()
    enter_all(me, n_dev)
    own.wait()
    cube = CubeGather(me, lambda dev, p: x_buf.at[dev, pl.ds(PARTS[p][0], PARTS[p][1])], send_sem, recv_sem, core_sem)
    cube.begin()

    def spread(hop):
        peer = lax.rem(me + hop, n_dev)
        return [
            pltpu.make_async_remote_copy(src_ref=small_ref, dst_ref=small_all.at[me], send_sem=misc_send.at[0, hop], recv_sem=misc_recv.at[0, me], device_id=(peer,), device_id_type=pl.DeviceIdType.MESH),
            pltpu.make_async_remote_copy(src_ref=w_ref.at[peer], dst_ref=w_buf.at[me], send_sem=misc_send.at[1, hop], recv_sem=misc_recv.at[1, me], device_id=(peer,), device_id_type=pl.DeviceIdType.MESH),
        ]

    for kind in range(2):
        @pl.loop(1, n_dev)
        def _(hop, kind=kind):
            spread(hop)[kind].start()

    cube.receive(1)
    cube.receive(2)
    own_w.wait()
    own_small.wait()

    @pl.loop(1, n_dev)
    def _(hop):
        src = lax.rem(me + hop, n_dev)
        landed(small_all.at[src], misc_recv.at[0, src])
        landed(w_buf.at[src], misc_recv.at[1, src])

    width = x_ref.shape[1]
    tok = x_ref.shape[0]
    rows = w_ref.shape[1]
    gain = jnp.concatenate([small_all[d, 0:1, 0:rows] for d in range(n_dev)], axis=1)
    weight = w_buf[...].reshape(width, w_ref.shape[2])
    keep = proj_t.shape[0]

    def project(dev):
        act = x_buf[dev].astype(F32)
        inv = lax.rsqrt(jnp.mean(act * act, axis=-1, keepdims=True) + RMS_EPS)
        normed = (act * inv * gain).astype(BF16)
        u_buf[dev] = normed
        proj_t[:, pl.ds(pl.multiple_of(dev * tok, tok), tok)] = mm(normed, weight).T[:keep]
        pltpu.make_async_copy(u_buf.at[dev], u_out.at[dev], u_sem.at[dev]).start()

    def project_pair(dev):
        @pl.loop(0, 2)
        def _(core):
            project(dev + core * (flip(dev, CORE) - dev))

    def project_across(dev):
        @pl.loop(0, 3)
        def _(i):
            project_pair(flip(dev, i * (i + 1) + 2))

    cube.receive_core(0)
    project_pair(me)
    cube.receive(4)
    cube.receive(3)
    for index in (1, 2, 4):
        cube.receive_core(index)
    project_across(me)
    cube.receive(5)
    cube.receive(6)
    for index in (3, 5, 6):
        cube.receive_core(index)
    far = flip(flip(flip(me, 2), 4), 8)
    project_across(far)
    cube.receive(7)
    cube.receive_core(7)
    project_pair(far)

    cube.finish()

    @pl.loop(1, n_dev)
    def _(hop):
        for copy in spread(hop):
            copy.wait_send()

    @pl.loop(0, n_dev)
    def _(dev):
        pltpu.make_async_copy(u_buf.at[dev], u_out.at[dev], u_sem.at[dev]).wait()


def gather_proj(n_dev, x_act, small, w_blocks, qkv):
    tok, width = x_act.shape
    seq = tok * n_dev
    any_spec = pl.BlockSpec(memory_space=pl.ANY)
    vmem_spec = pl.BlockSpec(memory_space=pltpu.VMEM)
    return pl.pallas_call(
        lambda *refs: gather_proj_kernel(n_dev, *refs),
        in_specs=[any_spec, vmem_spec, vmem_spec],
        out_specs=[any_spec, vmem_spec, vmem_spec],
        out_shape=[jax.ShapeDtypeStruct((n_dev, tok, width), BF16), jax.ShapeDtypeStruct((qkv, seq), F32), jax.ShapeDtypeStruct((n_dev,) + small.shape, F32)],
        scratch_shapes=[
            pltpu.VMEM((n_dev, tok, width), BF16),
            pltpu.VMEM((n_dev, tok, width), BF16),
            pltpu.VMEM(w_blocks.shape, BF16),
            pltpu.SemaphoreType.DMA((N_SENDS,)),
            pltpu.SemaphoreType.DMA((3, 8)),
            pltpu.SemaphoreType.DMA((3, 8)),
            pltpu.SemaphoreType.DMA((2, n_dev)),
            pltpu.SemaphoreType.DMA((2, n_dev)),
            pltpu.SemaphoreType.DMA((3,)),
            pltpu.SemaphoreType.DMA((n_dev,)),
        ],
        compiler_params=pltpu.CompilerParams(collective_id=0, has_side_effects=True),
        cost_estimate=pl.CostEstimate(flops=30 * seq * width * width, bytes_accessed=4 * seq * width, transcendentals=0),
        name='gather_proj',
    )(x_act, small, w_blocks)


def gate_backward(d_mixed, gate_pre, up_pre):
    gate_sig = jax.nn.sigmoid(gate_pre)
    d_up = (d_mixed * gate_pre * gate_sig).astype(BF16)
    d_gate = (d_mixed * up_pre * gate_sig * (1.0 + gate_pre * (1.0 - gate_sig))).astype(BF16)
    return d_gate, d_up


def join_columns_kernel(size, src, first, second):
    turned = [src[d, :size, :].T for d in range(src.shape[0])]
    rows = first.shape[0]
    first[...] = jnp.concatenate([block[:rows] for block in turned], axis=1)
    second[...] = jnp.concatenate([block[rows:] for block in turned], axis=1)


def join_columns(blocks, size):
    shape = jax.ShapeDtypeStruct((blocks.shape[2] // 2, blocks.shape[0] * size), F32)
    return pl.pallas_call(lambda *refs: join_columns_kernel(size, *refs), out_shape=[shape, shape], name='join_columns')(blocks)


def split_heads_kernel(head_dim, src, first, second, third):
    half = head_dim // 2
    for d in range(src.shape[0]):
        turned = src[d].T
        low, high = turned[:head_dim], turned[head_dim:]
        first[:, d, :] = low[:, :head_dim]
        second[:, d, :] = jnp.concatenate([low[:, head_dim:], high[:, :half]], axis=1)
        third[:, d, :] = high[:, half:]


def split_heads(blocks, head_dim):
    shape = jax.ShapeDtypeStruct((blocks.shape[2] // 2, blocks.shape[0], head_dim), F32)
    return pl.pallas_call(lambda *refs: split_heads_kernel(head_dim, *refs), out_shape=[shape] * 3, name='split_heads')(blocks)


def pack_pairs_kernel(rows, grad_t, *refs):
    out = refs[-1]
    half = grad_t.shape[0] // 2
    for d in range(out.shape[0]):
        at = slice(d * rows, (d + 1) * rows)
        out[d, :half, :] = jnp.concatenate([grad_t[:half, at], grad_t[half:, at]], axis=1)
        if len(refs) > 1:
            out[d, half:, :] = refs[0][d]


def pack_pairs(grad_t, n_dev, rows, *tail):
    height = grad_t.shape[0] // 2 + sum(part.shape[1] for part in tail)
    shape = jax.ShapeDtypeStruct((n_dev, height, 2 * rows), F32)
    return pl.pallas_call(lambda *refs: pack_pairs_kernel(rows, *refs), out_shape=shape, name='pack_pairs')(grad_t, *tail)


def weight_block_kernel(gate, up, w_o, down, out):
    rows = gate.shape[0]
    at = 0
    for part in (gate[...], up[...], w_o[0]):
        out[:, at:at + part.shape[1]] = part
        at += part.shape[1]
    for start in range(0, down.shape[0], rows):
        height = min(rows, down.shape[0] - start)
        out[:height, at:at + down.shape[1]] = down[start:start + height, :]
        if height < rows:
            out[height:, at:at + down.shape[1]] = jnp.zeros((rows - height, down.shape[1]), BF16)
        at += down.shape[1]


def weight_block(gate, up, w_o, down):
    rows = gate.shape[0]
    width = 2 * gate.shape[1] + w_o.shape[2] + pl.cdiv(down.shape[0], rows) * down.shape[1]
    return pl.pallas_call(weight_block_kernel, out_shape=jax.ShapeDtypeStruct((rows, width), BF16), name='weight_block')(gate, up, w_o, down)


def device_step(n_dev, x_act, positions, grad_out, g_attn_s, w_q, w_k, w_v, w_o, g_mlp_s, w_gate, w_up, w_down):
    tok, width = x_act.shape
    seq = tok * n_dev
    rows, heads, head_dim = w_q.shape
    ff = w_gate.shape[1]
    ff_s = ff // n_dev
    qkv = 3 * head_dim

    small = jnp.concatenate([jnp.concatenate([g_attn_s, g_mlp_s]).astype(F32)[None], positions.astype(F32).reshape(-1, 2 * rows)], axis=0)
    small = jnp.pad(small, ((0, 8 - small.shape[0]), (0, 0)))
    w_qkv = jnp.concatenate([w_q, w_k, w_v], axis=2)
    w_blocks = jnp.pad(jnp.transpose(w_qkv, (1, 0, 2)), ((0, 0), (0, 0), (0, 256 - qkv)))
    u_all, proj_t, small_all = gather_proj(n_dev, x_act, small, w_blocks, qkv)
    u_all = u_all.reshape(seq, width)
    g_attn = small_all[:, 0, :rows].reshape(width)
    g_mlp = small_all[:, 0, rows:2 * rows].reshape(width)
    pos_all = small_all[:, 1:1 + tok // (2 * rows)]

    w_all = gather(weight_block(w_gate, w_up, w_o, w_down))
    w_gu = w_all[:, :2 * ff]
    w_o_all = w_all[:, 2 * ff:2 * ff + width]
    w_down_at = 2 * ff + width
    down_all = [w_all[:, w_down_at + i * width:w_down_at + (i + 1) * width].reshape(n_dev, rows, width) for i in range(pl.cdiv(ff_s, rows))]
    w_down_all = jnp.concatenate(down_all, axis=1)[:, :ff_s].reshape(ff, width)
    me = lax.axis_index(SEQ_AXIS)
    w_cols = jnp.concatenate([lax.dynamic_slice(w_all, (0, at + me * ff_s), (width, ff_s)) for at in (0, ff)], axis=1)

    half = head_dim // 2
    inv_freq = ROPE_BASE ** (-(jnp.arange(half, dtype=F32) * (2.0 / head_dim)))
    angle_t = inv_freq[:, None] * pos_all.reshape(1, seq)
    cos_t, sin_t = jnp.cos(angle_t), jnp.sin(angle_t)

    q_t = (rope_t(proj_t[:head_dim], cos_t, sin_t).astype(BF16).astype(F32) * (head_dim ** -0.5)).astype(BF16)
    k_t = rope_t(proj_t[head_dim:2 * head_dim], cos_t, sin_t).astype(BF16)
    v_t = proj_t[2 * head_dim:].astype(BF16)
    k_in, v_in = k_t.T, v_t.T
    o_blocks, of_t, lse = attention_fwd(q_t, k_in, v_t, n_dev)
    o_loc = exchange(o_blocks).reshape(width, tok)
    w_parts = jnp.stack([w.reshape(rows, heads * head_dim) for w in (w_q, w_k, w_v)])
    o_loc, w_parts, v_in, w_down_all = lax.optimization_barrier((o_loc, w_parts, v_in, w_down_all))

    hidden = (x_act.astype(F32) + dot(o_loc, w_o_all, 0, 0)).astype(BF16)
    normed_mlp, inv_rms_mlp = rms_norm(hidden, g_mlp)
    a_dy = jnp.concatenate([normed_mlp, grad_out], axis=1)
    normed_mlp, a_dy = lax.optimization_barrier((normed_mlp, a_dy))
    a_dy = gather(a_dy)
    pre = with_layout_constraint(dot(normed_mlp, w_gu, 1, 0), Layout(major_to_minor=(0, 1)))
    gate_pre, up_pre = pre[:, :ff], pre[:, ff:]
    mixed = (jax.nn.silu(gate_pre) * up_pre).astype(BF16)
    y_out = (hidden.astype(F32) + dot(mixed, w_down_all, 1, 0)).astype(BF16)

    d_mixed = dot(grad_out, w_down_all, 1, 1).astype(BF16).astype(F32)
    d_gu = jnp.concatenate(gate_backward(d_mixed, gate_pre, up_pre), axis=1)
    d_normed = dot(d_gu, w_gu, 1, 1).astype(BF16)
    d_hid_norm, part_g_mlp = rms_norm_bwd(hidden, g_mlp, inv_rms_mlp, d_normed)
    d_hidden = (grad_out.astype(F32) + d_hid_norm).astype(BF16)
    do_blocks = exchange(dot(w_o_all, d_hidden, 1, 1).astype(BF16).reshape(n_dev, head_dim, tok))
    half_n = n_dev // 2
    pairs = [(i, (i + half_n) % n_dev) for i in range(n_dev)]
    near = (me // half_n) * half_n
    o_far = lax.ppermute(lax.dynamic_slice_in_dim(o_blocks, half_n - near, half_n), SEQ_AXIS, pairs)
    do_blocks, y_out = lax.optimization_barrier((do_blocks, y_out))
    dh_half = lax.all_gather(d_hidden, SEQ_AXIS, axis=0, tiled=True, axis_index_groups=[list(range(half_n)), list(range(half_n, n_dev))])

    do_t = jnp.transpose(do_blocks, (1, 0, 2)).reshape(head_dim, seq)
    d_blocks, d_proj_t, *w_qkv_all = attention_bwd(q_t, do_t, of_t, lse, k_in, k_t, v_in, cos_t, sin_t, w_parts, n_dev)
    d_proj = exchange(d_blocks)

    attn_send = pack_pairs(dot(d_proj_t, u_all, 1, 0), n_dev, rows)
    d_proj, attn_send = lax.optimization_barrier((d_proj, attn_send))
    attn_back = exchange(attn_send)
    d_proj = d_proj.reshape(heads, 3, head_dim, tok)
    inv_rms = lax.rsqrt(jnp.mean(jnp.square(x_act.astype(F32)), axis=-1, keepdims=True) + RMS_EPS)
    d_u = sum(dot(d_proj[:, p].reshape(heads * head_dim, tok), w_qkv_all[p].reshape(width, heads * head_dim), 0, 1) for p in range(3)).astype(BF16)
    d_x_norm, part_g_attn = rms_norm_bwd(x_act, g_attn, inv_rms, d_u)
    grad_x = (d_hidden.astype(F32) + d_x_norm).astype(BF16)
    gain_send = jnp.concatenate([part_g_attn.reshape(n_dev, 1, rows), part_g_mlp.reshape(n_dev, 1, rows)], axis=2)

    a_all, dy_all = a_dy[:, :width], a_dy[:, width:]
    pre_t = dot(w_cols, a_all, 0, 1)
    gate_t, up_t = pre_t[:ff_s], pre_t[ff_s:]
    d_mixed_t = dot(w_down, dy_all, 1, 1).astype(BF16).astype(F32)
    mixed_t = (jax.nn.silu(gate_t) * up_t).astype(BF16)
    d_gu_t = jnp.concatenate(gate_backward(d_mixed_t, gate_t, up_t), axis=0)
    mlp_send = pack_pairs(dot(d_gu_t, a_all, 1, 0), n_dev, rows, jnp.pad(gain_send, ((0, 0), (0, 7), (0, 0))))
    attn_back, mlp_send, mixed_t = lax.optimization_barrier((attn_back, mlp_send, mixed_t))
    mlp_back = exchange(mlp_send)
    grad_w_down = dot(mixed_t, dy_all, 1, 0)

    o_far, dh_half, o_blocks, grad_w_down = lax.optimization_barrier((o_far, dh_half, o_blocks, grad_w_down))
    o_pair = jnp.concatenate([lax.dynamic_slice_in_dim(o_blocks, near, half_n), o_far], axis=1)
    part_w_o = dot(o_pair.transpose(1, 0, 2).reshape(2 * head_dim, seq // 2), dh_half, 1, 0)
    grad_w_o = (part_w_o[:head_dim] + lax.ppermute(part_w_o[head_dim:], SEQ_AXIS, pairs))[None]

    grad_w_q, grad_w_k, grad_w_v = split_heads(attn_back, head_dim)
    mlp_back, grad_w_down, grad_w_q, grad_w_k, grad_w_v, grad_w_o = lax.optimization_barrier((mlp_back, grad_w_down, grad_w_q, grad_w_k, grad_w_v, grad_w_o))
    gains = jnp.sum(mlp_back[:, ff_s], axis=0)
    grad_g_attn, grad_g_mlp = gains[:rows], gains[rows:]
    grad_w_gate, grad_w_up = join_columns(mlp_back, ff_s)
    return (y_out, grad_x, grad_g_attn, grad_w_q, grad_w_k, grad_w_v, grad_w_o, grad_g_mlp, grad_w_gate, grad_w_up, grad_w_down)


def solution(mesh):
    n_dev = mesh.shape[SEQ_AXIS]
    token_spec = P(SEQ_AXIS, None)
    cube_spec = P(SEQ_AXIS, None, None)
    gain_spec = P(SEQ_AXIS)
    weight_specs = (gain_spec, cube_spec, cube_spec, cube_spec, cube_spec, gain_spec, token_spec, token_spec, token_spec)
    return jax.shard_map(lambda *args: device_step(n_dev, *args), mesh=mesh, in_specs=(token_spec, gain_spec, token_spec) + weight_specs, out_specs=(token_spec, token_spec) + weight_specs, check_vma=False)
```

```python
import jax
import jax.numpy as jnp
from jax import lax
from jax.experimental import pallas as pl
from jax.experimental.layout import Layout, with_layout_constraint
from jax.experimental.pallas import tpu as pltpu
from jax.sharding import PartitionSpec as P

SEQ_AXIS = 'sp'
RMS_EPS = 1e-5
ROPE_BASE = 10000.0
MASK_VALUE = -1e30
TILE = 512
F32 = jnp.float32
BF16 = jnp.bfloat16


def rms_norm(act_in, gain_vec):
    act_f = act_in.astype(F32)
    inv_rms = lax.rsqrt(jnp.mean(act_f * act_f, axis=-1, keepdims=True) + RMS_EPS)
    return (act_f * inv_rms * gain_vec.astype(F32)).astype(BF16), inv_rms


def rms_norm_bwd(act_in, gain_vec, inv_rms, d_normed):
    act_f = act_in.astype(F32)
    d_f = d_normed.astype(F32)
    scaled_d = d_f * gain_vec.astype(F32)
    proj_mean = jnp.mean(scaled_d * act_f, axis=-1, keepdims=True)
    d_act = inv_rms * scaled_d - act_f * (inv_rms * inv_rms * inv_rms) * proj_mean
    d_gain = jnp.sum(d_f * act_f * inv_rms, axis=0)
    return d_act, d_gain


def dot(lhs, rhs, l_dim, r_dim):
    return lax.dot_general(lhs, rhs, (((l_dim,), (r_dim,)), ((), ())), preferred_element_type=F32)


def gather(shard):
    return lax.all_gather(shard, SEQ_AXIS, axis=0, tiled=True)


def exchange(blocks):
    return lax.all_to_all(blocks, SEQ_AXIS, 0, 0, tiled=True)


def rope_t(vals, cos_tab, sin_tab):
    half = vals.shape[0] // 2
    first, second = vals[:half], vals[half:]
    return jnp.concatenate([first * cos_tab - second * sin_tab, second * cos_tab + first * sin_tab], axis=0)


def mm(lhs, rhs):
    return jnp.dot(lhs, rhs, preferred_element_type=F32)


def diag_mask(tile):
    key_at = lax.broadcasted_iota(jnp.int32, (tile, tile), 0)
    query_at = lax.broadcasted_iota(jnp.int32, (tile, tile), 1)
    return key_at <= query_at


def attn_fwd_kernel(tile, q_t, k_ref, v_t, o_ref, of_ref, lse_ref, s_buf):
    step = pl.program_id(0)
    query = q_t[...]

    def scores(j):
        return mm(k_ref[pl.ds(pl.multiple_of(j * tile, tile), tile), :], query)

    def keep(j, logits, top):
        s_buf[pl.ds(pl.multiple_of(j * tile, tile), tile), :] = logits
        return jnp.maximum(top, jnp.max(logits, axis=0, keepdims=True))

    top = keep(step, jnp.where(diag_mask(tile), scores(step), MASK_VALUE), jnp.full((1, tile), MASK_VALUE, F32))
    top = lax.fori_loop(0, step, lambda j, c: keep(j, scores(j), c), top)

    def weigh(j, carry):
        acc, total = carry
        at = pl.ds(pl.multiple_of(j * tile, tile), tile)
        prob = jnp.exp(s_buf[at, :] - top)
        return acc + mm(v_t[:, at], prob.astype(BF16)), total + jnp.sum(prob, axis=0, keepdims=True)

    out, total = lax.fori_loop(0, step + 1, weigh, (jnp.zeros((v_t.shape[0], tile), F32), jnp.zeros((1, tile), F32)))
    out = out / total
    lse = top + jnp.log(total)
    of_ref[...] = out
    lse_ref[...] = lse
    block = o_ref.shape[2]
    for part in range(tile // block):
        o_ref[part] = out[:, part * block:(part + 1) * block].astype(BF16)


def attention_fwd(q_t, k_in, v_t, n_blocks):
    head_dim, seq = q_t.shape
    block = seq // n_blocks
    per = TILE // block
    return pl.pallas_call(
        lambda *refs: attn_fwd_kernel(TILE, *refs),
        grid=(seq // TILE,),
        in_specs=[pl.BlockSpec((head_dim, TILE), lambda i: (0, i)), pl.BlockSpec((seq, head_dim), lambda i: (0, 0)), pl.BlockSpec((head_dim, seq), lambda i: (0, 0))],
        out_specs=[pl.BlockSpec((per, head_dim, block), lambda i: (i, 0, 0)), pl.BlockSpec((head_dim, TILE), lambda i: (0, i)), pl.BlockSpec((1, TILE), lambda i: (0, i))],
        out_shape=[jax.ShapeDtypeStruct((n_blocks, head_dim, block), BF16), jax.ShapeDtypeStruct((head_dim, seq), F32), jax.ShapeDtypeStruct((1, seq), F32)],
        scratch_shapes=[pltpu.VMEM((seq, TILE), F32)],
        cost_estimate=pl.CostEstimate(flops=8 * seq * seq * head_dim, bytes_accessed=8 * seq * head_dim, transcendentals=seq * seq),
        name='attn_fwd',
    )(q_t, k_in, v_t)


PARTS = ((0, 96), (96, 80), (176, 80))
CORE, CHIP_AXES = 1, (2, 4, 8)


def flip(dev, bit):
    return dev + bit * (1 - 2 * ((dev // bit) % 2))


def start_copy(src, dst, send_sem, recv_sem, peer):
    copy = pltpu.make_async_remote_copy(src_ref=src, dst_ref=dst, send_sem=send_sem, recv_sem=recv_sem, device_id=(peer,), device_id_type=pl.DeviceIdType.MESH)
    copy.start()
    return copy


def landed(ref, sem):
    pltpu.make_async_copy(ref, ref, sem).wait()


def enter_all(me, n_dev):
    barrier = pltpu.get_barrier_semaphore()

    @pl.loop(1, n_dev)
    def _(hop):
        pl.semaphore_signal(barrier, inc=1, device_id=(lax.rem(me + hop, n_dev),), device_id_type=pl.DeviceIdType.MESH)

    pl.semaphore_wait(barrier, n_dev - 1)


class CubeGather:
    def __init__(self, me, part, send_sem, recv_sem, core_sem):
        self.me, self.part = me, part
        self.send_sem, self.recv_sem, self.core_sem = send_sem, recv_sem, core_sem
        self.sent = []

    def axes(self, p):
        return [CHIP_AXES[(p + i) % 3] for i in range(3)]

    def owner(self, p, index, start=None):
        dev = self.me if start is None else start
        for i, bit in enumerate(self.axes(p)):
            if (index >> i) & 1:
                dev = flip(dev, bit)
        return dev

    def push(self, p, index, axis):
        ref = self.part(self.owner(p, index), p)
        start_copy(ref, ref, self.send_sem.at[len(self.sent)], self.recv_sem.at[p, index + (1 << axis)], flip(self.me, self.axes(p)[axis]))
        self.sent.append((p, index))

    def push_core(self, p, index):
        ref = self.part(self.owner(p, index), p)
        start_copy(ref, ref, self.send_sem.at[len(self.sent)], self.core_sem.at[p, index], flip(self.me, CORE))
        self.sent.append((p, index))

    def begin(self):
        for axis in range(3):
            for p in range(3):
                self.push(p, 0, axis)
        for p in range(3):
            self.push_core(p, 0)

    def receive(self, index):
        for p in range(3):
            landed(self.part(self.owner(p, index), p), self.recv_sem.at[p, index])
            for axis in range(index.bit_length(), 3):
                self.push(p, index, axis)
            self.push_core(p, index)

    def receive_core(self, index):
        for p in range(3):
            landed(self.part(self.owner(p, index, flip(self.me, CORE)), p), self.core_sem.at[p, index])

    def finish(self):
        for slot, (p, index) in enumerate(self.sent):
            landed(self.part(self.owner(p, index), p), self.send_sem.at[slot])


N_SENDS = 9 + 12 + 24


def attn_bwd_kernel(n_dev, tile, block, q_t, do_t, of_t, lse_ref, cos_ref, sin_ref, k_ref, k_t, v_ref, cos_all, sin_all, w_ref, d_blocks, d_proj_t, w_out_q, w_out_k, w_out_v, dq_acc, dk_acc, dv_acc, w_buf, send_sem, recv_sem, core_sem, local_sem):
    step = pl.program_id(0)
    last = pl.num_programs(0) - 1
    me = lax.axis_index(SEQ_AXIS)
    cube = CubeGather(me, lambda dev, p: w_buf.at[p, dev], send_sem, recv_sem, core_sem)

    @pl.when(step == 0)
    def _():
        own = [pltpu.make_async_copy(w_ref.at[p], w_buf.at[p, me], local_sem.at[p]) for p in range(3)]
        for copy in own:
            copy.start()
        enter_all(me, n_dev)
        for copy in own:
            copy.wait()
        cube.begin()

    for at_step, indices in ((4, (1,)), (5, (2,)), (6, (4,)), (7, (3,))):
        @pl.when(step == at_step)
        def _(indices=indices):
            for index in indices:
                cube.receive(index)

    head_dim = q_t.shape[0]
    query_t, d_out_t = q_t[...], do_t[...]
    lse = lse_ref[...]
    delta = jnp.sum(d_out_t.astype(F32) * of_t[...], axis=0, keepdims=True)

    @pl.when(step == 0)
    def _():
        dk_acc[...] = jnp.zeros_like(dk_acc)
        dv_acc[...] = jnp.zeros_like(dv_acc)

    dq_acc[...] = jnp.zeros_like(dq_acc)

    def visit(j, masked):
        at = pl.ds(pl.multiple_of(j * tile, tile), tile)
        prob = jnp.exp(mm(k_ref[at, :], query_t) - lse)
        if masked:
            prob = jnp.where(diag_mask(tile), prob, 0.0)
        d_prob = mm(v_ref[at, :], d_out_t).astype(BF16).astype(F32)
        d_logits = (prob * (d_prob - delta)).astype(BF16)
        dv_acc[:, at] += dot(d_out_t, prob.astype(BF16), 1, 1)
        dk_acc[:, at] += dot(query_t, d_logits, 1, 1)
        dq_acc[...] += mm(k_t[:, at], d_logits)

    visit(step, True)

    @pl.loop(0, step)
    def _(j):
        visit(j, False)

    def put(row, col_block, values):
        rows = slice(row, row + values.shape[0])
        d_proj_t[rows, pl.ds(pl.multiple_of(col_block * block, block), values.shape[1])] = values
        for part in range(values.shape[1] // block):
            d_blocks[col_block + part, rows, :] = values[:, part * block:(part + 1) * block]

    d_q = (dq_acc[...] * (head_dim ** -0.5)).astype(BF16).astype(F32)
    per = tile // block
    put(0, step * per, rope_t(d_q, cos_ref[...], -sin_ref[...]).astype(BF16))

    @pl.when(step == last)
    def _():
        @pl.loop(0, pl.num_programs(0))
        def _(j):
            at = pl.ds(pl.multiple_of(j * tile, tile), tile)
            put(head_dim, j * per, rope_t(dk_acc[:, at].astype(BF16).astype(F32), cos_all[:, at], -sin_all[:, at]).astype(BF16))
            put(2 * head_dim, j * per, dv_acc[:, at].astype(BF16))

        for index in (5, 6, 7):
            cube.receive(index)
        for index in range(8):
            cube.receive_core(index)
        flushes = [pltpu.make_async_copy(w_buf.at[p], out, local_sem.at[p]) for p, out in enumerate((w_out_q, w_out_k, w_out_v))]
        for flush in flushes:
            flush.start()
        cube.finish()
        for flush in flushes:
            flush.wait()


def attention_bwd(q_t, do_t, of_t, lse, k_in, k_t, v_in, cos_t, sin_t, w_parts, n_blocks):
    head_dim, seq = q_t.shape
    block = seq // n_blocks
    cols = pl.BlockSpec((head_dim, TILE), lambda i: (0, i))
    half_cols = pl.BlockSpec((head_dim // 2, TILE), lambda i: (0, i))
    all_rows = pl.BlockSpec((seq, head_dim), lambda i: (0, 0))
    all_cols = pl.BlockSpec((head_dim, seq), lambda i: (0, 0))
    all_half = pl.BlockSpec((head_dim // 2, seq), lambda i: (0, 0))
    w_all_shape = (3, n_blocks) + w_parts.shape[1:]
    return pl.pallas_call(
        lambda *refs: attn_bwd_kernel(n_blocks, TILE, block, *refs),
        grid=(seq // TILE,),
        in_specs=[cols, cols, cols, pl.BlockSpec((1, TILE), lambda i: (0, i)), half_cols, half_cols, all_rows, all_cols, all_rows, all_half, all_half, pl.BlockSpec(memory_space=pl.ANY)],
        out_specs=[pl.BlockSpec((n_blocks, 3 * head_dim, block), lambda i: (0, 0, 0)), pl.BlockSpec((3 * head_dim, seq), lambda i: (0, 0))] + [pl.BlockSpec(memory_space=pl.ANY)] * 3,
        out_shape=[jax.ShapeDtypeStruct((n_blocks, 3 * head_dim, block), BF16), jax.ShapeDtypeStruct((3 * head_dim, seq), BF16)] + [jax.ShapeDtypeStruct(w_all_shape[1:], BF16)] * 3,
        scratch_shapes=[
            pltpu.VMEM((head_dim, TILE), F32),
            pltpu.VMEM((head_dim, seq), F32),
            pltpu.VMEM((head_dim, seq), F32),
            pltpu.VMEM(w_all_shape, BF16),
            pltpu.SemaphoreType.DMA((N_SENDS,)),
            pltpu.SemaphoreType.DMA((3, 8)),
            pltpu.SemaphoreType.DMA((3, 8)),
            pltpu.SemaphoreType.DMA((3,)),
        ],
        compiler_params=pltpu.CompilerParams(collective_id=1, has_side_effects=True),
        cost_estimate=pl.CostEstimate(flops=20 * seq * seq * head_dim, bytes_accessed=20 * seq * head_dim, transcendentals=seq * seq),
        name='attn_bwd',
    )(q_t, do_t, of_t, lse, cos_t, sin_t, k_in, k_t, v_in, cos_t, sin_t, w_parts)


def gather_proj_kernel(n_dev, x_ref, small_ref, w_ref, u_out, proj_t, small_all, x_buf, u_buf, w_buf, send_sem, recv_sem, core_sem, misc_send, misc_recv, local_sem, u_sem):
    me = lax.axis_index(SEQ_AXIS)
    own = pltpu.make_async_copy(x_ref, x_buf.at[me], local_sem.at[0])
    own.start()
    own_w = pltpu.make_async_copy(w_ref.at[me], w_buf.at[me], local_sem.at[1])
    own_w.start()
    own_small = pltpu.make_async_copy(small_ref, small_all.at[me], local_sem.at[2])
    own_small.start()
    enter_all(me, n_dev)
    own.wait()
    cube = CubeGather(me, lambda dev, p: x_buf.at[dev, pl.ds(PARTS[p][0], PARTS[p][1])], send_sem, recv_sem, core_sem)
    cube.begin()

    def spread(hop):
        peer = lax.rem(me + hop, n_dev)
        return [
            pltpu.make_async_remote_copy(src_ref=small_ref, dst_ref=small_all.at[me], send_sem=misc_send.at[0, hop], recv_sem=misc_recv.at[0, me], device_id=(peer,), device_id_type=pl.DeviceIdType.MESH),
            pltpu.make_async_remote_copy(src_ref=w_ref.at[peer], dst_ref=w_buf.at[me], send_sem=misc_send.at[1, hop], recv_sem=misc_recv.at[1, me], device_id=(peer,), device_id_type=pl.DeviceIdType.MESH),
        ]

    for kind in range(2):
        @pl.loop(1, n_dev)
        def _(hop, kind=kind):
            spread(hop)[kind].start()

    cube.receive(1)
    cube.receive(2)
    own_w.wait()
    own_small.wait()

    @pl.loop(1, n_dev)
    def _(hop):
        src = lax.rem(me + hop, n_dev)
        landed(small_all.at[src], misc_recv.at[0, src])
        landed(w_buf.at[src], misc_recv.at[1, src])

    width = x_ref.shape[1]
    tok = x_ref.shape[0]
    rows = w_ref.shape[1]
    gain = jnp.concatenate([small_all[d, 0:1, 0:rows] for d in range(n_dev)], axis=1)
    weight = w_buf[...].reshape(width, w_ref.shape[2])
    keep = proj_t.shape[0]

    def project(dev):
        act = x_buf[dev].astype(F32)
        inv = lax.rsqrt(jnp.mean(act * act, axis=-1, keepdims=True) + RMS_EPS)
        normed = (act * inv * gain).astype(BF16)
        u_buf[dev] = normed
        proj_t[:, pl.ds(pl.multiple_of(dev * tok, tok), tok)] = mm(normed, weight).T[:keep]
        pltpu.make_async_copy(u_buf.at[dev], u_out.at[dev], u_sem.at[dev]).start()

    def project_pair(dev):
        @pl.loop(0, 2)
        def _(core):
            project(dev + core * (flip(dev, CORE) - dev))

    def project_across(dev):
        @pl.loop(0, 3)
        def _(i):
            project_pair(flip(dev, i * (i + 1) + 2))

    cube.receive_core(0)
    project_pair(me)
    cube.receive(4)
    cube.receive(3)
    for index in (1, 2, 4):
        cube.receive_core(index)
    project_across(me)
    cube.receive(5)
    cube.receive(6)
    for index in (3, 5, 6):
        cube.receive_core(index)
    far = flip(flip(flip(me, 2), 4), 8)
    project_across(far)
    cube.receive(7)
    cube.receive_core(7)
    project_pair(far)

    cube.finish()

    @pl.loop(1, n_dev)
    def _(hop):
        for copy in spread(hop):
            copy.wait_send()

    @pl.loop(0, n_dev)
    def _(dev):
        pltpu.make_async_copy(u_buf.at[dev], u_out.at[dev], u_sem.at[dev]).wait()


def gather_proj(n_dev, x_act, small, w_blocks, qkv):
    tok, width = x_act.shape
    seq = tok * n_dev
    any_spec = pl.BlockSpec(memory_space=pl.ANY)
    vmem_spec = pl.BlockSpec(memory_space=pltpu.VMEM)
    return pl.pallas_call(
        lambda *refs: gather_proj_kernel(n_dev, *refs),
        in_specs=[any_spec, vmem_spec, vmem_spec],
        out_specs=[any_spec, vmem_spec, vmem_spec],
        out_shape=[jax.ShapeDtypeStruct((n_dev, tok, width), BF16), jax.ShapeDtypeStruct((qkv, seq), F32), jax.ShapeDtypeStruct((n_dev,) + small.shape, F32)],
        scratch_shapes=[
            pltpu.VMEM((n_dev, tok, width), BF16),
            pltpu.VMEM((n_dev, tok, width), BF16),
            pltpu.VMEM(w_blocks.shape, BF16),
            pltpu.SemaphoreType.DMA((N_SENDS,)),
            pltpu.SemaphoreType.DMA((3, 8)),
            pltpu.SemaphoreType.DMA((3, 8)),
            pltpu.SemaphoreType.DMA((2, n_dev)),
            pltpu.SemaphoreType.DMA((2, n_dev)),
            pltpu.SemaphoreType.DMA((3,)),
            pltpu.SemaphoreType.DMA((n_dev,)),
        ],
        compiler_params=pltpu.CompilerParams(collective_id=0, has_side_effects=True),
        cost_estimate=pl.CostEstimate(flops=30 * seq * width * width, bytes_accessed=4 * seq * width, transcendentals=0),
        name='gather_proj',
    )(x_act, small, w_blocks)


def gate_backward(d_mixed, gate_pre, up_pre):
    gate_sig = jax.nn.sigmoid(gate_pre)
    d_up = (d_mixed * gate_pre * gate_sig).astype(BF16)
    d_gate = (d_mixed * up_pre * gate_sig * (1.0 + gate_pre * (1.0 - gate_sig))).astype(BF16)
    return d_gate, d_up


def join_columns_kernel(size, src, first, second):
    turned = [src[d, :size, :].T for d in range(src.shape[0])]
    rows = first.shape[0]
    first[...] = jnp.concatenate([block[:rows] for block in turned], axis=1)
    second[...] = jnp.concatenate([block[rows:] for block in turned], axis=1)


def join_columns(blocks, size):
    shape = jax.ShapeDtypeStruct((blocks.shape[2] // 2, blocks.shape[0] * size), F32)
    return pl.pallas_call(lambda *refs: join_columns_kernel(size, *refs), out_shape=[shape, shape], name='join_columns')(blocks)


def split_heads_kernel(head_dim, src, first, second, third):
    half = head_dim // 2
    for d in range(src.shape[0]):
        turned = src[d].T
        low, high = turned[:head_dim], turned[head_dim:]
        first[:, d, :] = low[:, :head_dim]
        second[:, d, :] = jnp.concatenate([low[:, head_dim:], high[:, :half]], axis=1)
        third[:, d, :] = high[:, half:]


def split_heads(blocks, head_dim):
    shape = jax.ShapeDtypeStruct((blocks.shape[2] // 2, blocks.shape[0], head_dim), F32)
    return pl.pallas_call(lambda *refs: split_heads_kernel(head_dim, *refs), out_shape=[shape] * 3, name='split_heads')(blocks)


def pack_pairs_kernel(rows, grad_t, *refs):
    out = refs[-1]
    half = grad_t.shape[0] // 2
    for d in range(out.shape[0]):
        at = slice(d * rows, (d + 1) * rows)
        out[d, :half, :] = jnp.concatenate([grad_t[:half, at], grad_t[half:, at]], axis=1)
        if len(refs) > 1:
            out[d, half:, :] = refs[0][d]


def pack_pairs(grad_t, n_dev, rows, *tail):
    height = grad_t.shape[0] // 2 + sum(part.shape[1] for part in tail)
    shape = jax.ShapeDtypeStruct((n_dev, height, 2 * rows), F32)
    return pl.pallas_call(lambda *refs: pack_pairs_kernel(rows, *refs), out_shape=shape, name='pack_pairs')(grad_t, *tail)


def weight_block_kernel(gate, up, w_o, down, out):
    rows = gate.shape[0]
    at = 0
    for part in (gate[...], up[...], w_o[0]):
        out[:, at:at + part.shape[1]] = part
        at += part.shape[1]
    for start in range(0, down.shape[0], rows):
        height = min(rows, down.shape[0] - start)
        out[:height, at:at + down.shape[1]] = down[start:start + height, :]
        if height < rows:
            out[height:, at:at + down.shape[1]] = jnp.zeros((rows - height, down.shape[1]), BF16)
        at += down.shape[1]


def weight_block(gate, up, w_o, down):
    rows = gate.shape[0]
    width = 2 * gate.shape[1] + w_o.shape[2] + pl.cdiv(down.shape[0], rows) * down.shape[1]
    return pl.pallas_call(weight_block_kernel, out_shape=jax.ShapeDtypeStruct((rows, width), BF16), name='weight_block')(gate, up, w_o, down)


def device_step(n_dev, x_act, positions, grad_out, g_attn_s, w_q, w_k, w_v, w_o, g_mlp_s, w_gate, w_up, w_down):
    tok, width = x_act.shape
    seq = tok * n_dev
    rows, heads, head_dim = w_q.shape
    ff = w_gate.shape[1]
    ff_s = ff // n_dev
    qkv = 3 * head_dim

    small = jnp.concatenate([jnp.concatenate([g_attn_s, g_mlp_s]).astype(F32)[None], positions.astype(F32).reshape(-1, 2 * rows)], axis=0)
    small = jnp.pad(small, ((0, 8 - small.shape[0]), (0, 0)))
    w_qkv = jnp.concatenate([w_q, w_k, w_v], axis=2)
    w_blocks = jnp.pad(jnp.transpose(w_qkv, (1, 0, 2)), ((0, 0), (0, 0), (0, 256 - qkv)))
    u_all, proj_t, small_all = gather_proj(n_dev, x_act, small, w_blocks, qkv)
    u_all = u_all.reshape(seq, width)
    g_attn = small_all[:, 0, :rows].reshape(width)
    g_mlp = small_all[:, 0, rows:2 * rows].reshape(width)
    pos_all = small_all[:, 1:1 + tok // (2 * rows)]

    w_all = gather(weight_block(w_gate, w_up, w_o, w_down))
    w_gu = w_all[:, :2 * ff]
    w_o_all = w_all[:, 2 * ff:2 * ff + width]
    w_down_at = 2 * ff + width
    down_all = [w_all[:, w_down_at + i * width:w_down_at + (i + 1) * width].reshape(n_dev, rows, width) for i in range(pl.cdiv(ff_s, rows))]
    w_down_all = jnp.concatenate(down_all, axis=1)[:, :ff_s].reshape(ff, width)
    me = lax.axis_index(SEQ_AXIS)
    w_cols = jnp.concatenate([lax.dynamic_slice(w_all, (0, at + me * ff_s), (width, ff_s)) for at in (0, ff)], axis=1)

    half = head_dim // 2
    inv_freq = ROPE_BASE ** (-(jnp.arange(half, dtype=F32) * (2.0 / head_dim)))
    angle_t = inv_freq[:, None] * pos_all.reshape(1, seq)
    cos_t, sin_t = jnp.cos(angle_t), jnp.sin(angle_t)

    q_t = (rope_t(proj_t[:head_dim], cos_t, sin_t).astype(BF16).astype(F32) * (head_dim ** -0.5)).astype(BF16)
    k_t = rope_t(proj_t[head_dim:2 * head_dim], cos_t, sin_t).astype(BF16)
    v_t = proj_t[2 * head_dim:].astype(BF16)
    k_in, v_in = k_t.T, v_t.T
    o_blocks, of_t, lse = attention_fwd(q_t, k_in, v_t, n_dev)
    o_loc = exchange(o_blocks).reshape(width, tok)
    w_parts = jnp.stack([w.reshape(rows, heads * head_dim) for w in (w_q, w_k, w_v)])
    o_loc, w_parts, v_in, w_down_all = lax.optimization_barrier((o_loc, w_parts, v_in, w_down_all))

    hidden = (x_act.astype(F32) + dot(o_loc, w_o_all, 0, 0)).astype(BF16)
    normed_mlp, inv_rms_mlp = rms_norm(hidden, g_mlp)
    a_dy = jnp.concatenate([normed_mlp, grad_out], axis=1)
    normed_mlp, a_dy = lax.optimization_barrier((normed_mlp, a_dy))
    a_dy = gather(a_dy)
    pre = with_layout_constraint(dot(normed_mlp, w_gu, 1, 0), Layout(major_to_minor=(0, 1)))
    gate_pre, up_pre = pre[:, :ff], pre[:, ff:]
    mixed = (jax.nn.silu(gate_pre) * up_pre).astype(BF16)
    y_out = (hidden.astype(F32) + dot(mixed, w_down_all, 1, 0)).astype(BF16)

    d_mixed = dot(grad_out, w_down_all, 1, 1).astype(BF16).astype(F32)
    d_gu = jnp.concatenate(gate_backward(d_mixed, gate_pre, up_pre), axis=1)
    d_normed = dot(d_gu, w_gu, 1, 1).astype(BF16)
    d_hid_norm, part_g_mlp = rms_norm_bwd(hidden, g_mlp, inv_rms_mlp, d_normed)
    d_hidden = (grad_out.astype(F32) + d_hid_norm).astype(BF16)
    do_blocks = exchange(dot(w_o_all, d_hidden, 1, 1).astype(BF16).reshape(n_dev, head_dim, tok))
    half_n = n_dev // 2
    pairs = [(i, (i + half_n) % n_dev) for i in range(n_dev)]
    near = (me // half_n) * half_n
    o_far = lax.ppermute(lax.dynamic_slice_in_dim(o_blocks, half_n - near, half_n), SEQ_AXIS, pairs)
    do_blocks, y_out = lax.optimization_barrier((do_blocks, y_out))
    dh_half = lax.all_gather(d_hidden, SEQ_AXIS, axis=0, tiled=True, axis_index_groups=[list(range(half_n)), list(range(half_n, n_dev))])

    do_t = jnp.transpose(do_blocks, (1, 0, 2)).reshape(head_dim, seq)
    d_blocks, d_proj_t, *w_qkv_all = attention_bwd(q_t, do_t, of_t, lse, k_in, k_t, v_in, cos_t, sin_t, w_parts, n_dev)
    d_proj = exchange(d_blocks)

    grad_w_qkv = dot(d_proj_t, u_all, 1, 0)
    attn_send = pack_pairs(grad_w_qkv, n_dev, rows)
    d_proj, attn_send = lax.optimization_barrier((d_proj, attn_send))
    attn_back = exchange(attn_send)
    d_proj = d_proj.reshape(heads, 3, head_dim, tok)
    inv_rms = lax.rsqrt(jnp.mean(jnp.square(x_act.astype(F32)), axis=-1, keepdims=True) + RMS_EPS)
    d_u = sum(dot(d_proj[:, p].reshape(heads * head_dim, tok), w_qkv_all[p].reshape(width, heads * head_dim), 0, 1) for p in range(3)).astype(BF16)
    d_x_norm, part_g_attn = rms_norm_bwd(x_act, g_attn, inv_rms, d_u)
    grad_x = (d_hidden.astype(F32) + d_x_norm).astype(BF16)
    gain_send = jnp.concatenate([part_g_attn.reshape(n_dev, 1, rows), part_g_mlp.reshape(n_dev, 1, rows)], axis=2)

    a_all, dy_all = a_dy[:, :width], a_dy[:, width:]
    pre_t = dot(w_cols, a_all, 0, 1)
    gate_t, up_t = pre_t[:ff_s], pre_t[ff_s:]
    d_mixed_t = dot(w_down, dy_all, 1, 1).astype(BF16).astype(F32)
    mixed_t = (jax.nn.silu(gate_t) * up_t).astype(BF16)
    d_gu_t = jnp.concatenate(gate_backward(d_mixed_t, gate_t, up_t), axis=0)
    grad_w_gu = dot(d_gu_t, a_all, 1, 0)
    mlp_send = pack_pairs(grad_w_gu, n_dev, rows, jnp.pad(gain_send, ((0, 0), (0, 7), (0, 0))))
    attn_back, mlp_send, mixed_t = lax.optimization_barrier((attn_back, mlp_send, mixed_t))
    mlp_back = exchange(mlp_send)
    grad_w_down = dot(mixed_t, dy_all, 1, 0)

    o_far, dh_half, o_blocks, grad_w_down = lax.optimization_barrier((o_far, dh_half, o_blocks, grad_w_down))
    o_pair = jnp.concatenate([lax.dynamic_slice_in_dim(o_blocks, near, half_n), o_far], axis=1)
    part_w_o = dot(o_pair.transpose(1, 0, 2).reshape(2 * head_dim, seq // 2), dh_half, 1, 0)
    grad_w_o = (part_w_o[:head_dim] + lax.ppermute(part_w_o[head_dim:], SEQ_AXIS, pairs))[None]

    grad_w_q, grad_w_k, grad_w_v = split_heads(attn_back, head_dim)
    mlp_back, grad_w_down, grad_w_q, grad_w_k, grad_w_v, grad_w_o = lax.optimization_barrier((mlp_back, grad_w_down, grad_w_q, grad_w_k, grad_w_v, grad_w_o))
    gains = jnp.sum(mlp_back[:, ff_s], axis=0)
    grad_g_attn, grad_g_mlp = gains[:rows], gains[rows:]
    grad_w_gate, grad_w_up = join_columns(mlp_back, ff_s)
    return (y_out, grad_x, grad_g_attn, grad_w_q, grad_w_k, grad_w_v, grad_w_o, grad_g_mlp, grad_w_gate, grad_w_up, grad_w_down)


def solution(mesh):
    n_dev = mesh.shape[SEQ_AXIS]
    token_spec = P(SEQ_AXIS, None)
    cube_spec = P(SEQ_AXIS, None, None)
    gain_spec = P(SEQ_AXIS)
    weight_specs = (gain_spec, cube_spec, cube_spec, cube_spec, cube_spec, gain_spec, token_spec, token_spec, token_spec)
    return jax.shard_map(lambda *args: device_step(n_dev, *args), mesh=mesh, in_specs=(token_spec, gain_spec, token_spec) + weight_specs, out_specs=(token_spec, token_spec) + weight_specs, check_vma=False)
```

```python
import jax
import jax.numpy as jnp
from jax import lax
from jax.experimental import pallas as pl
from jax.experimental.layout import Layout, with_layout_constraint
from jax.experimental.pallas import tpu as pltpu
from jax.sharding import PartitionSpec as P

SEQ_AXIS = 'sp'
RMS_EPS = 1e-5
ROPE_BASE = 10000.0
MASK_VALUE = -1e30
TILE = 512
F32 = jnp.float32
BF16 = jnp.bfloat16


def rms_norm(act_in, gain_vec):
    act_f = act_in.astype(F32)
    inv_rms = lax.rsqrt(jnp.mean(act_f * act_f, axis=-1, keepdims=True) + RMS_EPS)
    return (act_f * inv_rms * gain_vec.astype(F32)).astype(BF16), inv_rms


def rms_norm_bwd(act_in, gain_vec, inv_rms, d_normed):
    act_f = act_in.astype(F32)
    d_f = d_normed.astype(F32)
    scaled_d = d_f * gain_vec.astype(F32)
    proj_mean = jnp.mean(scaled_d * act_f, axis=-1, keepdims=True)
    d_act = inv_rms * scaled_d - act_f * (inv_rms * inv_rms * inv_rms) * proj_mean
    d_gain = jnp.sum(d_f * act_f * inv_rms, axis=0)
    return d_act, d_gain


def dot(lhs, rhs, l_dim, r_dim):
    return lax.dot_general(lhs, rhs, (((l_dim,), (r_dim,)), ((), ())), preferred_element_type=F32)


def gather(shard):
    return lax.all_gather(shard, SEQ_AXIS, axis=0, tiled=True)


def exchange(blocks):
    return lax.all_to_all(blocks, SEQ_AXIS, 0, 0, tiled=True)


def rope_t(vals, cos_tab, sin_tab):
    half = vals.shape[0] // 2
    first, second = vals[:half], vals[half:]
    return jnp.concatenate([first * cos_tab - second * sin_tab, second * cos_tab + first * sin_tab], axis=0)


def mm(lhs, rhs):
    return jnp.dot(lhs, rhs, preferred_element_type=F32)


def diag_mask(tile):
    key_at = lax.broadcasted_iota(jnp.int32, (tile, tile), 0)
    query_at = lax.broadcasted_iota(jnp.int32, (tile, tile), 1)
    return key_at <= query_at


def attn_fwd_kernel(tile, q_t, k_ref, v_t, o_ref, of_ref, lse_ref, s_buf):
    step = pl.program_id(0)
    query = q_t[...]

    def scores(j):
        return mm(k_ref[pl.ds(pl.multiple_of(j * tile, tile), tile), :], query)

    def keep(j, logits, top):
        s_buf[pl.ds(pl.multiple_of(j * tile, tile), tile), :] = logits
        return jnp.maximum(top, jnp.max(logits, axis=0, keepdims=True))

    top = keep(step, jnp.where(diag_mask(tile), scores(step), MASK_VALUE), jnp.full((1, tile), MASK_VALUE, F32))
    top = lax.fori_loop(0, step, lambda j, c: keep(j, scores(j), c), top)

    def weigh(j, carry):
        acc, total = carry
        at = pl.ds(pl.multiple_of(j * tile, tile), tile)
        prob = jnp.exp(s_buf[at, :] - top)
        return acc + mm(v_t[:, at], prob.astype(BF16)), total + jnp.sum(prob, axis=0, keepdims=True)

    out, total = lax.fori_loop(0, step + 1, weigh, (jnp.zeros((v_t.shape[0], tile), F32), jnp.zeros((1, tile), F32)))
    out = out / total
    lse = top + jnp.log(total)
    of_ref[...] = out
    lse_ref[...] = lse
    block = o_ref.shape[2]
    for part in range(tile // block):
        o_ref[part] = out[:, part * block:(part + 1) * block].astype(BF16)


def attention_fwd(q_t, k_in, v_t, n_blocks):
    head_dim, seq = q_t.shape
    block = seq // n_blocks
    per = TILE // block
    return pl.pallas_call(
        lambda *refs: attn_fwd_kernel(TILE, *refs),
        grid=(seq // TILE,),
        in_specs=[pl.BlockSpec((head_dim, TILE), lambda i: (0, i)), pl.BlockSpec((seq, head_dim), lambda i: (0, 0)), pl.BlockSpec((head_dim, seq), lambda i: (0, 0))],
        out_specs=[pl.BlockSpec((per, head_dim, block), lambda i: (i, 0, 0)), pl.BlockSpec((head_dim, TILE), lambda i: (0, i)), pl.BlockSpec((1, TILE), lambda i: (0, i))],
        out_shape=[jax.ShapeDtypeStruct((n_blocks, head_dim, block), BF16), jax.ShapeDtypeStruct((head_dim, seq), F32), jax.ShapeDtypeStruct((1, seq), F32)],
        scratch_shapes=[pltpu.VMEM((seq, TILE), F32)],
        cost_estimate=pl.CostEstimate(flops=8 * seq * seq * head_dim, bytes_accessed=8 * seq * head_dim, transcendentals=seq * seq),
        name='attn_fwd',
    )(q_t, k_in, v_t)


PARTS = ((0, 96), (96, 80), (176, 80))
CORE, CHIP_AXES = 1, (2, 4, 8)


def flip(dev, bit):
    return dev + bit * (1 - 2 * ((dev // bit) % 2))


def start_copy(src, dst, send_sem, recv_sem, peer):
    copy = pltpu.make_async_remote_copy(src_ref=src, dst_ref=dst, send_sem=send_sem, recv_sem=recv_sem, device_id=(peer,), device_id_type=pl.DeviceIdType.MESH)
    copy.start()
    return copy


def landed(ref, sem):
    pltpu.make_async_copy(ref, ref, sem).wait()


def enter_all(me, n_dev):
    barrier = pltpu.get_barrier_semaphore()

    @pl.loop(1, n_dev)
    def _(hop):
        pl.semaphore_signal(barrier, inc=1, device_id=(lax.rem(me + hop, n_dev),), device_id_type=pl.DeviceIdType.MESH)

    pl.semaphore_wait(barrier, n_dev - 1)


class CubeGather:
    def __init__(self, me, part, send_sem, recv_sem, core_sem):
        self.me, self.part = me, part
        self.send_sem, self.recv_sem, self.core_sem = send_sem, recv_sem, core_sem
        self.sent = []

    def axes(self, p):
        return [CHIP_AXES[(p + i) % 3] for i in range(3)]

    def owner(self, p, index, start=None):
        dev = self.me if start is None else start
        for i, bit in enumerate(self.axes(p)):
            if (index >> i) & 1:
                dev = flip(dev, bit)
        return dev

    def push(self, p, index, axis):
        ref = self.part(self.owner(p, index), p)
        start_copy(ref, ref, self.send_sem.at[len(self.sent)], self.recv_sem.at[p, index + (1 << axis)], flip(self.me, self.axes(p)[axis]))
        self.sent.append((p, index))

    def push_core(self, p, index):
        ref = self.part(self.owner(p, index), p)
        start_copy(ref, ref, self.send_sem.at[len(self.sent)], self.core_sem.at[p, index], flip(self.me, CORE))
        self.sent.append((p, index))

    def begin(self):
        for axis in range(3):
            for p in range(3):
                self.push(p, 0, axis)
        for p in range(3):
            self.push_core(p, 0)

    def receive(self, index):
        for p in range(3):
            landed(self.part(self.owner(p, index), p), self.recv_sem.at[p, index])
            for axis in range(index.bit_length(), 3):
                self.push(p, index, axis)
            self.push_core(p, index)

    def receive_core(self, index):
        for p in range(3):
            landed(self.part(self.owner(p, index, flip(self.me, CORE)), p), self.core_sem.at[p, index])

    def finish(self):
        for slot, (p, index) in enumerate(self.sent):
            landed(self.part(self.owner(p, index), p), self.send_sem.at[slot])


N_SENDS = 9 + 12 + 24


def attn_bwd_kernel(n_dev, tile, block, q_t, do_t, of_t, lse_ref, cos_ref, sin_ref, k_ref, k_t, v_ref, cos_all, sin_all, w_ref, d_blocks, d_proj_t, w_out_q, w_out_k, w_out_v, dq_acc, dk_acc, dv_acc, w_buf, send_sem, recv_sem, core_sem, local_sem):
    step = pl.program_id(0)
    last = pl.num_programs(0) - 1
    me = lax.axis_index(SEQ_AXIS)
    cube = CubeGather(me, lambda dev, p: w_buf.at[p, dev], send_sem, recv_sem, core_sem)

    @pl.when(step == 0)
    def _():
        own = [pltpu.make_async_copy(w_ref.at[p], w_buf.at[p, me], local_sem.at[p]) for p in range(3)]
        for copy in own:
            copy.start()
        enter_all(me, n_dev)
        for copy in own:
            copy.wait()
        cube.begin()

    for at_step, indices in ((4, (1,)), (5, (2,)), (6, (4,)), (7, (3,))):
        @pl.when(step == at_step)
        def _(indices=indices):
            for index in indices:
                cube.receive(index)

    head_dim = q_t.shape[0]
    query_t, d_out_t = q_t[...], do_t[...]
    lse = lse_ref[...]
    delta = jnp.sum(d_out_t.astype(F32) * of_t[...], axis=0, keepdims=True)

    @pl.when(step == 0)
    def _():
        dk_acc[...] = jnp.zeros_like(dk_acc)
        dv_acc[...] = jnp.zeros_like(dv_acc)

    dq_acc[...] = jnp.zeros_like(dq_acc)

    def visit(j, masked):
        at = pl.ds(pl.multiple_of(j * tile, tile), tile)
        prob = jnp.exp(mm(k_ref[at, :], query_t) - lse)
        if masked:
            prob = jnp.where(diag_mask(tile), prob, 0.0)
        d_prob = mm(v_ref[at, :], d_out_t).astype(BF16).astype(F32)
        d_logits = (prob * (d_prob - delta)).astype(BF16)
        dv_acc[:, at] += dot(d_out_t, prob.astype(BF16), 1, 1)
        dk_acc[:, at] += dot(query_t, d_logits, 1, 1)
        dq_acc[...] += mm(k_t[:, at], d_logits)

    visit(step, True)

    @pl.loop(0, step)
    def _(j):
        visit(j, False)

    def put(row, col_block, values):
        rows = slice(row, row + values.shape[0])
        d_proj_t[rows, pl.ds(pl.multiple_of(col_block * block, block), values.shape[1])] = values
        for part in range(values.shape[1] // block):
            d_blocks[col_block + part, rows, :] = values[:, part * block:(part + 1) * block]

    d_q = (dq_acc[...] * (head_dim ** -0.5)).astype(BF16).astype(F32)
    per = tile // block
    put(0, step * per, rope_t(d_q, cos_ref[...], -sin_ref[...]).astype(BF16))

    @pl.when(step == last)
    def _():
        @pl.loop(0, pl.num_programs(0))
        def _(j):
            at = pl.ds(pl.multiple_of(j * tile, tile), tile)
            put(head_dim, j * per, rope_t(dk_acc[:, at].astype(BF16).astype(F32), cos_all[:, at], -sin_all[:, at]).astype(BF16))
            put(2 * head_dim, j * per, dv_acc[:, at].astype(BF16))

        for index in (5, 6, 7):
            cube.receive(index)
        for index in range(8):
            cube.receive_core(index)
        flushes = [pltpu.make_async_copy(w_buf.at[p], out, local_sem.at[p]) for p, out in enumerate((w_out_q, w_out_k, w_out_v))]
        for flush in flushes:
            flush.start()
        cube.finish()
        for flush in flushes:
            flush.wait()


def attention_bwd(q_t, do_t, of_t, lse, k_in, k_t, v_in, cos_t, sin_t, w_parts, n_blocks):
    head_dim, seq = q_t.shape
    block = seq // n_blocks
    cols = pl.BlockSpec((head_dim, TILE), lambda i: (0, i))
    half_cols = pl.BlockSpec((head_dim // 2, TILE), lambda i: (0, i))
    all_rows = pl.BlockSpec((seq, head_dim), lambda i: (0, 0))
    all_cols = pl.BlockSpec((head_dim, seq), lambda i: (0, 0))
    all_half = pl.BlockSpec((head_dim // 2, seq), lambda i: (0, 0))
    w_all_shape = (3, n_blocks) + w_parts.shape[1:]
    return pl.pallas_call(
        lambda *refs: attn_bwd_kernel(n_blocks, TILE, block, *refs),
        grid=(seq // TILE,),
        in_specs=[cols, cols, cols, pl.BlockSpec((1, TILE), lambda i: (0, i)), half_cols, half_cols, all_rows, all_cols, all_rows, all_half, all_half, pl.BlockSpec(memory_space=pl.ANY)],
        out_specs=[pl.BlockSpec((n_blocks, 3 * head_dim, block), lambda i: (0, 0, 0)), pl.BlockSpec((3 * head_dim, seq), lambda i: (0, 0))] + [pl.BlockSpec(memory_space=pl.ANY)] * 3,
        out_shape=[jax.ShapeDtypeStruct((n_blocks, 3 * head_dim, block), BF16), jax.ShapeDtypeStruct((3 * head_dim, seq), BF16)] + [jax.ShapeDtypeStruct(w_all_shape[1:], BF16)] * 3,
        scratch_shapes=[
            pltpu.VMEM((head_dim, TILE), F32),
            pltpu.VMEM((head_dim, seq), F32),
            pltpu.VMEM((head_dim, seq), F32),
            pltpu.VMEM(w_all_shape, BF16),
            pltpu.SemaphoreType.DMA((N_SENDS,)),
            pltpu.SemaphoreType.DMA((3, 8)),
            pltpu.SemaphoreType.DMA((3, 8)),
            pltpu.SemaphoreType.DMA((3,)),
        ],
        compiler_params=pltpu.CompilerParams(collective_id=1, has_side_effects=True),
        cost_estimate=pl.CostEstimate(flops=20 * seq * seq * head_dim, bytes_accessed=20 * seq * head_dim, transcendentals=seq * seq),
        name='attn_bwd',
    )(q_t, do_t, of_t, lse, cos_t, sin_t, k_in, k_t, v_in, cos_t, sin_t, w_parts)


def gather_proj_kernel(n_dev, x_ref, small_ref, w_ref, u_out, proj_t, small_all, x_buf, u_buf, w_buf, send_sem, recv_sem, core_sem, misc_send, misc_recv, local_sem, u_sem):
    me = lax.axis_index(SEQ_AXIS)
    own = pltpu.make_async_copy(x_ref, x_buf.at[me], local_sem.at[0])
    own.start()
    own_w = pltpu.make_async_copy(w_ref.at[me], w_buf.at[me], local_sem.at[1])
    own_w.start()
    own_small = pltpu.make_async_copy(small_ref, small_all.at[me], local_sem.at[2])
    own_small.start()
    enter_all(me, n_dev)
    own.wait()
    cube = CubeGather(me, lambda dev, p: x_buf.at[dev, pl.ds(PARTS[p][0], PARTS[p][1])], send_sem, recv_sem, core_sem)
    cube.begin()

    def spread(hop):
        peer = lax.rem(me + hop, n_dev)
        return [
            pltpu.make_async_remote_copy(src_ref=small_ref, dst_ref=small_all.at[me], send_sem=misc_send.at[0, hop], recv_sem=misc_recv.at[0, me], device_id=(peer,), device_id_type=pl.DeviceIdType.MESH),
            pltpu.make_async_remote_copy(src_ref=w_ref.at[peer], dst_ref=w_buf.at[me], send_sem=misc_send.at[1, hop], recv_sem=misc_recv.at[1, me], device_id=(peer,), device_id_type=pl.DeviceIdType.MESH),
        ]

    for kind in range(2):
        @pl.loop(1, n_dev)
        def _(hop, kind=kind):
            spread(hop)[kind].start()

    cube.receive(1)
    cube.receive(2)
    own_w.wait()
    own_small.wait()

    @pl.loop(1, n_dev)
    def _(hop):
        src = lax.rem(me + hop, n_dev)
        landed(small_all.at[src], misc_recv.at[0, src])
        landed(w_buf.at[src], misc_recv.at[1, src])

    width = x_ref.shape[1]
    tok = x_ref.shape[0]
    rows = w_ref.shape[1]
    gain = jnp.concatenate([small_all[d, 0:1, 0:rows] for d in range(n_dev)], axis=1)
    weight = w_buf[...].reshape(width, w_ref.shape[2])
    keep = proj_t.shape[0]

    def project(dev):
        act = x_buf[dev].astype(F32)
        inv = lax.rsqrt(jnp.mean(act * act, axis=-1, keepdims=True) + RMS_EPS)
        normed = (act * inv * gain).astype(BF16)
        u_buf[dev] = normed
        proj_t[:, pl.ds(pl.multiple_of(dev * tok, tok), tok)] = mm(normed, weight).T[:keep]
        pltpu.make_async_copy(u_buf.at[dev], u_out.at[dev], u_sem.at[dev]).start()

    def project_pair(dev):
        @pl.loop(0, 2)
        def _(core):
            project(dev + core * (flip(dev, CORE) - dev))

    def project_across(dev):
        @pl.loop(0, 3)
        def _(i):
            project_pair(flip(dev, i * (i + 1) + 2))

    cube.receive_core(0)
    project_pair(me)
    cube.receive(4)
    cube.receive(3)
    for index in (1, 2, 4):
        cube.receive_core(index)
    project_across(me)
    cube.receive(5)
    cube.receive(6)
    for index in (3, 5, 6):
        cube.receive_core(index)
    far = flip(flip(flip(me, 2), 4), 8)
    project_across(far)
    cube.receive(7)
    cube.receive_core(7)
    project_pair(far)

    cube.finish()

    @pl.loop(1, n_dev)
    def _(hop):
        for copy in spread(hop):
            copy.wait_send()

    @pl.loop(0, n_dev)
    def _(dev):
        pltpu.make_async_copy(u_buf.at[dev], u_out.at[dev], u_sem.at[dev]).wait()


def gather_proj(n_dev, x_act, small, w_blocks, qkv):
    tok, width = x_act.shape
    seq = tok * n_dev
    any_spec = pl.BlockSpec(memory_space=pl.ANY)
    vmem_spec = pl.BlockSpec(memory_space=pltpu.VMEM)
    return pl.pallas_call(
        lambda *refs: gather_proj_kernel(n_dev, *refs),
        in_specs=[any_spec, vmem_spec, vmem_spec],
        out_specs=[any_spec, vmem_spec, vmem_spec],
        out_shape=[jax.ShapeDtypeStruct((n_dev, tok, width), BF16), jax.ShapeDtypeStruct((qkv, seq), F32), jax.ShapeDtypeStruct((n_dev,) + small.shape, F32)],
        scratch_shapes=[
            pltpu.VMEM((n_dev, tok, width), BF16),
            pltpu.VMEM((n_dev, tok, width), BF16),
            pltpu.VMEM(w_blocks.shape, BF16),
            pltpu.SemaphoreType.DMA((N_SENDS,)),
            pltpu.SemaphoreType.DMA((3, 8)),
            pltpu.SemaphoreType.DMA((3, 8)),
            pltpu.SemaphoreType.DMA((2, n_dev)),
            pltpu.SemaphoreType.DMA((2, n_dev)),
            pltpu.SemaphoreType.DMA((3,)),
            pltpu.SemaphoreType.DMA((n_dev,)),
        ],
        compiler_params=pltpu.CompilerParams(collective_id=0, has_side_effects=True),
        cost_estimate=pl.CostEstimate(flops=30 * seq * width * width, bytes_accessed=4 * seq * width, transcendentals=0),
        name='gather_proj',
    )(x_act, small, w_blocks)


def gate_backward(d_mixed, gate_pre, up_pre):
    gate_sig = jax.nn.sigmoid(gate_pre)
    d_up = (d_mixed * gate_pre * gate_sig).astype(BF16)
    d_gate = (d_mixed * up_pre * gate_sig * (1.0 + gate_pre * (1.0 - gate_sig))).astype(BF16)
    return d_gate, d_up


def join_columns_kernel(size, src, first, second):
    turned = [src[d, :size, :].T for d in range(src.shape[0])]
    rows = first.shape[0]
    first[...] = jnp.concatenate([block[:rows] for block in turned], axis=1)
    second[...] = jnp.concatenate([block[rows:] for block in turned], axis=1)


def join_columns(blocks, size):
    shape = jax.ShapeDtypeStruct((blocks.shape[2] // 2, blocks.shape[0] * size), F32)
    return pl.pallas_call(lambda *refs: join_columns_kernel(size, *refs), out_shape=[shape, shape], name='join_columns')(blocks)


def split_heads_kernel(head_dim, src, first, second, third):
    half = head_dim // 2
    for d in range(src.shape[0]):
        turned = src[d].T
        low, high = turned[:head_dim], turned[head_dim:]
        first[:, d, :] = low[:, :head_dim]
        second[:, d, :] = jnp.concatenate([low[:, head_dim:], high[:, :half]], axis=1)
        third[:, d, :] = high[:, half:]


def split_heads(blocks, head_dim):
    shape = jax.ShapeDtypeStruct((blocks.shape[2] // 2, blocks.shape[0], head_dim), F32)
    return pl.pallas_call(lambda *refs: split_heads_kernel(head_dim, *refs), out_shape=[shape] * 3, name='split_heads')(blocks)


def pack_pairs_kernel(rows, grad_t, *refs):
    out = refs[-1]
    half = grad_t.shape[0] // 2
    for d in range(out.shape[0]):
        at = slice(d * rows, (d + 1) * rows)
        out[d, :half, :] = jnp.concatenate([grad_t[:half, at], grad_t[half:, at]], axis=1)
        if len(refs) > 1:
            out[d, half:, :] = refs[0][d]


def pack_pairs(grad_t, n_dev, rows, *tail):
    height = grad_t.shape[0] // 2 + sum(part.shape[1] for part in tail)
    shape = jax.ShapeDtypeStruct((n_dev, height, 2 * rows), F32)
    return pl.pallas_call(lambda *refs: pack_pairs_kernel(rows, *refs), out_shape=shape, name='pack_pairs')(grad_t, *tail)


def weight_block_kernel(gate, up, w_o, down, out):
    rows = gate.shape[0]
    at = 0
    for part in (gate[...], up[...], w_o[0]):
        out[:, at:at + part.shape[1]] = part
        at += part.shape[1]
    for start in range(0, down.shape[0], rows):
        height = min(rows, down.shape[0] - start)
        out[:height, at:at + down.shape[1]] = down[start:start + height, :]
        if height < rows:
            out[height:, at:at + down.shape[1]] = jnp.zeros((rows - height, down.shape[1]), BF16)
        at += down.shape[1]


def weight_block(gate, up, w_o, down):
    rows = gate.shape[0]
    width = 2 * gate.shape[1] + w_o.shape[2] + pl.cdiv(down.shape[0], rows) * down.shape[1]
    return pl.pallas_call(weight_block_kernel, out_shape=jax.ShapeDtypeStruct((rows, width), BF16), name='weight_block')(gate, up, w_o, down)


def join_down_kernel(start, src, out, sem):
    rows, width = src.shape[1], out.shape[2]
    copies = []
    for i, top in enumerate(range(0, out.shape[1], rows)):
        height = min(rows, out.shape[1] - top)
        copies.append(pltpu.make_async_copy(src.at[:, pl.ds(0, height), pl.ds(start + i * width, width)], out.at[:, pl.ds(top, height), :], sem.at[i]))
    for copy in copies:
        copy.start()
    for copy in copies:
        copy.wait()


def join_down(w_all, start, shape):
    return pl.pallas_call(
        lambda *refs: join_down_kernel(start, *refs),
        in_specs=[pl.BlockSpec(memory_space=pl.ANY)],
        out_specs=pl.BlockSpec(memory_space=pltpu.VMEM),
        out_shape=jax.ShapeDtypeStruct(shape, BF16),
        scratch_shapes=[pltpu.SemaphoreType.DMA((pl.cdiv(shape[1], w_all.shape[1]),))],
        name='join_down',
    )(w_all)


def device_step(n_dev, x_act, positions, grad_out, g_attn_s, w_q, w_k, w_v, w_o, g_mlp_s, w_gate, w_up, w_down):
    tok, width = x_act.shape
    seq = tok * n_dev
    rows, heads, head_dim = w_q.shape
    ff = w_gate.shape[1]
    ff_s = ff // n_dev
    qkv = 3 * head_dim

    small = jnp.concatenate([jnp.concatenate([g_attn_s, g_mlp_s]).astype(F32)[None], positions.astype(F32).reshape(-1, 2 * rows)], axis=0)
    small = jnp.pad(small, ((0, 8 - small.shape[0]), (0, 0)))
    w_qkv = jnp.concatenate([w_q, w_k, w_v], axis=2)
    w_blocks = jnp.pad(jnp.transpose(w_qkv, (1, 0, 2)), ((0, 0), (0, 0), (0, 256 - qkv)))
    u_all, proj_t, small_all = gather_proj(n_dev, x_act, small, w_blocks, qkv)
    u_all = u_all.reshape(seq, width)
    g_attn = small_all[:, 0, :rows].reshape(width)
    g_mlp = small_all[:, 0, rows:2 * rows].reshape(width)
    pos_all = small_all[:, 1:1 + tok // (2 * rows)]

    w_all = gather(weight_block(w_gate, w_up, w_o, w_down))
    w_gu = w_all[:, :2 * ff]
    w_o_all = w_all[:, 2 * ff:2 * ff + width]
    w_down_at = 2 * ff + width
    w_down_all = join_down(w_all.reshape(n_dev, rows, w_all.shape[1]), w_down_at, (n_dev, ff_s, width)).reshape(ff, width)
    me = lax.axis_index(SEQ_AXIS)
    w_cols = jnp.concatenate([lax.dynamic_slice(w_all, (0, at + me * ff_s), (width, ff_s)) for at in (0, ff)], axis=1)

    half = head_dim // 2
    inv_freq = ROPE_BASE ** (-(jnp.arange(half, dtype=F32) * (2.0 / head_dim)))
    angle_t = inv_freq[:, None] * pos_all.reshape(1, seq)
    cos_t, sin_t = jnp.cos(angle_t), jnp.sin(angle_t)

    q_t = (rope_t(proj_t[:head_dim], cos_t, sin_t).astype(BF16).astype(F32) * (head_dim ** -0.5)).astype(BF16)
    k_t = rope_t(proj_t[head_dim:2 * head_dim], cos_t, sin_t).astype(BF16)
    v_t = proj_t[2 * head_dim:].astype(BF16)
    k_in, v_in = k_t.T, v_t.T
    o_blocks, of_t, lse = attention_fwd(q_t, k_in, v_t, n_dev)
    o_loc = exchange(o_blocks).reshape(width, tok)
    w_parts = jnp.stack([w.reshape(rows, heads * head_dim) for w in (w_q, w_k, w_v)])
    o_loc, w_parts, v_in, w_down_all = lax.optimization_barrier((o_loc, w_parts, v_in, w_down_all))

    hidden = (x_act.astype(F32) + dot(o_loc, w_o_all, 0, 0)).astype(BF16)
    normed_mlp, inv_rms_mlp = rms_norm(hidden, g_mlp)
    a_dy = jnp.concatenate([normed_mlp, grad_out], axis=1)
    normed_mlp, a_dy = lax.optimization_barrier((normed_mlp, a_dy))
    a_dy = gather(a_dy)
    pre = with_layout_constraint(dot(normed_mlp, w_gu, 1, 0), Layout(major_to_minor=(0, 1)))
    gate_pre, up_pre = pre[:, :ff], pre[:, ff:]
    mixed = (jax.nn.silu(gate_pre) * up_pre).astype(BF16)
    y_out = (hidden.astype(F32) + dot(mixed, w_down_all, 1, 0)).astype(BF16)

    d_mixed = dot(grad_out, w_down_all, 1, 1).astype(BF16).astype(F32)
    d_gu = jnp.concatenate(gate_backward(d_mixed, gate_pre, up_pre), axis=1)
    d_normed = dot(d_gu, w_gu, 1, 1).astype(BF16)
    d_hid_norm, part_g_mlp = rms_norm_bwd(hidden, g_mlp, inv_rms_mlp, d_normed)
    d_hidden = (grad_out.astype(F32) + d_hid_norm).astype(BF16)
    do_blocks = exchange(dot(w_o_all, d_hidden, 1, 1).astype(BF16).reshape(n_dev, head_dim, tok))
    half_n = n_dev // 2
    pairs = [(i, (i + half_n) % n_dev) for i in range(n_dev)]
    near = (me // half_n) * half_n
    o_far = lax.ppermute(lax.dynamic_slice_in_dim(o_blocks, half_n - near, half_n), SEQ_AXIS, pairs)
    do_blocks, y_out = lax.optimization_barrier((do_blocks, y_out))
    dh_half = lax.all_gather(d_hidden, SEQ_AXIS, axis=0, tiled=True, axis_index_groups=[list(range(half_n)), list(range(half_n, n_dev))])

    do_t = jnp.transpose(do_blocks, (1, 0, 2)).reshape(head_dim, seq)
    d_blocks, d_proj_t, *w_qkv_all = attention_bwd(q_t, do_t, of_t, lse, k_in, k_t, v_in, cos_t, sin_t, w_parts, n_dev)
    d_proj = exchange(d_blocks)

    grad_w_qkv = dot(d_proj_t, u_all, 1, 0)
    attn_send = pack_pairs(grad_w_qkv, n_dev, rows)
    d_proj, attn_send = lax.optimization_barrier((d_proj, attn_send))
    attn_back = exchange(attn_send)
    d_proj = d_proj.reshape(heads, 3, head_dim, tok)
    inv_rms = lax.rsqrt(jnp.mean(jnp.square(x_act.astype(F32)), axis=-1, keepdims=True) + RMS_EPS)
    d_u = sum(dot(d_proj[:, p].reshape(heads * head_dim, tok), w_qkv_all[p].reshape(width, heads * head_dim), 0, 1) for p in range(3)).astype(BF16)
    d_x_norm, part_g_attn = rms_norm_bwd(x_act, g_attn, inv_rms, d_u)
    grad_x = (d_hidden.astype(F32) + d_x_norm).astype(BF16)
    gain_send = jnp.concatenate([part_g_attn.reshape(n_dev, 1, rows), part_g_mlp.reshape(n_dev, 1, rows)], axis=2)

    a_all, dy_all = a_dy[:, :width], a_dy[:, width:]
    pre_t = dot(w_cols, a_all, 0, 1)
    gate_t, up_t = pre_t[:ff_s], pre_t[ff_s:]
    d_mixed_t = dot(w_down, dy_all, 1, 1).astype(BF16).astype(F32)
    mixed_t = (jax.nn.silu(gate_t) * up_t).astype(BF16)
    d_gu_t = jnp.concatenate(gate_backward(d_mixed_t, gate_t, up_t), axis=0)
    grad_w_gu = dot(d_gu_t, a_all, 1, 0)
    mlp_send = pack_pairs(grad_w_gu, n_dev, rows, jnp.pad(gain_send, ((0, 0), (0, 7), (0, 0))))
    attn_back, mlp_send, mixed_t = lax.optimization_barrier((attn_back, mlp_send, mixed_t))
    mlp_back = exchange(mlp_send)
    grad_w_down = dot(mixed_t, dy_all, 1, 0)

    o_far, dh_half, o_blocks, grad_w_down = lax.optimization_barrier((o_far, dh_half, o_blocks, grad_w_down))
    o_pair = jnp.concatenate([lax.dynamic_slice_in_dim(o_blocks, near, half_n), o_far], axis=1)
    part_w_o = dot(o_pair.transpose(1, 0, 2).reshape(2 * head_dim, seq // 2), dh_half, 1, 0)
    grad_w_o = (part_w_o[:head_dim] + lax.ppermute(part_w_o[head_dim:], SEQ_AXIS, pairs))[None]

    grad_w_q, grad_w_k, grad_w_v = split_heads(attn_back, head_dim)
    mlp_back, grad_w_down, grad_w_q, grad_w_k, grad_w_v, grad_w_o = lax.optimization_barrier((mlp_back, grad_w_down, grad_w_q, grad_w_k, grad_w_v, grad_w_o))
    gains = jnp.sum(mlp_back[:, ff_s], axis=0)
    grad_g_attn, grad_g_mlp = gains[:rows], gains[rows:]
    grad_w_gate, grad_w_up = join_columns(mlp_back, ff_s)
    return (y_out, grad_x, grad_g_attn, grad_w_q, grad_w_k, grad_w_v, grad_w_o, grad_g_mlp, grad_w_gate, grad_w_up, grad_w_down)


def solution(mesh):
    n_dev = mesh.shape[SEQ_AXIS]
    token_spec = P(SEQ_AXIS, None)
    cube_spec = P(SEQ_AXIS, None, None)
    gain_spec = P(SEQ_AXIS)
    weight_specs = (gain_spec, cube_spec, cube_spec, cube_spec, cube_spec, gain_spec, token_spec, token_spec, token_spec)
    return jax.shard_map(lambda *args: device_step(n_dev, *args), mesh=mesh, in_specs=(token_spec, gain_spec, token_spec) + weight_specs, out_specs=(token_spec, token_spec) + weight_specs, check_vma=False)
```
